32 devices in a mesh: shard: 4 (over z), ctx: 2 (over x), tp: 4 (over y, core).
Axes of the slice: x: 2, y: 2, z: 4, core: 2. Of those that a mesh axis runs over, the one named last changes fastest.
Arguments:
- noised: bfloat16 [4, 4, 64, 64], P('shard', None, ('ctx', 'tp')), may hold values from -6 to 6
- velocity: bfloat16 [4, 4, 64, 64], P('shard', None, ('ctx', 'tp')), may hold values from -6 to 6
- labels: int32 [4], P('shard'), may hold values from 0 to 999
- time_ids: int32 [4], P('shard'), may hold values from 0 to 999
- stem: float32 [3592, 768], P(None, ('shard', 'tp')), may hold values from -0.21875 to 0.21875
- stem_mean: float32 [3592, 768], P(None, ('shard', 'tp')), may hold values from -0.00036621094 to 0.00036621094
- stem_square: float32 [3592, 768], P(None, ('shard', 'tp')), may hold values from 1e-10 to 1e-08
- modulation: float32 [4, 768, 4608], P(None, ('shard', 'tp')), may hold values from -0.875 to 0.875
- modulation_mean: float32 [4, 768, 4608], P(None, ('shard', 'tp')), may hold values from -0.00036621094 to 0.00036621094
- modulation_square: float32 [4, 768, 4608], P(None, ('shard', 'tp')), may hold values from 1e-10 to 1e-08
- attention_in: float32 [4, 3, 768, 768], P(None, None, 'shard', 'tp'), may hold values from -0.21875 to 0.21875
- attention_in_mean: float32 [4, 3, 768, 768], P(None, None, 'shard', 'tp'), may hold values from -0.00036621094 to 0.00036621094
- attention_in_square: float32 [4, 3, 768, 768], P(None, None, 'shard', 'tp'), may hold values from 1e-10 to 1e-08
- attention_out: float32 [4, 768, 768], P(None, 'shard', 'tp'), may hold values from -0.875 to 0.875
- attention_out_mean: float32 [4, 768, 768], P(None, 'shard', 'tp'), may hold values from -0.00036621094 to 0.00036621094
- attention_out_square: float32 [4, 768, 768], P(None, 'shard', 'tp'), may hold values from 1e-10 to 1e-08
- feedforward: float32 [4, 2, 768, 3072], P(None, None, 'shard', 'tp'), may hold values from -0.21875 to 0.21875
- feedforward_mean: float32 [4, 2, 768, 3072], P(None, None, 'shard', 'tp'), may hold values from -0.00036621094 to 0.00036621094
- feedforward_square: float32 [4, 2, 768, 3072], P(None, None, 'shard', 'tp'), may hold values from 1e-10 to 1e-08
Outputs:
- train_loss: float32 [], replicated
- total_norm: float32 [], replicated
- stem_new: float32 [3592, 768], P(None, ('shard', 'tp'))
- stem_mean_new: float32 [3592, 768], P(None, ('shard', 'tp'))
- stem_square_new: float32 [3592, 768], P(None, ('shard', 'tp'))
- stem_copy: bfloat16 [3592, 768], P(None, ('shard', 'tp'))
- modulation_new: float32 [4, 768, 4608], P(None, ('shard', 'tp'))
- modulation_mean_new: float32 [4, 768, 4608], P(None, ('shard', 'tp'))
- modulation_square_new: float32 [4, 768, 4608], P(None, ('shard', 'tp'))
- modulation_copy: bfloat16 [4, 768, 4608], P(None, ('shard', 'tp'))
- attention_in_new: float32 [4, 3, 768, 768], P(None, None, 'shard', 'tp')
- attention_in_mean_new: float32 [4, 3, 768, 768], P(None, None, 'shard', 'tp')
- attention_in_square_new: float32 [4, 3, 768, 768], P(None, None, 'shard', 'tp')
- attention_in_copy: bfloat16 [4, 3, 768, 768], P(None, None, 'shard', 'tp')
- attention_out_new: float32 [4, 768, 768], P(None, 'shard', 'tp')
- attention_out_mean_new: float32 [4, 768, 768], P(None, 'shard', 'tp')
- attention_out_square_new: float32 [4, 768, 768], P(None, 'shard', 'tp')
- attention_out_copy: bfloat16 [4, 768, 768], P(None, 'shard', 'tp')
- feedforward_new: float32 [4, 2, 768, 3072], P(None, None, 'shard', 'tp')
- feedforward_mean_new: float32 [4, 2, 768, 3072], P(None, None, 'shard', 'tp')
- feedforward_square_new: float32 [4, 2, 768, 3072], P(None, None, 'shard', 'tp')
- feedforward_copy: bfloat16 [4, 2, 768, 3072], P(None, None, 'shard', 'tp')
The draws below stay inside these ranges and needn't reach their ends.
All inputs are finite; a program needn't handle non-finite values.
Results may differ from the reference program's by a relative error of at most 0.019.
The reference program's roundings to bfloat16 on the way (of `features`, `time_hidden`, `gated_condition`, `pieces`, `normed_one`, `mixed_heads` and `activated`) count: a program that leaves them out, or rounds other values in their place, can miss the bound.
Values may be sent and summed in bfloat16 or wider, within the bound.
A program may use at most 320 MiB of HBM per device.

```python
import math
import jax
import jax.numpy as jnp
from jax import lax

D = 768
HEADS = 12
HEAD_DIM = 64
FF = 3072
CLASSES = 1000
FREQ = 256
CHANNELS = 4
SIDE = 64
PATCH = 2
STEPS = 1000
LAYERS = 4
GRID = 32
PATCHES = 1024
PDIM = 16
MISC_ROWS = 3592
LATENTS = 4


def plant(values, key, smallest, high):
    longest = values.shape.index(max(values.shape))
    spots = []
    for shift in (0, 1):
        where = [jax.random.randint(jax.random.fold_in(key, axis), (), 0, length) for axis, length in enumerate(values.shape)]
        where[longest] = (where[longest] + shift) % values.shape[longest]
        spots.append(tuple(where))
    return values.at[spots[0]].set(smallest).at[spots[1]].set(high)


def level_of(stream_key, dims, cuts, least, high):
    gain, own = 1.0, jax.random.fold_in(stream_key, 6)
    for dim, parts in cuts:
        draws = jnp.exp(jax.random.uniform(jax.random.fold_in(own, dim), (parts,), jnp.float32, least / len(cuts), high / len(cuts)))
        gain = gain * jnp.repeat(draws, dims[dim] // parts).reshape([-1 if axis == dim else 1 for axis in range(len(dims))])
    return gain


def centred(key, shape, width, limit, split=(), dtype=jnp.bfloat16):
    values = width * jax.random.normal(key, shape, jnp.float32)
    if split:
        values = values * level_of(key, shape, split, -0.22, 0.18)
    return jnp.clip(values, -limit, limit).astype(dtype)


def setup_inputs(seed: int = 0) -> dict:
    seeds = jax.random.split(jax.random.key(seed), 20)
    noised = centred(seeds[0], (LATENTS, CHANNELS, SIDE, SIDE), 1.0, 6.0, ((0, 4), (2, 8)))
    velocity = centred(seeds[1], (LATENTS, CHANNELS, SIDE, SIDE), 1.0, 6.0, ((0, 4), (2, 8)))
    labels = plant(jax.random.randint(seeds[2], (LATENTS,), 0, CLASSES), jax.random.fold_in(seeds[2], 1), 0, CLASSES - 1).astype(jnp.int32)
    time_ids = plant(jax.random.randint(seeds[3], (LATENTS,), 0, STEPS), jax.random.fold_in(seeds[3], 1), 0, STEPS - 1).astype(jnp.int32)
    stem = centred(seeds[4], (MISC_ROWS, D), D ** -0.5, 0.21875, ((1, 16),), jnp.float32)
    stem_mean = centred(seeds[5], (MISC_ROWS, D), 0.00006, 0.00036621094, ((1, 16),), jnp.float32)
    stem_square = jnp.clip(jnp.exp(math.log(9.99999993922529e-09) - 4.6051702 * jax.random.uniform(seeds[6], (MISC_ROWS, D), jnp.float32) ** level_of(seeds[6], (MISC_ROWS, D), ((1, 16),), -0.2, 0.2)), 1.000000013351432e-10, 9.99999993922529e-09)
    modulation = centred(seeds[7], (LAYERS, D, 6 * D), 0.15, 0.875, ((1, 16),), jnp.float32)
    modulation_mean = centred(seeds[8], (LAYERS, D, 6 * D), 0.00006, 0.00036621094, ((1, 16),), jnp.float32)
    modulation_square = jnp.clip(jnp.exp(math.log(9.99999993922529e-09) - 4.6051702 * jax.random.uniform(seeds[9], (LAYERS, D, 6 * D), jnp.float32) ** level_of(seeds[9], (LAYERS, D, 6 * D), ((1, 16),), -0.2, 0.2)), 1.000000013351432e-10, 9.99999993922529e-09)
    attention_in = centred(seeds[10], (LAYERS, 3, D, D), D ** -0.5, 0.21875, ((2, 4), (3, 4)), jnp.float32)
    attention_in_mean = centred(seeds[11], (LAYERS, 3, D, D), 0.00006, 0.00036621094, ((2, 4), (3, 4)), jnp.float32)
    attention_in_square = jnp.clip(jnp.exp(math.log(9.99999993922529e-09) - 4.6051702 * jax.random.uniform(seeds[12], (LAYERS, 3, D, D), jnp.float32) ** level_of(seeds[12], (LAYERS, 3, D, D), ((2, 4), (3, 4)), -0.2, 0.2)), 1.000000013351432e-10, 9.99999993922529e-09)
    attention_out = centred(seeds[13], (LAYERS, D, D), (D // 16) ** -0.5, 0.875, ((1, 4), (2, 4)), jnp.float32)
    attention_out_mean = centred(seeds[14], (LAYERS, D, D), 0.00006, 0.00036621094, ((1, 4), (2, 4)), jnp.float32)
    attention_out_square = jnp.clip(jnp.exp(math.log(9.99999993922529e-09) - 4.6051702 * jax.random.uniform(seeds[15], (LAYERS, D, D), jnp.float32) ** level_of(seeds[15], (LAYERS, D, D), ((1, 4), (2, 4)), -0.2, 0.2)), 1.000000013351432e-10, 9.99999993922529e-09)
    feedforward = centred(seeds[16], (LAYERS, 2, D, FF), D ** -0.5, 0.21875, ((2, 4), (3, 4)), jnp.float32)
    feedforward_mean = centred(seeds[17], (LAYERS, 2, D, FF), 0.00006, 0.00036621094, ((2, 4), (3, 4)), jnp.float32)
    feedforward_square = jnp.clip(jnp.exp(math.log(9.99999993922529e-09) - 4.6051702 * jax.random.uniform(seeds[18], (LAYERS, 2, D, FF), jnp.float32) ** level_of(seeds[18], (LAYERS, 2, D, FF), ((2, 4), (3, 4)), -0.2, 0.2)), 1.000000013351432e-10, 9.99999993922529e-09)
    return dict(noised=noised, velocity=velocity, labels=labels, time_ids=time_ids, stem=stem, stem_mean=stem_mean, stem_square=stem_square, modulation=modulation, modulation_mean=modulation_mean, modulation_square=modulation_square, attention_in=attention_in, attention_in_mean=attention_in_mean, attention_in_square=attention_in_square, attention_out=attention_out, attention_out_mean=attention_out_mean, attention_out_square=attention_out_square, feedforward=feedforward, feedforward_mean=feedforward_mean, feedforward_square=feedforward_square)


norm_eps = 1e-06
clip_level = 0.5
learn_rate = 0.01
beta_first = 0.5
beta_second = 0.5
adam_eps = 1e-08
weight_decay = 0.1
bias_fix = 0.875
highest = lax.Precision.HIGHEST

@jax.custom_vjp
def low(v):
    return lax.optimization_barrier(v.astype(jnp.bfloat16)).astype(jnp.float32)

@jax.custom_vjp
def low_back(v):
    return v

def low_keep(v):
    return (low(v), None)

def low_pass(kept, grad):
    return (grad,)

def back_keep(v):
    return (v, None)

def back_low(kept, grad):
    return (low(grad),)
low.defvjp(low_keep, low_pass)
low_back.defvjp(back_keep, back_low)

def layer_norm(values):
    centre = values - lax.optimization_barrier(jnp.mean(values, -1, keepdims=True))
    spread = lax.optimization_barrier(jnp.mean(centre * centre, -1, keepdims=True))
    return centre * lax.rsqrt(spread + norm_eps)

def modulate(values, shift_rows, scale_rows):
    return layer_norm(values) * (1.0 + scale_rows) + shift_rows

def gelu_tanh(values):
    return jax.nn.gelu(values, approximate=True)

def patchify(image_in):
    latent_count, channels, height, columns = image_in.shape
    shaped = image_in.reshape(latent_count, channels, height // PATCH, PATCH, columns // PATCH, PATCH)
    shaped = shaped.transpose(0, 2, 4, 3, 5, 1)
    return shaped.reshape(latent_count, height // PATCH * (columns // PATCH), PATCH * PATCH * channels)

def positions(first_row, height, columns, model_width):
    quarter = model_width // 4
    omegas = jnp.exp(-math.log(10000.0) * jnp.arange(quarter).astype(jnp.float32) / quarter)
    row_angle = (first_row + jnp.arange(height)).astype(jnp.float32)[:, None] * omegas[None, :]
    col_angle = jnp.arange(columns).astype(jnp.float32)[:, None] * omegas[None, :]
    row_part = jnp.concatenate([jnp.sin(row_angle), jnp.cos(row_angle)], -1)
    col_part = jnp.concatenate([jnp.sin(col_angle), jnp.cos(col_angle)], -1)
    grid_table = jnp.concatenate([jnp.broadcast_to(col_part[None], (height, columns, 2 * quarter)), jnp.broadcast_to(row_part[:, None], (height, columns, 2 * quarter))], -1)
    return grid_table.reshape(height * columns, model_width)

def time_features(step_ids):
    half_width = FREQ // 2
    frequencies = jnp.exp(-math.log(10000.0) * jnp.arange(half_width).astype(jnp.float32) / half_width)
    angles = step_ids.astype(jnp.float32)[:, None] * frequencies[None, :]
    return jnp.concatenate([jnp.cos(angles), jnp.sin(angles)], -1)

def split_stem(stem_rows):
    bounds = [CLASSES, FREQ, D, D, D, PDIM, PDIM]
    pieces_out = []
    offset = 0
    for extent in bounds:
        pieces_out.append(stem_rows[offset:offset + extent])
        offset = offset + extent
    return pieces_out

def group_loss(weights, noised_g, velocity_g, label_g, time_g):
    stem, modulation, attention_in, attention_out, feedforward = weights
    class_table, time_in, time_out, final_shift, final_scale, patch_in, head_rows = split_stem(stem)
    group_size = noised_g.shape[0]
    score_scale = HEAD_DIM ** (-0.5)
    features = low(time_features(time_g))
    time_hidden = jax.nn.silu(jnp.dot(features, time_in, precision=highest))
    time_embed = jnp.dot(low(time_hidden), time_out, precision=highest)
    onehot = (label_g[:, None] == jnp.arange(CLASSES)[None, :]).astype(jnp.float32)
    condition = time_embed + jnp.dot(onehot, class_table, precision=highest)
    gated_condition = low(jax.nn.silu(condition))
    pieces = patchify(noised_g)
    embedded = low_back(jnp.einsum('bpf,fd->bpd', pieces, patch_in, precision=highest))
    hidden = embedded + positions(0, GRID, GRID, D)[None]
    for layer_at in range(LAYERS):
        layer_modulation = jnp.dot(gated_condition, modulation[layer_at], precision=highest).reshape(group_size, 6, 1, D)
        shift_one, scale_one, gate_one, shift_two, scale_two, gate_two = [layer_modulation[:, number] for number in range(6)]
        normed_one = low(modulate(hidden, shift_one, scale_one))
        query_heads = low(low_back(score_scale * jnp.einsum('bpd,de->bpe', normed_one, attention_in[layer_at, 0], precision=highest)))
        key_heads = low(low_back(jnp.einsum('bpd,de->bpe', normed_one, attention_in[layer_at, 1], precision=highest)))
        value_heads = low(low_back(jnp.einsum('bpd,de->bpe', normed_one, attention_in[layer_at, 2], precision=highest)))
        query_heads = query_heads.reshape(group_size, PATCHES, HEADS, HEAD_DIM)
        key_heads = key_heads.reshape(group_size, PATCHES, HEADS, HEAD_DIM)
        value_heads = value_heads.reshape(group_size, PATCHES, HEADS, HEAD_DIM)
        scores = low_back(jnp.einsum('bqhe,bkhe->bhqk', query_heads, key_heads, precision=highest))
        weights_low = low(jax.nn.softmax(scores, -1))
        mixed_heads = low(low_back(jnp.einsum('bhqk,bkhe->bqhe', weights_low, value_heads, precision=highest)))
        mixed_heads = mixed_heads.reshape(group_size, PATCHES, D)
        branch_one = low_back(jnp.einsum('bpe,de->bpd', mixed_heads, attention_out[layer_at], precision=highest))
        hidden = hidden + gate_one * branch_one
        normed_two = low(modulate(hidden, shift_two, scale_two))
        hidden_pre = low_back(jnp.einsum('bpd,df->bpf', normed_two, feedforward[layer_at, 0], precision=highest))
        activated = low(gelu_tanh(hidden_pre))
        branch_two = low_back(jnp.einsum('bpf,df->bpd', activated, feedforward[layer_at, 1], precision=highest))
        hidden = hidden + gate_two * branch_two
    end_shift = jnp.dot(gated_condition, final_shift, precision=highest)[:, None, :]
    end_scale = jnp.dot(gated_condition, final_scale, precision=highest)[:, None, :]
    final_normed = low(modulate(hidden, end_shift, end_scale))
    predicted = low_back(jnp.einsum('bpd,cd->bpc', final_normed, head_rows, precision=highest))
    misfit = predicted - patchify(velocity_g)
    weighting = 0.5 + time_g.astype(jnp.float32) / STEPS
    return jnp.sum(weighting[:, None, None] * misfit * misfit)

def adam_update(master, first_moment, second_moment, gradient, factor):
    clipped = gradient * factor
    first_new = beta_first * first_moment + (1.0 - beta_first) * clipped
    second_new = beta_second * second_moment + (1.0 - beta_second) * clipped * clipped
    direction = first_new / bias_fix / (jnp.sqrt(second_new / bias_fix) + adam_eps)
    master_new = master - learn_rate * (direction + weight_decay * master)
    return (master_new, first_new, second_new, master_new.astype(jnp.bfloat16))

def reference(noised, velocity, labels, time_ids, stem, stem_mean, stem_square, modulation, modulation_mean, modulation_square, attention_in, attention_in_mean, attention_in_square, attention_out, attention_out_mean, attention_out_square, feedforward, feedforward_mean, feedforward_square):
    group_size = math.gcd(LATENTS, 4)
    group_count = LATENTS // group_size
    group_in = (noised.astype(jnp.float32).reshape((group_count, group_size) + noised.shape[1:]), velocity.astype(jnp.float32).reshape((group_count, group_size) + velocity.shape[1:]), labels.reshape(group_count, group_size), time_ids.reshape(group_count, group_size))
    checked = jax.checkpoint(group_loss)

    def total_loss(params):
        rounded = tuple((low(array) for array in params))

        def accumulate(running, inputs_now):
            return (running + checked(rounded, inputs_now[0], inputs_now[1], inputs_now[2], inputs_now[3]), None)
        summed, unused = lax.scan(accumulate, jnp.zeros((), jnp.float32), group_in)
        return summed / (LATENTS * PATCHES * PDIM)
    params = (stem, modulation, attention_in, attention_out, feedforward)
    train_loss, pullback = jax.vjp(total_loss, params)
    gradients = pullback(jnp.ones((), jnp.float32))[0]
    squares = sum((jnp.sum(gradient * gradient) for gradient in gradients))
    total_norm = jnp.sqrt(squares)
    factor = clip_level / jnp.maximum(total_norm, clip_level)
    stem_out = adam_update(stem, stem_mean, stem_square, gradients[0], factor)
    mod_out = adam_update(modulation, modulation_mean, modulation_square, gradients[1], factor)
    in_out = adam_update(attention_in, attention_in_mean, attention_in_square, gradients[2], factor)
    proj_out = adam_update(attention_out, attention_out_mean, attention_out_square, gradients[3], factor)
    feed_out = adam_update(feedforward, feedforward_mean, feedforward_square, gradients[4], factor)
    return (train_loss, total_norm, stem_out[0], stem_out[1], stem_out[2], stem_out[3], mod_out[0], mod_out[1], mod_out[2], mod_out[3], in_out[0], in_out[1], in_out[2], in_out[3], proj_out[0], proj_out[1], proj_out[2], proj_out[3], feed_out[0], feed_out[1], feed_out[2], feed_out[3])
```

```python
import math

import jax
import jax.numpy as jnp
from jax import lax
from jax.sharding import PartitionSpec as P

D = 768
HEAD_DIM = 64
CLASSES = 1000
FREQ = 256
PATCH = 2
STEPS = 1000
LAYERS = 4
PATCHES = 1024
PDIM = 16


norm_eps = 1e-06
clip_level = 0.5
learn_rate = 0.01
beta_first = 0.5
beta_second = 0.5
adam_eps = 1e-08
weight_decay = 0.1
bias_fix = 0.875
highest = lax.Precision.HIGHEST


def layer_norm(values):
    centre = values - jnp.mean(values, -1, keepdims=True)
    spread = jnp.mean(centre * centre, -1, keepdims=True)
    return centre * lax.rsqrt(spread + norm_eps)


def modulate(values, shift_rows, scale_rows):
    return layer_norm(values) * (1.0 + scale_rows) + shift_rows


def gelu_tanh(values):
    return jax.nn.gelu(values, approximate=True)


def patchify(image_in):
    latent_count, channels, height, columns = image_in.shape
    shaped = image_in.reshape(
        latent_count, channels, height // PATCH, PATCH, columns // PATCH, PATCH
    )
    shaped = shaped.transpose(0, 2, 4, 3, 5, 1)
    return shaped.reshape(
        latent_count, height // PATCH * (columns // PATCH), PATCH * PATCH * channels
    )


def positions(first_row, height, columns, model_width):
    quarter = model_width // 4
    omegas = jnp.exp(-math.log(10000.0) * jnp.arange(quarter).astype(jnp.float32) / quarter)
    row_angle = (first_row + jnp.arange(height)).astype(jnp.float32)[:, None] * omegas[None, :]
    col_angle = jnp.arange(columns).astype(jnp.float32)[:, None] * omegas[None, :]
    row_part = jnp.concatenate([jnp.sin(row_angle), jnp.cos(row_angle)], -1)
    col_part = jnp.concatenate([jnp.sin(col_angle), jnp.cos(col_angle)], -1)
    grid_table = jnp.concatenate(
        [
            jnp.broadcast_to(col_part[None], (height, columns, 2 * quarter)),
            jnp.broadcast_to(row_part[:, None], (height, columns, 2 * quarter)),
        ],
        -1,
    )
    return grid_table.reshape(height * columns, model_width)


def time_features(step_ids):
    half_width = FREQ // 2
    frequencies = jnp.exp(
        -math.log(10000.0) * jnp.arange(half_width).astype(jnp.float32) / half_width
    )
    angles = step_ids.astype(jnp.float32)[:, None] * frequencies[None, :]
    return jnp.concatenate([jnp.cos(angles), jnp.sin(angles)], -1)


def split_stem(stem_rows):
    bounds = [CLASSES, FREQ, D, D, D, PDIM, PDIM]
    pieces_out = []
    offset = 0
    for extent in bounds:
        pieces_out.append(stem_rows[offset : offset + extent])
        offset = offset + extent
    return pieces_out


def adam_update(master, first_moment, second_moment, gradient, factor):
    clipped = gradient * factor
    first_new = beta_first * first_moment + (1.0 - beta_first) * clipped
    second_new = beta_second * second_moment + (1.0 - beta_second) * clipped * clipped
    direction = first_new / bias_fix / (jnp.sqrt(second_new / bias_fix) + adam_eps)
    master_new = master - learn_rate * (direction + weight_decay * master)
    return (master_new, first_new, second_new, master_new.astype(jnp.bfloat16))


GROUP = ("ctx", "tp")
OWNERS = ("shard", "tp")
EVERY = ("shard", "ctx", "tp")


def gather_group(values):
    return lax.all_gather(values, GROUP, axis=0, tiled=True)


def scatter_group(part_sum):
    return lax.psum_scatter(
        part_sum.astype(jnp.bfloat16), GROUP, scatter_dimension=0, tiled=True
    ).astype(jnp.float32)


def scatter_tp(part_sum):
    return lax.psum_scatter(
        part_sum.astype(jnp.bfloat16), "tp", scatter_dimension=0, tiled=True
    ).astype(jnp.float32)


def own_half(values):
    half = values.shape[0] // lax.axis_size("ctx")
    return lax.dynamic_slice_in_dim(values, lax.axis_index("ctx") * half, half, 0)


def into_heads(values):
    return values.reshape(values.shape[0], -1, HEAD_DIM)


def attention_forward(hidden, mods, weights):
    width = weights.shape[1] // 4
    shift, scale, gate = mods[0:1], mods[1:2], mods[2:3]
    normed = gather_group(modulate(hidden, shift, scale).astype(jnp.bfloat16))
    query = jnp.dot(own_half(normed), weights[:, :width], preferred_element_type=jnp.float32)
    query = into_heads((query * HEAD_DIM**-0.5).astype(jnp.bfloat16))
    key_value = jnp.dot(
        normed, weights[:, width : 3 * width], preferred_element_type=jnp.float32
    ).astype(jnp.bfloat16)
    key, value = into_heads(key_value[:, :width]), into_heads(key_value[:, width:])
    scores = jnp.einsum("qhe,khe->hqk", query, key, preferred_element_type=jnp.float32)
    row_top = jnp.max(scores, -1, keepdims=True)
    exponent = jnp.exp(scores - row_top)
    row_total = jnp.sum(exponent, -1, keepdims=True)
    log_total = row_top + jnp.log(row_total)
    weights_low = (exponent / row_total).astype(jnp.bfloat16)
    mixed = jnp.einsum("hqk,khe->qhe", weights_low, value, preferred_element_type=jnp.float32)
    mixed = mixed.astype(jnp.bfloat16).reshape(mixed.shape[0], -1)
    branch = scatter_tp(
        jnp.einsum(
            "pe,de->pd", mixed, weights[:, 3 * width :], preferred_element_type=jnp.float32
        )
    )
    kept = (hidden, normed, query, key, value, log_total, mixed, branch)
    return hidden + gate * branch, kept


def feed_forward(hidden, mods, weights):
    width = weights.shape[1] // 2
    shift, scale, gate = mods[3:4], mods[4:5], mods[5:6]
    normed = gather_group(modulate(hidden, shift, scale).astype(jnp.bfloat16))
    hidden_pre = jnp.dot(normed, weights[:, :width], preferred_element_type=jnp.float32)
    activated = gelu_tanh(hidden_pre).astype(jnp.bfloat16)
    branch = scatter_group(
        jnp.einsum("pf,df->pd", activated, weights[:, width:], preferred_element_type=jnp.float32)
    )
    return hidden + gate * branch, (hidden, normed, hidden_pre, branch)


def feed_backward(grad_hidden, mods, weights, kept):
    hidden, normed, hidden_pre, branch = kept
    width = weights.shape[1] // 2
    shift, scale, gate = mods[3:4], mods[4:5], mods[5:6]
    grad_gate = jnp.sum(grad_hidden * branch, 0, keepdims=True)
    grad_branch = gather_group((gate * grad_hidden).astype(jnp.bfloat16))
    activated, gelu_pull = jax.vjp(gelu_tanh, hidden_pre)
    grad_down = jnp.einsum(
        "pd,pf->df",
        grad_branch,
        activated.astype(jnp.bfloat16),
        preferred_element_type=jnp.float32,
    )
    grad_act = jnp.dot(grad_branch, weights[:, width:], preferred_element_type=jnp.float32)
    grad_pre = gelu_pull(grad_act)[0].astype(jnp.bfloat16)
    grad_up = jnp.einsum("pd,pf->df", normed, grad_pre, preferred_element_type=jnp.float32)
    grad_normed = scatter_group(
        jnp.einsum("pf,df->pd", grad_pre, weights[:, :width], preferred_element_type=jnp.float32)
    )
    step, grad_shift, grad_scale = jax.vjp(modulate, hidden, shift, scale)[1](grad_normed)
    grads = jnp.concatenate([grad_up, grad_down], 1).astype(jnp.bfloat16)
    return grad_hidden + step, grads, jnp.concatenate([grad_shift, grad_scale, grad_gate], 0)


def attention_backward(grad_hidden, mods, weights, kept):
    hidden, normed, query, key, value, log_total, mixed, branch = kept
    width = weights.shape[1] // 4
    shift, scale, gate = mods[0:1], mods[1:2], mods[2:3]
    grad_gate = jnp.sum(grad_hidden * branch, 0, keepdims=True)
    grad_branch = lax.all_gather(
        (gate * grad_hidden).astype(jnp.bfloat16), "tp", axis=0, tiled=True
    )
    grad_out = jnp.einsum("pd,pe->de", grad_branch, mixed, preferred_element_type=jnp.float32)
    grad_mixed = into_heads(
        jnp.dot(grad_branch, weights[:, 3 * width :], preferred_element_type=jnp.float32).astype(
            jnp.bfloat16
        )
    )
    scores = jnp.einsum("qhe,khe->hqk", query, key, preferred_element_type=jnp.float32)
    attention_weights = jnp.exp(scores - log_total)
    weights_low = attention_weights.astype(jnp.bfloat16)
    grad_value = jnp.einsum(
        "hqk,qhe->khe", weights_low, grad_mixed, preferred_element_type=jnp.float32
    ).astype(jnp.bfloat16)
    grad_probs = jnp.einsum(
        "qhe,khe->hqk", grad_mixed, value, preferred_element_type=jnp.float32
    )
    inner_sum = jnp.sum(attention_weights * grad_probs, -1, keepdims=True)
    grad_scores = (attention_weights * (grad_probs - inner_sum)).astype(jnp.bfloat16)
    grad_query = jnp.einsum(
        "hqk,khe->qhe", grad_scores, key, preferred_element_type=jnp.float32
    ).astype(jnp.bfloat16)
    grad_key = jnp.einsum(
        "hqk,qhe->khe", grad_scores, query, preferred_element_type=jnp.float32
    ).astype(jnp.bfloat16)
    rows = normed.shape[0]
    grad_query = (grad_query * HEAD_DIM**-0.5).astype(jnp.bfloat16).reshape(query.shape[0], -1)
    pair = jnp.concatenate([grad_key.reshape(rows, -1), grad_value.reshape(rows, -1)], 1)
    grad_wq = jnp.einsum(
        "pd,pe->de", own_half(normed), grad_query, preferred_element_type=jnp.float32
    )
    grad_kv = jnp.einsum("pd,pe->de", normed, pair, preferred_element_type=jnp.float32)
    from_pair = jnp.einsum(
        "pe,de->pd", pair, weights[:, width : 3 * width], preferred_element_type=jnp.float32
    )
    from_query = jnp.einsum(
        "pe,de->pd", grad_query, weights[:, :width], preferred_element_type=jnp.float32
    )
    first = lax.axis_index("ctx") * query.shape[0]
    mine = lax.dynamic_slice_in_dim(from_pair, first, query.shape[0], 0) + from_query
    grad_normed = scatter_group(lax.dynamic_update_slice_in_dim(from_pair, mine, first, 0))
    step, grad_shift, grad_scale = jax.vjp(modulate, hidden, shift, scale)[1](grad_normed)
    grads = jnp.concatenate([grad_wq, grad_kv, grad_out], 1).astype(jnp.bfloat16)
    return grad_hidden + step, grads, jnp.concatenate([grad_shift, grad_scale, grad_gate], 0)


def silu_grad(values):
    gate = jax.nn.sigmoid(values)
    return gate * (1.0 + values * (1.0 - gate))


def local(
    noised,
    velocity,
    labels,
    time_ids,
    stem,
    stem_mean,
    stem_square,
    modulation,
    modulation_mean,
    modulation_square,
    attention_in,
    attention_in_mean,
    attention_in_square,
    attention_out,
    attention_out_mean,
    attention_out_square,
    feedforward,
    feedforward_mean,
    feedforward_square,
):
    tensor_ways = lax.axis_size("tp")
    shard_ways = lax.axis_size("shard")
    own_latent = lax.axis_index("shard")
    own_ctx = lax.axis_index("ctx")
    owned = stem.shape[1]
    first_owned = (own_latent * tensor_ways + lax.axis_index("tp")) * owned

    def own_columns(values):
        return lax.dynamic_slice_in_dim(values, first_owned, owned, values.ndim - 1)

    stem_low = stem.astype(jnp.bfloat16)
    class_own, time_in_own, time_out_own, shift_own, scale_own, patch_own, head_own = split_stem(
        stem_low
    )
    modulation_low = modulation.astype(jnp.bfloat16)
    packed_ids = lax.all_gather(
        jnp.stack([labels, time_ids], 1), "shard", axis=0, tiled=True
    )
    all_labels, all_times = packed_ids[:, 0], packed_ids[:, 1]
    latents = all_labels.shape[0]
    features = time_features(all_times).astype(jnp.bfloat16)
    time_pre = jnp.dot(features, time_in_own, preferred_element_type=jnp.float32)
    time_hidden_own = jax.nn.silu(time_pre).astype(jnp.bfloat16)
    packed = lax.all_gather(
        jnp.concatenate([time_hidden_own, patch_own, head_own], 0), OWNERS, axis=1, tiled=True
    )
    time_hidden = packed[:latents]
    patch_in, head_rows = packed[latents : latents + PDIM], packed[latents + PDIM :]
    onehot = (all_labels[:, None] == jnp.arange(CLASSES)[None, :]).astype(jnp.bfloat16)
    condition = jnp.dot(time_hidden, time_out_own, preferred_element_type=jnp.float32) + jnp.dot(
        onehot, class_own, preferred_element_type=jnp.float32
    )
    gated_own = jax.nn.silu(condition).astype(jnp.bfloat16)
    mod_part = jnp.einsum(
        "bd,lde->ble", gated_own, modulation_low, preferred_element_type=jnp.float32
    )
    layer_mods = lax.psum(
        lax.psum_scatter(mod_part, "shard", scatter_dimension=0, tiled=True), "tp"
    )[0].reshape(LAYERS, 6, D)
    gated = lax.all_gather(gated_own, OWNERS, axis=1, tiled=True)
    end_own = jnp.stack(
        [
            jnp.dot(gated, shift_own, preferred_element_type=jnp.float32),
            jnp.dot(gated, scale_own, preferred_element_type=jnp.float32),
        ],
        1,
    )
    end_all = lax.all_gather(end_own, OWNERS, axis=2, tiled=True)
    end_mods = lax.dynamic_index_in_dim(end_all, own_latent, 0, keepdims=False)
    end_shift, end_scale = end_mods[0:1], end_mods[1:2]

    hidden_half = feedforward.shape[3] // lax.axis_size("ctx")
    feed_low = lax.dynamic_slice_in_dim(feedforward, own_ctx * hidden_half, hidden_half, 3).astype(
        jnp.bfloat16
    )
    in_low, out_low = attention_in.astype(jnp.bfloat16), attention_out.astype(jnp.bfloat16)
    attention_blocks, feed_blocks = [], []
    for layer_at in range(LAYERS):
        block = jnp.concatenate([in_low[layer_at, number] for number in range(3)] + [out_low[layer_at]], 1)
        attention_blocks.append(lax.all_gather(block, "shard", axis=0, tiled=True))
        block = jnp.concatenate([feed_low[layer_at, 0], feed_low[layer_at, 1]], 1)
        feed_blocks.append(lax.all_gather(block, "shard", axis=0, tiled=True))

    pieces = patchify(noised)[0]
    rows_here = noised.shape[2] // PATCH
    first_row = (own_ctx * tensor_ways + lax.axis_index("tp")) * rows_here
    embedded = jnp.dot(pieces, patch_in, preferred_element_type=jnp.float32)
    hidden = embedded + positions(first_row, rows_here, noised.shape[3] // PATCH, D)
    kept_attention, kept_feed = [], []
    for layer_at in range(LAYERS):
        hidden, kept = attention_forward(hidden, layer_mods[layer_at], attention_blocks[layer_at])
        kept_attention.append(kept)
        hidden, kept = feed_forward(hidden, layer_mods[layer_at], feed_blocks[layer_at])
        kept_feed.append(kept)

    final_normed = modulate(hidden, end_shift, end_scale).astype(jnp.bfloat16)
    predicted = jnp.einsum(
        "pd,cd->pc", final_normed, head_rows, preferred_element_type=jnp.float32
    )
    target_rows = patchify(velocity)[0].astype(jnp.float32)
    weighting = 0.5 + time_ids.astype(jnp.float32)[0] / STEPS
    misfit = predicted - target_rows
    loss_scale = 1.0 / (shard_ways * PATCHES * PDIM)
    loss_local = jnp.sum(weighting * misfit * misfit) * loss_scale
    grad_pred = (2.0 * loss_scale * weighting * misfit).astype(jnp.bfloat16)
    grad_head = jnp.einsum("pc,pd->cd", grad_pred, final_normed, preferred_element_type=jnp.float32)
    grad_normed = jnp.dot(grad_pred, head_rows, preferred_element_type=jnp.float32)
    grad_hidden, grad_end_shift, grad_end_scale = jax.vjp(modulate, hidden, end_shift, end_scale)[
        1
    ](grad_normed)

    small = []
    shard_attention, shard_feed = [None] * LAYERS, [None] * LAYERS
    for layer_at in reversed(range(LAYERS)):
        grad_hidden, grads, small_two = feed_backward(
            grad_hidden, layer_mods[layer_at], feed_blocks[layer_at], kept_feed[layer_at]
        )
        shard_feed[layer_at] = lax.psum_scatter(grads, "shard", scatter_dimension=0, tiled=True)
        grad_hidden, grads, small_one = attention_backward(
            grad_hidden, layer_mods[layer_at], attention_blocks[layer_at], kept_attention[layer_at]
        )
        shard_attention[layer_at] = lax.psum_scatter(
            grads, "shard", scatter_dimension=0, tiled=True
        )
        small.append(jnp.concatenate([small_one, small_two], 0))
    grad_embed = grad_hidden.astype(jnp.bfloat16)
    grad_patch = jnp.einsum("pf,pd->fd", pieces, grad_embed, preferred_element_type=jnp.float32)

    small = jnp.concatenate(small[::-1] + [grad_end_shift, grad_end_scale], 0)
    small = lax.all_gather(lax.psum(small, GROUP), "shard", axis=0, tiled=False)
    grad_mod = small[:, : 6 * LAYERS].reshape(latents, LAYERS, 6 * D)
    grad_ends = small[:, 6 * LAYERS :]
    ends_here = own_columns(grad_ends)
    gated_part = jnp.dot(
        ends_here[:, 0], shift_own.astype(jnp.float32).T, precision=highest
    ) + jnp.dot(ends_here[:, 1], scale_own.astype(jnp.float32).T, precision=highest)
    grad_gated = lax.psum_scatter(
        gated_part, OWNERS, scatter_dimension=1, tiled=True
    ) + jnp.einsum(
        "ble,lde->bd", grad_mod, modulation_low.astype(jnp.float32), precision=highest
    )
    grad_condition = grad_gated * silu_grad(condition)
    grad_time_hidden = lax.psum_scatter(
        jnp.dot(grad_condition, time_out_own.astype(jnp.float32).T, precision=highest),
        OWNERS,
        scatter_dimension=1,
        tiled=True,
    )
    grad_time_pre = grad_time_hidden * silu_grad(time_pre)
    gated_wide = gated.astype(jnp.float32)
    grad_ends_own = lax.psum(
        lax.psum_scatter(
            jnp.concatenate([grad_patch, grad_head], 0), OWNERS, scatter_dimension=1, tiled=True
        ),
        "ctx",
    )
    shard_stem = jnp.concatenate(
        [
            jnp.dot(onehot.astype(jnp.float32).T, grad_condition, precision=highest),
            jnp.dot(features.astype(jnp.float32).T, grad_time_pre, precision=highest),
            jnp.dot(time_hidden.astype(jnp.float32).T, grad_condition, precision=highest),
            jnp.dot(gated_wide.T, ends_here[:, 0], precision=highest),
            jnp.dot(gated_wide.T, ends_here[:, 1], precision=highest),
            grad_ends_own,
        ],
        0,
    )
    shard_modulation = jnp.einsum(
        "bd,ble->lde", gated_own.astype(jnp.float32), grad_mod, precision=highest
    )
    shard_attention = lax.psum(jnp.stack(shard_attention), "ctx").astype(jnp.float32)
    cut = attention_in.shape[3]
    shard_in = jnp.stack(
        [shard_attention[:, :, number * cut : (number + 1) * cut] for number in range(3)], 1
    )
    shard_out = shard_attention[:, :, 3 * cut :]
    shard_hidden = jnp.stack(shard_feed).reshape(LAYERS, -1, 2, hidden_half).transpose(0, 2, 1, 3)
    shard_hidden = lax.all_gather(shard_hidden, "ctx", axis=3, tiled=True).astype(jnp.float32)
    squares = (
        jnp.sum(shard_stem * shard_stem)
        + jnp.sum(shard_modulation * shard_modulation)
        + jnp.sum(shard_in * shard_in)
        + jnp.sum(shard_out * shard_out)
        + jnp.sum(shard_hidden * shard_hidden)
    )
    squares = jnp.where(own_ctx == 0, squares, jnp.zeros((), jnp.float32))
    sums = lax.psum(jnp.stack([squares, loss_local]), EVERY)
    square_total, train_loss = sums[0], sums[1]
    total_norm = jnp.sqrt(square_total)
    factor = clip_level / jnp.maximum(total_norm, clip_level)
    stem_out = adam_update(stem, stem_mean, stem_square, shard_stem, factor)
    mod_out = adam_update(modulation, modulation_mean, modulation_square, shard_modulation, factor)
    in_out = adam_update(attention_in, attention_in_mean, attention_in_square, shard_in, factor)
    proj_out = adam_update(
        attention_out, attention_out_mean, attention_out_square, shard_out, factor
    )
    feed_out = adam_update(feedforward, feedforward_mean, feedforward_square, shard_hidden, factor)
    return (
        train_loss,
        total_norm,
        stem_out[0],
        stem_out[1],
        stem_out[2],
        stem_out[3],
        mod_out[0],
        mod_out[1],
        mod_out[2],
        mod_out[3],
        in_out[0],
        in_out[1],
        in_out[2],
        in_out[3],
        proj_out[0],
        proj_out[1],
        proj_out[2],
        proj_out[3],
        feed_out[0],
        feed_out[1],
        feed_out[2],
        feed_out[3],
    )


def solution(mesh):
    placed = (
        P("shard", None, ("ctx", "tp"), None),
        P("shard", None, ("ctx", "tp"), None),
        P("shard"),
        P("shard"),
        P(None, ("shard", "tp")),
        P(None, ("shard", "tp")),
        P(None, ("shard", "tp")),
        P(None, ("shard", "tp"), None),
        P(None, ("shard", "tp"), None),
        P(None, ("shard", "tp"), None),
        P(None, None, "shard", "tp"),
        P(None, None, "shard", "tp"),
        P(None, None, "shard", "tp"),
        P(None, "shard", "tp"),
        P(None, "shard", "tp"),
        P(None, "shard", "tp"),
        P(None, None, "shard", "tp"),
        P(None, None, "shard", "tp"),
        P(None, None, "shard", "tp"),
    )
    return jax.shard_map(
        local,
        mesh=mesh,
        in_specs=placed,
        out_specs=(
            P(),
            P(),
            P(None, ("shard", "tp")),
            P(None, ("shard", "tp")),
            P(None, ("shard", "tp")),
            P(None, ("shard", "tp")),
            P(None, ("shard", "tp"), None),
            P(None, ("shard", "tp"), None),
            P(None, ("shard", "tp"), None),
            P(None, ("shard", "tp"), None),
            P(None, None, "shard", "tp"),
            P(None, None, "shard", "tp"),
            P(None, None, "shard", "tp"),
            P(None, None, "shard", "tp"),
            P(None, "shard", "tp"),
            P(None, "shard", "tp"),
            P(None, "shard", "tp"),
            P(None, "shard", "tp"),
            P(None, None, "shard", "tp"),
            P(None, None, "shard", "tp"),
            P(None, None, "shard", "tp"),
            P(None, None, "shard", "tp"),
        ),
        check_vma=False,
    )
```

```python
import functools
import math

import jax
import jax.numpy as jnp
from jax import lax
from jax.experimental import pallas as pl
from jax.experimental.pallas import tpu as pltpu
from jax.sharding import PartitionSpec as P

D = 768
HEAD_DIM = 64
CLASSES = 1000
FREQ = 256
PATCH = 2
STEPS = 1000
LAYERS = 4
PATCHES = 1024
PDIM = 16


norm_eps = 1e-06
clip_level = 0.5
learn_rate = 0.01
beta_first = 0.5
beta_second = 0.5
adam_eps = 1e-08
weight_decay = 0.1
bias_fix = 0.875
highest = lax.Precision.HIGHEST


def layer_norm(values):
    centre = values - jnp.mean(values, -1, keepdims=True)
    spread = jnp.mean(centre * centre, -1, keepdims=True)
    return centre * lax.rsqrt(spread + norm_eps)


def modulate(values, shift_rows, scale_rows):
    return layer_norm(values) * (1.0 + scale_rows) + shift_rows


def gelu_tanh(values):
    return jax.nn.gelu(values, approximate=True)


def patchify(image_in):
    latent_count, channels, height, columns = image_in.shape
    shaped = image_in.reshape(
        latent_count, channels, height // PATCH, PATCH, columns // PATCH, PATCH
    )
    shaped = shaped.transpose(0, 2, 4, 3, 5, 1)
    return shaped.reshape(
        latent_count, height // PATCH * (columns // PATCH), PATCH * PATCH * channels
    )


def positions(first_row, height, columns, model_width):
    quarter = model_width // 4
    omegas = jnp.exp(-math.log(10000.0) * jnp.arange(quarter).astype(jnp.float32) / quarter)
    row_angle = (first_row + jnp.arange(height)).astype(jnp.float32)[:, None] * omegas[None, :]
    col_angle = jnp.arange(columns).astype(jnp.float32)[:, None] * omegas[None, :]
    row_part = jnp.concatenate([jnp.sin(row_angle), jnp.cos(row_angle)], -1)
    col_part = jnp.concatenate([jnp.sin(col_angle), jnp.cos(col_angle)], -1)
    grid_table = jnp.concatenate(
        [
            jnp.broadcast_to(col_part[None], (height, columns, 2 * quarter)),
            jnp.broadcast_to(row_part[:, None], (height, columns, 2 * quarter)),
        ],
        -1,
    )
    return grid_table.reshape(height * columns, model_width)


def time_features(step_ids):
    half_width = FREQ // 2
    frequencies = jnp.exp(
        -math.log(10000.0) * jnp.arange(half_width).astype(jnp.float32) / half_width
    )
    angles = step_ids.astype(jnp.float32)[:, None] * frequencies[None, :]
    return jnp.concatenate([jnp.cos(angles), jnp.sin(angles)], -1)


def split_stem(stem_rows):
    bounds = [CLASSES, FREQ, D, D, D, PDIM, PDIM]
    pieces_out = []
    offset = 0
    for extent in bounds:
        pieces_out.append(stem_rows[offset : offset + extent])
        offset = offset + extent
    return pieces_out


def adam_update(master, first_moment, second_moment, gradient, factor):
    clipped = gradient * factor
    first_new = beta_first * first_moment + (1.0 - beta_first) * clipped
    second_new = beta_second * second_moment + (1.0 - beta_second) * clipped * clipped
    direction = first_new / bias_fix / (jnp.sqrt(second_new / bias_fix) + adam_eps)
    master_new = master - learn_rate * (direction + weight_decay * master)
    return (master_new, first_new, second_new, master_new.astype(jnp.bfloat16))


GROUP = ("ctx", "tp")
OWNERS = ("shard", "tp")
EVERY = ("shard", "ctx", "tp")
HOP_WAYS = 8


MESH = pl.DeviceIdType.MESH
BF = jnp.bfloat16
F32 = jnp.float32
SCORE_SCALE = HEAD_DIM**-0.5


def place():
    ctx, tp = lax.axis_index("ctx"), lax.axis_index("tp")
    core = tp % 2
    row = tp // 2
    return ctx, row, core


def square(ctx, row, core):
    return ctx * 4 + row * 2 + core


def remote(index, src, dst, send, recv, **where):
    return pltpu.make_async_remote_copy(
        src_ref=src,
        dst_ref=dst,
        send_sem=send.at[index],
        recv_sem=recv.at[index],
        device_id=where,
        device_id_type=MESH,
    )


def greet_signal(shard_ways):
    ctx, row, core = place()
    barrier = pltpu.get_barrier_semaphore()
    tp = row * 2 + core
    pl.semaphore_signal(barrier, inc=1, device_id={"ctx": 1 - ctx}, device_id_type=MESH)
    pl.semaphore_signal(barrier, inc=1, device_id={"tp": (tp + 2) % 4}, device_id_type=MESH)
    pl.semaphore_signal(
        barrier, inc=1, device_id={"tp": row * 2 + 1 - core}, device_id_type=MESH
    )
    if shard_ways == 1:
        return
    at = lax.axis_index("shard")

    @pl.when(at > 0)
    def _():
        pl.semaphore_signal(barrier, inc=1, device_id={"shard": at - 1}, device_id_type=MESH)

    @pl.when(at < shard_ways - 1)
    def _():
        pl.semaphore_signal(barrier, inc=1, device_id={"shard": at + 1}, device_id_type=MESH)


def greet_wait(shard_ways):
    barrier = pltpu.get_barrier_semaphore()
    if shard_ways == 1:
        pl.semaphore_wait(barrier, 3)
        return
    at = lax.axis_index("shard")

    @pl.when((at > 0) & (at < shard_ways - 1))
    def _():
        pl.semaphore_wait(barrier, 5)

    @pl.when((at == 0) | (at == shard_ways - 1))
    def _():
        pl.semaphore_wait(barrier, 4)


GATHER_COPIES = 13


class GroupGather:
    def __init__(self, buf, send, recv):
        ctx, row, core = place()
        half = buf.shape[1] // 2
        tp = row * 2 + core
        across, along = {"ctx": 1 - ctx}, {"tp": (tp + 2) % 4}
        beside = {"tp": row * 2 + 1 - core}
        own = square(ctx, row, core)
        self.by_x, self.by_y = square(1 - ctx, row, core), square(ctx, 1 - row, core)
        self.far = square(1 - ctx, 1 - row, core)

        def piece(block, which):
            if which is None:
                return buf.at[block]
            return buf.at[block, pl.ds(which * half, half)]

        def make(index, block, which, where):
            return remote(index, piece(block, which), piece(block, which), send, recv, **where)

        self.first = [
            make(0, own, 0, across),
            make(1, own, 1, along),
            make(2, own, None, beside),
            make(3, own, 1, across),
            make(4, own, 0, along),
        ]
        self.second = [
            (0, make(5, self.by_x, 0, along)),
            (0, make(6, self.by_x, 0, beside)),
            (1, make(7, self.by_y, 1, across)),
            (1, make(8, self.by_y, 1, beside)),
            (3, make(9, self.by_x, 1, beside)),
            (4, make(10, self.by_y, 0, beside)),
        ]
        self.third = [
            (5, make(11, self.far, 0, beside)),
            (7, make(12, self.far, 1, beside)),
        ]
        self.all = self.first + [c for _, c in self.second] + [c for _, c in self.third]

    def start(self):
        for copy in self.first:
            copy.start()

    def relay(self):
        waited = set()
        for needs, copy in self.second:
            if needs not in waited:
                self.all[needs].wait_recv()
                waited.add(needs)
            copy.start()

    def relay_far(self):
        for needs, copy in self.third:
            self.all[needs].wait_recv()
            copy.start()

    def wait_chip(self, which):
        for index in {"own": (2,), "x": (6, 9), "y": (8, 10), "far": (11, 12)}[which]:
            self.all[index].wait_recv()

    def finish(self):
        for copy in self.all:
            copy.wait_send()


SCATTER_COPIES = 10


class GroupScatter:
    def __init__(self, part, beside_in, summed, turn_in, send, recv, base):
        ctx, row, core = place()
        half = part.shape[1] // 2
        tp = row * 2 + core
        across, along = {"ctx": 1 - ctx}, {"tp": (tp + 2) % 4}
        beside = {"tp": row * 2 + 1 - core}
        self.part, self.beside_in, self.summed, self.turn_in = part, beside_in, summed, turn_in
        self.core, self.half = core, half
        self.chips = {
            "far": (1 - ctx, 1 - row),
            "x": (1 - ctx, row),
            "y": (ctx, 1 - row),
            "own": (ctx, row),
        }
        self.slot = {name: a * 2 + b for name, (a, b) in self.chips.items()}
        self.order = ["far", "x", "y", "own"]
        self.pair = {}
        for number, name in enumerate(self.order):
            a, b = self.chips[name]
            self.pair[name] = remote(
                base + number,
                part.at[square(a, b, 1 - core)],
                beside_in.at[self.slot[name]],
                send,
                recv,
                **beside,
            )

        def turn(index, name, which, place_at, where):
            return remote(
                base + index,
                summed.at[self.slot[name], pl.ds(which * half, half)],
                turn_in.at[place_at],
                send,
                recv,
                **where,
            )

        self.far_x = turn(4, "far", 0, 0, across)
        self.far_y = turn(5, "far", 1, 1, along)
        self.near_x = turn(6, "x", 0, 2, across)
        self.near_y = turn(7, "y", 1, 3, along)
        self.last_y = turn(8, "y", 0, 4, along)
        self.last_x = turn(9, "x", 1, 5, across)
        self.all = list(self.pair.values()) + [
            self.far_x,
            self.far_y,
            self.near_x,
            self.near_y,
            self.last_y,
            self.last_x,
        ]

    def send_pair(self, name):
        self.pair[name].start()

    def add_pair(self, name):
        self.pair[name].wait_recv()
        a, b = self.chips[name]
        mine = self.part[square(a, b, self.core)].astype(F32)
        slot = self.slot[name]
        self.summed[slot] = (mine + self.beside_in[slot].astype(F32)).astype(BF)
        if name == "far":
            self.far_x.start()
            self.far_y.start()
        if name == "x":
            self.near_x.start()
        if name == "y":
            self.near_y.start()

    def turn_corner(self):
        half = self.half
        low, high = pl.ds(0, half), pl.ds(half, half)
        self.far_x.wait_recv()
        slot = self.slot["y"]
        kept = self.summed[slot, low].astype(F32) + self.turn_in[0].astype(F32)
        self.summed[slot, low] = kept.astype(BF)
        self.last_y.start()
        self.far_y.wait_recv()
        slot = self.slot["x"]
        kept = self.summed[slot, high].astype(F32) + self.turn_in[1].astype(F32)
        self.summed[slot, high] = kept.astype(BF)
        self.last_x.start()

    def total(self):
        half = self.half
        slot = self.slot["own"]
        for copy in (self.near_x, self.near_y, self.last_y, self.last_x):
            copy.wait_recv()
        low = (
            self.summed[slot, pl.ds(0, half)].astype(F32)
            + self.turn_in[2].astype(F32)
            + self.turn_in[4].astype(F32)
        )
        high = (
            self.summed[slot, pl.ds(half, half)].astype(F32)
            + self.turn_in[3].astype(F32)
            + self.turn_in[5].astype(F32)
        )
        return jnp.concatenate([low, high], 0)

    def finish(self):
        for copy in self.all:
            copy.wait_send()


class LineGather:
    def __init__(self, ways, src, buf, local_sem, send, recv, base):
        self.ways, self.at = ways, lax.axis_index("shard")
        at = self.at
        rows = src.shape[0]
        self.own = pltpu.make_async_copy(src, buf.at[pl.ds(at * rows, rows)], local_sem)

        def hop(index, block, first, to):
            target = buf.at[pl.ds(block * rows, rows)]
            return remote(index, src if first else target, target, send, recv, shard=to)

        def clip(v):
            return jnp.clip(v, 0, ways - 1)

        steps = ways - 1
        self.right = [
            hop(base + k - 1, clip(at - k + 1), k == 1, clip(at + 1)) for k in range(1, ways)
        ]
        self.left = [
            hop(base + steps + k - 1, clip(at + k - 1), k == 1, clip(at - 1))
            for k in range(1, ways)
        ]

    def start(self):
        self.own.start()
        self.step(1)

    def step(self, k):
        at, ways = self.at, self.ways
        if k > 1:
            pl.when(at >= k - 1)(self.right[k - 2].wait_recv)
        pl.when((at < ways - 1) & (at >= k - 1))(self.right[k - 1].start)
        if k > 1:
            pl.when(at <= ways - k)(self.left[k - 2].wait_recv)
        pl.when((at > 0) & (at <= ways - k))(self.left[k - 1].start)

    def finish(self):
        at, ways = self.at, self.ways
        last = ways - 1
        pl.when(at >= last)(self.right[last - 1].wait_recv)
        pl.when(at <= 0)(self.left[last - 1].wait_recv)
        for k in range(1, ways):
            pl.when((at < ways - 1) & (at >= k - 1))(self.right[k - 1].wait_send)
            pl.when((at > 0) & (at <= ways - k))(self.left[k - 1].wait_send)
        self.own.wait()


def norm_rows(values):
    centre = values - jnp.mean(values, -1, keepdims=True)
    spread = jnp.mean(centre * centre, -1, keepdims=True)
    return centre, lax.rsqrt(spread + norm_eps)


def dot(left, right):
    return lax.dot_general(left, right, (((1,), (0,)), ((), ())), preferred_element_type=F32)


def dot_wide(left, right):
    return lax.dot_general(left, right, (((1,), (1,)), ((), ())), preferred_element_type=F32)


def dot_tall(left, right):
    return lax.dot_general(left, right, (((0,), (0,)), ((), ())), preferred_element_type=F32)


def gelu_parts(values):
    inner = math.sqrt(2.0 / math.pi) * (values + 0.044715 * (values * values * values))
    return jnp.tanh(inner)


def feed_forward_kernel(
    ways,
    gate,
    ready,
    hidden_ref,
    mods_ref,
    weights_hbm,
    *rest,
):
    if ways > 1:
        next_src, *rest = rest
    hidden_out, branch_out, normed_hbm, pre_hbm, *rest = rest
    if ways > 1:
        next_hbm, *rest = rest
    weights, gathered, pre, part, beside_in, summed, turn_in, *rest = rest
    if ways > 1:
        next_buf, *rest = rest
    local, send, recv = rest
    rows = hidden_ref.shape[0]
    if gate is not None:
        greet_signal(gate)
    if not ready:
        load = pltpu.make_async_copy(weights_hbm, weights, local.at[0])
        load.start()
    centre, scale_by = norm_rows(hidden_ref[...])
    normed = centre * scale_by * (1.0 + mods_ref[4:5, :]) + mods_ref[3:4, :]
    ctx, row, core = place()
    gathered[square(ctx, row, core)] = normed.astype(BF)
    gather = GroupGather(gathered, send, recv)
    scatter = GroupScatter(part, beside_in, summed, turn_in, send, recv, GATHER_COPIES)
    if gate is not None:
        greet_wait(gate)
    gather.start()
    if ways > 1:
        line = LineGather(
            ways, next_src, next_buf, local.at[3], send, recv, GATHER_COPIES + SCATTER_COPIES
        )
        line.start()
    if not ready:
        load.wait()
    width = pre.shape[-1]

    def up(name):
        a, b = scatter.chips[name]
        first = square(a, b, 0)
        rows_here = gathered[pl.ds(first, 2)].reshape(2 * rows, gathered.shape[2])
        value = dot(rows_here, weights[:, :width])
        pre[pl.ds(first, 2)] = value.reshape(2, rows, width)

    def down(name):
        a, b = scatter.chips[name]
        first = square(a, b, 0)
        value = pre[pl.ds(first, 2)].reshape(2 * rows, width)
        act = (0.5 * value * (1.0 + gelu_parts(value))).astype(BF)
        out = dot_wide(act, weights[:, width:]).astype(BF)
        part[pl.ds(first, 2)] = out.reshape(2, rows, out.shape[1])

    gather.wait_chip("own")
    up("own")
    gather.relay()
    gather.wait_chip("x")
    up("x")
    gather.wait_chip("y")
    up("y")
    if ways > 1:
        line.step(2)
    gather.relay_far()
    gather.wait_chip("far")
    keep_normed = pltpu.make_async_copy(gathered, normed_hbm, local.at[1])
    keep_normed.start()
    up("far")
    keep_pre = pltpu.make_async_copy(pre, pre_hbm, local.at[2])
    keep_pre.start()
    down("far")
    scatter.send_pair("far")
    down("x")
    scatter.send_pair("x")
    scatter.add_pair("far")
    down("y")
    scatter.send_pair("y")
    scatter.add_pair("x")
    down("own")
    scatter.send_pair("own")
    scatter.add_pair("y")
    scatter.add_pair("own")
    if ways > 1:
        for k in range(3, ways):
            line.step(k)
    scatter.turn_corner()
    branch = scatter.total()
    branch_out[...] = branch
    hidden_out[...] = hidden_ref[...] + mods_ref[5:6, :] * branch
    gather.finish()
    scatter.finish()
    keep_normed.wait()
    keep_pre.wait()
    if ways > 1:
        line.finish()
        keep_next = pltpu.make_async_copy(next_buf, next_hbm, local.at[0])
        keep_next.start()
        keep_next.wait()


ANY = pl.BlockSpec(memory_space=pl.ANY)
VMEM = pl.BlockSpec(memory_space=pltpu.VMEM)


def line_copies(ways):
    return 2 * (ways - 1) if ways > 1 else 0


def sds(shape, dtype):
    return jax.ShapeDtypeStruct(shape, dtype)


PAIR_COPIES = 3


class RowScatter:
    def __init__(self, part, beside_in, summed, turn_in, send, recv, base):
        ctx, row, core = place()
        tp = row * 2 + core
        beside = {"tp": row * 2 + 1 - core}
        self.part, self.beside_in, self.summed, self.turn_in = part, beside_in, summed, turn_in
        self.core = core
        self.chip = {"y": 1 - row, "own": row}
        self.pair = {}
        for number, name in enumerate(("y", "own")):
            self.pair[name] = remote(
                base + number,
                part.at[self.chip[name] * 2 + 1 - core],
                beside_in.at[number],
                send,
                recv,
                **beside,
            )
        self.turn = remote(base + 2, summed, turn_in, send, recv, tp=(tp + 2) % 4)
        self.all = list(self.pair.values()) + [self.turn]

    def send_pair(self, name):
        self.pair[name].start()

    def add_pair(self, name):
        number = 0 if name == "y" else 1
        self.pair[name].wait_recv()
        mine = self.part[self.chip[name] * 2 + self.core].astype(F32)
        return mine + self.beside_in[number].astype(F32)

    def send_far(self):
        self.summed[...] = self.add_pair("y").astype(BF)
        self.turn.start()

    def total(self):
        own = self.add_pair("own")
        self.turn.wait_recv()
        return own + self.turn_in[...].astype(F32)

    def finish(self):
        for copy in self.all:
            copy.wait_send()


def attention_forward_kernel(ways, gate, hidden_ref, mods_ref, weights_hbm, *rest):
    if ways > 1:
        next_src, *rest = rest
    hidden_out, branch_out, normed_hbm, q_hbm, k_hbm, v_hbm, lse_hbm, mixed_hbm, *rest = rest
    if ways > 1:
        next_hbm, *rest = rest
    weights, gathered, q, k, v, lse, mixed, part, beside_in, summed, turn_in, *rest = rest
    if ways > 1:
        next_buf, *rest = rest
    local, send, recv = rest
    rows, model = hidden_ref.shape
    heads = q.shape[0]
    cut = heads * HEAD_DIM
    greet_signal(gate)
    load = pltpu.make_async_copy(weights_hbm, weights, local.at[0])
    load.start()
    centre, scale_by = norm_rows(hidden_ref[...])
    normed = centre * scale_by * (1.0 + mods_ref[1:2, :]) + mods_ref[0:1, :]
    ctx, row, core = place()
    gathered[square(ctx, row, core)] = normed.astype(BF)
    gather = GroupGather(gathered, send, recv)
    scatter = RowScatter(part, beside_in, summed, turn_in, send, recv, GATHER_COPIES)
    greet_wait(gate)
    gather.start()
    if ways > 1:
        line = LineGather(
            ways, next_src, next_buf, local.at[8], send, recv, GATHER_COPIES + PAIR_COPIES
        )
        line.start()
    load.wait()
    chips = {
        "own": (ctx, row),
        "x": (1 - ctx, row),
        "y": (ctx, 1 - row),
        "far": (1 - ctx, 1 - row),
    }

    def project(name):
        a, b = chips[name]
        first = square(a, b, 0)
        here = gathered[pl.ds(first, 2)].reshape(2 * rows, model)
        span = pl.ds(pl.multiple_of(first * rows, 2 * rows), 2 * rows)
        pair = dot(here, weights[:, 2 * cut :]).astype(BF)
        for head in range(heads):
            k[head, span] = pair[:, head * HEAD_DIM : (head + 1) * HEAD_DIM]
            v[head, span] = pair[:, cut + head * HEAD_DIM : cut + (head + 1) * HEAD_DIM]
        if name in ("own", "y"):
            query = (dot(here, weights[:, :cut]) * SCORE_SCALE).astype(BF)
            span = pl.ds(pl.multiple_of(b * 2 * rows, 2 * rows), 2 * rows)
            for head in range(heads):
                q[head, span] = query[:, head * HEAD_DIM : (head + 1) * HEAD_DIM]

    gather.wait_chip("own")
    project("own")
    gather.relay()
    gather.wait_chip("x")
    project("x")
    gather.wait_chip("y")
    project("y")
    if ways > 1:
        line.step(2)
    gather.relay_far()
    gather.wait_chip("far")
    keep = [pltpu.make_async_copy(gathered, normed_hbm, local.at[1])]
    keep[0].start()
    project("far")
    for number, (src, dst) in enumerate(((q, q_hbm), (k, k_hbm), (v, v_hbm))):
        keep.append(pltpu.make_async_copy(src, dst, local.at[2 + number]))
        keep[-1].start()

    def attend(name):
        b = chips[name][1]
        for head in range(heads):
            @pl.loop(0, 2)
            def _(step):
                at = b * 2 + step
                span = pl.ds(pl.multiple_of(at * rows, rows), rows)
                scores = dot_wide(q[head, span], k[head])
                top = jnp.max(scores, -1, keepdims=True)
                exponent = jnp.exp(scores - top)
                total = jnp.sum(exponent, -1, keepdims=True)
                out = dot(exponent.astype(BF), v[head]) / total
                mixed[span, head * HEAD_DIM : (head + 1) * HEAD_DIM] = out.astype(BF)
                wide = jnp.broadcast_to(top + jnp.log(total), (rows, rows))
                lse[head, pl.ds(at, 1)] = wide.T[0:1]

        @pl.loop(0, 2)
        def _(step):
            at = b * 2 + step
            span = pl.ds(pl.multiple_of(at * rows, rows), rows)
            part[at] = dot_wide(mixed[span, :], weights[:, cut : 2 * cut]).astype(BF)

    attend("y")
    scatter.send_pair("y")
    if ways > 1:
        line.step(3)
    attend("own")
    scatter.send_pair("own")
    scatter.send_far()
    for number, (src, dst) in enumerate(((lse, lse_hbm), (mixed, mixed_hbm))):
        keep.append(pltpu.make_async_copy(src, dst, local.at[5 + number]))
        keep[-1].start()
    branch = scatter.total()
    branch_out[...] = branch
    hidden_out[...] = hidden_ref[...] + mods_ref[2:3, :] * branch
    gather.finish()
    scatter.finish()
    for copy in keep:
        copy.wait()
    if ways > 1:
        line.finish()
        keep_next = pltpu.make_async_copy(next_buf, next_hbm, local.at[0])
        keep_next.start()
        keep_next.wait()


def layer_forward_kernel(ways, last, *refs):
    hop, more = int(ways > 1), int(ways > 1 and not last)
    (
        (hidden, mods, weights),
        feed_weights,
        feed_own,
        ahead,
        outs,
        feed_block,
        feed_outs,
        ahead_block,
        scratch,
        feed_buf,
        sems,
        feed_scratch,
        ahead_buf,
        feed_sems,
    ) = split_refs(refs, 3, 1 - hop, hop, more, 8, hop, 4, more, 11, 1, 3, 6, more, 3)
    attention_forward_kernel(
        ways,
        ways,
        hidden,
        mods,
        weights,
        *feed_own,
        *outs,
        *feed_block,
        *scratch,
        *(feed_buf if hop else ()),
        *sems,
    )
    feed_forward_kernel(
        ways if more else 1,
        None,
        hop == 1,
        outs[0],
        mods,
        *(feed_weights or (None,)),
        *ahead,
        *feed_outs,
        *ahead_block,
        *feed_buf,
        *feed_scratch,
        *ahead_buf,
        *feed_sems,
    )


def layer_forward(hidden, mods, weights, feed_weights, feed_own, ahead, number):
    rows, model = hidden.shape
    cut = weights.shape[1] // 4
    heads = cut // HEAD_DIM
    ways = 1 if feed_own is None else lax.axis_size("shard")
    hop, last = ways > 1, ahead is None
    kept = [
        sds((8, rows, model), BF),
        sds((heads, 4 * rows, HEAD_DIM), BF),
        sds((heads, 8 * rows, HEAD_DIM), BF),
        sds((heads, 8 * rows, HEAD_DIM), BF),
        sds((heads, 4, rows), F32),
        sds((4 * rows, cut), BF),
    ]
    wide = sds(weights.shape, BF)
    width = weights.shape[1] // 2
    row_pair = [sds((rows, model), F32), sds((rows, model), F32)]
    feed_kept = [sds((8, rows, model), BF), sds((8, rows, width), F32)]
    outs = row_pair + kept + [wide] * hop + row_pair + feed_kept + [wide] * (hop and not last)
    out_specs = [VMEM, VMEM] + [ANY] * (len(kept) + hop)
    out_specs += [VMEM, VMEM] + [ANY] * (2 + (hop and not last))

    def buffers(copies, locals_used):
        return [
            pltpu.SemaphoreType.DMA((locals_used,)),
            pltpu.SemaphoreType.DMA((copies,)),
            pltpu.SemaphoreType.DMA((copies,)),
        ]

    scratch = [pltpu.VMEM(weights.shape, BF)]
    scratch += [pltpu.VMEM(leaf.shape, leaf.dtype) for leaf in kept]
    scratch += [
        pltpu.VMEM((4, rows, model), BF),
        pltpu.VMEM((2, rows, model), BF),
        pltpu.VMEM((rows, model), BF),
        pltpu.VMEM((rows, model), BF),
        pltpu.VMEM(weights.shape, BF),
    ]
    scratch += buffers(GATHER_COPIES + PAIR_COPIES + line_copies(ways), 9)
    scratch += [
        pltpu.VMEM((8, rows, model), BF),
        pltpu.VMEM((8, rows, width), F32),
        pltpu.VMEM((8, rows, model), BF),
        pltpu.VMEM((4, rows, model), BF),
        pltpu.VMEM((4, rows, model), BF),
        pltpu.VMEM((6, rows // 2, model), BF),
    ]
    if hop and not last:
        scratch.append(pltpu.VMEM(weights.shape, BF))
    scratch += buffers(GATHER_COPIES + SCATTER_COPIES + line_copies(ways), 4)
    given = [weights] + ([feed_own] if hop else [feed_weights]) + [ahead] * (hop and not last)
    result = pl.pallas_call(
        functools.partial(layer_forward_kernel, ways, last),
        out_shape=outs,
        in_specs=[VMEM, VMEM] + [ANY] * len(given),
        out_specs=out_specs,
        scratch_shapes=scratch,
        compiler_params=pltpu.CompilerParams(collective_id=number, has_side_effects=True),
        name="layer_forward",
    )(hidden, mods, *given)
    middle, branch, *rest = result
    saved, rest = rest[:6], rest[6:]
    if hop:
        feed_weights, rest = rest[0], rest[1:]
    hidden_new, feed_branch, normed, pre, *rest = rest
    kept_attention = (hidden, branch, *saved)
    kept_feed = (middle, normed, pre, feed_branch)
    return hidden_new, kept_attention, kept_feed, feed_weights, rest[0] if rest else None


class LineScatter:
    def __init__(self, ways, src, arrived, sums, total, send, recv, base):
        self.ways, self.at, self.src = ways, lax.axis_index("shard"), src
        self.arrived, self.sums, self.total = arrived, sums, total
        self.rows = total.shape[0]
        self.sem = send, recv, base
        at, steps = self.at, ways - 1
        self.sides = []
        for side in range(2):
            place_at = at if side == 0 else ways - 1 - at
            to = jnp.clip(at + 1 if side == 0 else at - 1, 0, ways - 1)
            first, summed = [], []
            for k in range(1, ways):
                index = side * steps + k - 1
                block = ways - k if side == 0 else k - 1
                first.append(self.hop(index, self.block(block), to))
                summed.append(self.hop(index, sums.at[index], to) if k > 1 else None)
            self.sides.append((place_at, first, summed))

    def block(self, number):
        return self.src.at[pl.ds(number * self.rows, self.rows)]

    def hop(self, index, src, to):
        send, recv, base = self.sem
        return pltpu.make_async_remote_copy(
            src_ref=src,
            dst_ref=self.arrived.at[index],
            send_sem=send.at[base + index],
            recv_sem=recv.at[base + index],
            device_id={"shard": to},
            device_id_type=MESH,
        )

    def step(self, k):
        ways, at = self.ways, self.at
        for side, (place_at, first, summed) in enumerate(self.sides):
            pl.when(place_at == 0)(first[k - 1].start)
            if k == 1:
                continue
            index = side * (ways - 1) + k - 1
            block = at + ways - k if side == 0 else at - ways + k

            @pl.when((place_at >= 1) & (place_at <= k - 1) & (place_at < ways - 1))
            def _():
                first[k - 2].wait_recv()
                mine = self.block(jnp.clip(block, 0, ways - 1))[...].astype(F32)
                self.sums[index] = (mine + self.arrived[index - 1].astype(F32)).astype(BF)
                summed[k - 1].start()

    def finish(self):
        ways, at = self.ways, self.at
        self.total[...] = self.block(at)[...].astype(F32)
        for side, (place_at, first, summed) in enumerate(self.sides):
            @pl.when(place_at >= 1)
            def _():
                first[ways - 2].wait_recv()
                index = side * (ways - 1) + ways - 2
                self.total[...] = self.total[...] + self.arrived[index].astype(F32)

            for k in range(1, ways):
                pl.when((place_at <= k - 1) & (place_at < ways - 1))(first[k - 1].wait_send)


class Extra:
    def __init__(self, ways, sums_src, swap_src, refs, local, first_local, send, recv, base):
        self.ways = ways
        self.sums_hbm, self.swap_hbm = sums_src, swap_src
        self.refs, self.local, self.at = refs, local, first_local
        self.ready = sums_src is not None and sums_src is refs["src"]
        if sums_src is not None and not self.ready:
            self.load = pltpu.make_async_copy(sums_src, refs["src"], local.at[first_local])
        if sums_src is not None:
            self.line = LineScatter(
                ways, refs["src"], refs["arrived"], refs["sums"], refs["total"], send, recv, base
            )
            base = base + 2 * (ways - 1)
        if swap_src is not None:
            ctx = lax.axis_index("ctx")
            self.swaps = [
                remote(base + number, src, refs["swap"].at[number], send, recv, ctx=1 - ctx)
                for number, src in enumerate(swap_src)
            ]

    def begin(self):
        if self.sums_hbm is not None and not self.ready:
            self.load.start()

    def start(self):
        if self.sums_hbm is not None:
            if not self.ready:
                self.load.wait()
            self.line.step(1)

    def start_swap(self):
        if self.swap_hbm is not None:
            for copy in self.swaps:
                copy.start()

    def step(self, k):
        if self.sums_hbm is not None and k < self.ways:
            self.line.step(k)

    def finish(self):
        keep = []
        if self.swap_hbm is not None:
            for number, copy in enumerate(self.swaps):
                copy.wait_recv()
                copy.wait_send()
            keep.append(
                pltpu.make_async_copy(
                    self.refs["swap"], self.refs["swap_out"], self.local.at[self.at + 1]
                )
            )
            keep[-1].start()
        if self.sums_hbm is not None:
            self.line.finish()
            self.refs["shard_out"][...] = self.refs["total"][...].astype(BF)
        for copy in keep:
            copy.wait()


def extra_shapes(ways, grads, swaps):
    given, outs, specs, scratch, copies = [], [], [], [], 0
    if grads is not None:
        rows, width = grads.shape[0] // ways, grads.shape[1]
        given.append(grads)
        outs.append(sds((rows, width), BF))
        specs.append(VMEM)
        scratch += [
            pltpu.VMEM(grads.shape, BF),
            pltpu.VMEM((2 * (ways - 1), rows, width), BF),
            pltpu.VMEM((2 * (ways - 1), rows, width), BF),
            pltpu.VMEM((rows, width), F32),
        ]
        copies += 2 * (ways - 1)
    if swaps:
        given += list(swaps)
        shape = (len(swaps), *swaps[0].shape)
        outs.append(sds(shape, BF))
        specs.append(ANY)
        scratch.append(pltpu.VMEM(shape, BF))
        copies += len(swaps)
    return given, outs, specs, scratch, copies


def take_extra(has_sums, swaps, ins, outs, scratch):
    refs = {}
    ins, outs, scratch = list(ins), list(outs), list(scratch)
    sums_src = swap_src = None
    if has_sums:
        sums_src = ins.pop(0)
        refs["shard_out"] = outs.pop(0)
        for name in ("src", "arrived", "sums", "total"):
            refs[name] = scratch.pop(0)
    if swaps:
        swap_src = [ins.pop(0) for _ in range(swaps)]
        refs["swap_out"] = outs.pop(0)
        refs["swap"] = scratch.pop(0)
    return sums_src, swap_src, refs


def modulate_backward(grad, hidden, scale, step_ref, small_ref):
    centre, scale_by = norm_rows(hidden)
    normed = centre * scale_by
    both = grad * normed
    small_ref[0:1, :] = jnp.sum(grad, 0, keepdims=True)
    small_ref[1:2, :] = jnp.sum(both, 0, keepdims=True)
    inner = grad * (1.0 + scale)
    mean = jnp.mean(inner, -1, keepdims=True)
    along = jnp.mean(inner * normed, -1, keepdims=True)
    step_ref[...] = step_ref[...] + (inner - mean - normed * along) * scale_by


def split_refs(refs, *counts):
    out, at = [], 0
    for count in counts:
        out.append(refs[at : at + count])
        at += count
    return out


def feed_backward_kernel(ways, gate, has_sums, swaps, *refs):
    extra_in, extra_out = int(has_sums) + swaps, int(has_sums) + int(swaps > 0)
    extra_scratch = 4 * int(has_sums) + int(swaps > 0)
    ins, ex_in, outs, ex_out, scratch, ex_scratch, sems = split_refs(
        refs, 7, extra_in, 3, extra_out, 11, extra_scratch, 3
    )
    grad_ref, hidden_ref, branch_ref, mods_ref, weights_hbm, normed_hbm, pre_hbm = ins
    grad_out, small_out, dw_hbm = outs
    weights, gathered, normed, pre, act, dpre, dw, part, beside_in, summed, turn_in = scratch
    local, send, recv = sems
    rows, model = grad_ref.shape
    width = pre.shape[-1]
    greet_signal(gate)
    loads = [
        pltpu.make_async_copy(src, dst, local.at[number])
        for number, (src, dst) in enumerate(
            ((weights_hbm, weights), (pre_hbm, pre), (normed_hbm, normed))
        )
    ]
    for copy in loads:
        copy.start()
    sums_src, swap_src, ex = take_extra(has_sums, swaps, ex_in, ex_out, ex_scratch)
    extra = Extra(
        ways, sums_src, swap_src, ex, local, 4, send, recv, GATHER_COPIES + SCATTER_COPIES
    )
    extra.begin()
    ctx, row, core = place()
    grad = grad_ref[...]
    gathered[square(ctx, row, core)] = (mods_ref[5:6, :] * grad).astype(BF)
    gather = GroupGather(gathered, send, recv)
    scatter = GroupScatter(part, beside_in, summed, turn_in, send, recv, GATHER_COPIES)
    greet_wait(gate)
    gather.start()
    extra.start()
    extra.start_swap()
    small_out[2:3, :] = jnp.sum(grad * branch_ref[...], 0, keepdims=True)
    loads[0].wait()
    loads[1].wait()

    def span_of(name):
        a, b = scatter.chips[name]
        return pl.ds(pl.multiple_of(square(a, b, 0) * rows, 2 * rows), 2 * rows)

    def back(name):
        a, b = scatter.chips[name]
        here = gathered[pl.ds(square(a, b, 0), 2)].reshape(2 * rows, model)
        value = pre[pl.ds(square(a, b, 0), 2)].reshape(2 * rows, width)
        grad_act = dot(here, weights[:, width:])
        root = math.sqrt(2.0 / math.pi)
        bend = gelu_parts(value)
        act[span_of(name), :] = (0.5 * value * (1.0 + bend)).astype(BF)
        slope = 0.5 * (1.0 + bend) + 0.5 * value * (1.0 - bend * bend) * root * (
            1.0 + 3.0 * 0.044715 * value * value
        )
        dpre[span_of(name), :] = (grad_act * slope).astype(BF)

    def down(name):
        a, b = scatter.chips[name]
        out = dot_wide(dpre[span_of(name), :], weights[:, :width]).astype(BF)
        part[pl.ds(square(a, b, 0), 2)] = out.reshape(2, rows, model)

    gather.wait_chip("own")
    back("own")
    gather.relay()
    gather.wait_chip("x")
    back("x")
    gather.wait_chip("y")
    back("y")
    extra.step(2)
    gather.relay_far()
    gather.wait_chip("far")
    back("far")
    down("far")
    scatter.send_pair("far")
    down("x")
    scatter.send_pair("x")
    scatter.add_pair("far")
    down("y")
    scatter.send_pair("y")
    scatter.add_pair("x")
    down("own")
    scatter.send_pair("own")
    scatter.add_pair("y")
    scatter.add_pair("own")
    loads[2].wait()
    tile = 256

    def wide_rows(ref, at):
        return ref[:, :, pl.ds(pl.multiple_of(at * tile, tile), tile)].reshape(8 * rows, tile)

    def out_rows(at):
        return pl.ds(pl.multiple_of(at * tile, tile), tile)

    @pl.loop(0, model // tile)
    def _(at):
        dw[out_rows(at), :width] = dot_tall(wide_rows(normed, at), dpre[...]).astype(BF)

    for k in range(3, ways):
        extra.step(k)
    scatter.turn_corner()

    @pl.loop(0, model // tile)
    def _(at):
        dw[out_rows(at), width:] = dot_tall(wide_rows(gathered, at), act[...]).astype(BF)

    keep = pltpu.make_async_copy(dw, dw_hbm, local.at[3])
    keep.start()
    grad_out[...] = grad
    modulate_backward(scatter.total(), hidden_ref[...], mods_ref[4:5, :], grad_out, small_out)
    gather.finish()
    scatter.finish()
    extra.finish()
    keep.wait()


class RowGather:
    def __init__(self, buf, send, recv):
        ctx, row, core = place()
        tp = row * 2 + core
        along, beside = {"tp": (tp + 2) % 4}, {"tp": row * 2 + 1 - core}
        other = (1 - row) * 2 + core
        self.to_y = remote(0, buf.at[tp], buf.at[tp], send, recv, **along)
        self.to_core = remote(1, buf.at[tp], buf.at[tp], send, recv, **beside)
        self.passed = remote(2, buf.at[other], buf.at[other], send, recv, **beside)

    def start(self):
        self.to_y.start()
        self.to_core.start()

    def relay(self):
        self.to_y.wait_recv()
        self.passed.start()

    def finish(self):
        for copy in (self.to_y, self.to_core, self.passed):
            copy.wait_send()


def attention_backward_kernel(ways, has_sums, swaps, *refs):
    extra_in, extra_out = int(has_sums) + swaps, int(has_sums) + int(swaps > 0)
    extra_scratch = 4 * int(has_sums) + int(swaps > 0)
    ins, ex_in, outs, ex_out, scratch, ex_scratch, sems = split_refs(
        refs, 11, extra_in, 3, extra_out, 18, extra_scratch, 3
    )
    grad_ref, hidden_ref, branch_ref, mods_ref = ins[:4]
    grad_out, small_out, dw_hbm = outs
    weights, normed, q, k, v, lse, mixed = scratch[:7]
    gathered, dmixed, dqh, dq, dkv, dk, dw, part, beside_in, summed, turn_in = scratch[7:]
    local, send, recv = sems
    rows, model = grad_ref.shape
    heads = q.shape[0]
    cut = heads * HEAD_DIM
    loads = [
        pltpu.make_async_copy(src, dst, local.at[number])
        for number, (src, dst) in enumerate(zip(ins[4:], scratch[:7]))
    ]
    for copy in loads:
        copy.start()
    sums_src, swap_src, ex = take_extra(has_sums, swaps, ex_in, ex_out, ex_scratch)
    extra = Extra(
        ways, sums_src, swap_src, ex, local, 8, send, recv, PAIR_COPIES + SCATTER_COPIES
    )
    extra.begin()
    ctx, row, core = place()
    grad = grad_ref[...]
    gathered[row * 2 + core] = (mods_ref[2:3, :] * grad).astype(BF)
    gather = RowGather(gathered, send, recv)
    scatter = GroupScatter(part, beside_in, summed, turn_in, send, recv, PAIR_COPIES)
    gather.start()
    extra.start()
    extra.start_swap()
    small_out[2:3, :] = jnp.sum(grad * branch_ref[...], 0, keepdims=True)
    for copy in loads:
        copy.wait()

    def attend(name, first):
        b = scatter.chips[name][1]
        span = pl.ds(pl.multiple_of(b * 2 * rows, 2 * rows), 2 * rows)
        here = gathered[pl.ds(b * 2, 2)].reshape(2 * rows, model)
        out = dot(here, weights[:, cut : 2 * cut]).astype(BF)
        for head in range(heads):
            dmixed[head, span] = out[:, head * HEAD_DIM : (head + 1) * HEAD_DIM]

        @pl.loop(0, heads)
        def _(head):
            query, upper = q[head, span], dmixed[head, span]
            scores = dot_wide(k[head], query)
            top = jnp.concatenate(
                [lse[head, pl.ds(b * 2, 1)], lse[head, pl.ds(b * 2 + 1, 1)]], 1
            )
            weight = jnp.exp(scores - top)
            grad_prob = dot_wide(v[head], upper)
            inner = jnp.sum(weight * grad_prob, 0, keepdims=True)
            grad_score = (weight * (grad_prob - inner)).astype(BF)
            grad_value = dot(weight.astype(BF), upper)
            grad_key = dot(grad_score, query)
            grad_query = dot_tall(grad_score, k[head])
            dqh[head, span] = (grad_query * SCORE_SCALE).astype(BF)
            if first:
                dk[head] = grad_key
                dk[heads + head] = grad_value
            else:
                dk[head] = dk[head] + grad_key
                dk[heads + head] = dk[heads + head] + grad_value

    gather.to_core.wait_recv()
    attend("own", True)
    gather.relay()
    extra.step(2)
    gather.passed.wait_recv()
    attend("y", False)
    for head in range(heads):
        dq[:, head * HEAD_DIM : (head + 1) * HEAD_DIM] = dqh[head]
    for head in range(2 * heads):
        dkv[:, head * HEAD_DIM : (head + 1) * HEAD_DIM] = dk[head].astype(BF)
    for step in range(3, ways):
        extra.step(step)

    def span_of(name):
        a, b = scatter.chips[name]
        return pl.ds(pl.multiple_of(square(a, b, 0) * rows, 2 * rows), 2 * rows)

    def down(name):
        a, b = scatter.chips[name]
        out = dot_wide(dkv[span_of(name), :], weights[:, 2 * cut :])
        if name in ("own", "y"):
            span = pl.ds(pl.multiple_of(b * 2 * rows, 2 * rows), 2 * rows)
            out = out + dot_wide(dq[span, :], weights[:, :cut])
        part[pl.ds(square(a, b, 0), 2)] = out.astype(BF).reshape(2, rows, model)

    down("far")
    scatter.send_pair("far")
    down("x")
    scatter.send_pair("x")
    scatter.add_pair("far")
    down("y")
    scatter.send_pair("y")
    scatter.add_pair("x")
    down("own")
    scatter.send_pair("own")
    scatter.add_pair("y")
    scatter.add_pair("own")
    tile = 256

    def out_rows(at):
        return pl.ds(pl.multiple_of(at * tile, tile), tile)

    @pl.loop(0, model // tile)
    def _(at):
        lanes = out_rows(at)
        all_rows = normed[:, :, lanes].reshape(8 * rows, tile)
        dw[out_rows(at), 2 * cut :] = dot_tall(all_rows, dkv[...]).astype(BF)

    scatter.turn_corner()

    @pl.loop(0, model // tile)
    def _(at):
        lanes = out_rows(at)
        mine = normed[pl.ds(ctx * 4, 4), :, lanes].reshape(4 * rows, tile)
        dw[out_rows(at), :cut] = dot_tall(mine, dq[...]).astype(BF)
        upper = gathered[:, :, lanes].reshape(4 * rows, tile)
        dw[out_rows(at), cut : 2 * cut] = dot_tall(upper, mixed[...]).astype(BF)

    keep = pltpu.make_async_copy(dw, dw_hbm, local.at[7])
    keep.start()
    grad_out[...] = grad
    modulate_backward(scatter.total(), hidden_ref[...], mods_ref[1:2, :], grad_out, small_out)
    gather.finish()
    scatter.finish()
    extra.finish()
    keep.wait()


def layer_backward_kernel(ways, prior, *refs):
    hop, before = int(ways > 1), int(ways > 1 and prior)
    (
        (grad, mods),
        feed_in,
        attention_in,
        prior_grads,
        prior_shard,
        (grad_out, small_feed, small_attention, dw_feed, dw_attention),
        shard_before,
        shard_feed,
        swap_out,
        (middle,),
        feed_scratch,
        feed_extra,
        feed_sems,
        scratch,
        hops,
        swap_buf,
        sems,
    ) = split_refs(
        refs, 2, 5, 9, before, before, 5, before, hop, before, 1, 11, 4 * before, 3, 18, 3 * hop,
        before, 3,
    )
    hidden, branch, *rest = feed_in
    feed_backward_kernel(
        ways,
        ways,
        before == 1,
        0,
        grad,
        hidden,
        branch,
        mods,
        *rest,
        *prior_grads,
        middle,
        small_feed,
        dw_feed,
        *shard_before,
        *feed_scratch,
        *feed_extra,
        *feed_sems,
    )
    hidden, branch, *rest = attention_in
    dw = feed_scratch[6]
    sources = ((dw,) if hop else ()) + tuple(prior_shard) + tuple(shard_before)
    attention_backward_kernel(
        ways,
        hop == 1,
        2 * before,
        middle,
        hidden,
        branch,
        mods,
        *rest,
        *sources,
        grad_out,
        small_attention,
        dw_attention,
        *shard_feed,
        *swap_out,
        *scratch,
        *((dw,) if hop else ()),
        *hops,
        *swap_buf,
        *sems,
    )


def layer_backward(grad, mods, blocks, kept_attention, kept_feed, prior, number):
    rows, model = grad.shape
    attention_weights, feed_weights = blocks
    shape = attention_weights.shape
    cut, width = shape[1] // 4, shape[1] // 2
    heads = cut // HEAD_DIM
    ways = lax.axis_size("shard")
    if ways > HOP_WAYS:
        ways = 1
    hop, before = ways > 1, prior is not None
    shard = (shape[0] // ways, shape[1])
    hidden, normed, pre, branch = kept_feed
    feed_in = [hidden, branch, feed_weights, normed, pre]
    hidden, branch, *saved = kept_attention
    attention_in = [hidden, branch, attention_weights, *saved]
    outs = [sds((rows, model), F32), sds((3, model), F32), sds((3, model), F32)]
    outs += [sds(shape, BF)] * 2
    specs = [VMEM, VMEM, VMEM, ANY, ANY]
    outs += [sds(shard, BF)] * (before + hop) + [sds((2, *shard), BF)] * before
    specs += [VMEM] * (before + hop) + [ANY] * before
    hops = pltpu.VMEM((line_copies(ways), *shard), BF)
    line = [hops, hops, pltpu.VMEM(shard, F32)]

    def buffers(copies, locals_used):
        return [
            pltpu.SemaphoreType.DMA((locals_used,)),
            pltpu.SemaphoreType.DMA((copies,)),
            pltpu.SemaphoreType.DMA((copies,)),
        ]

    group = [
        pltpu.VMEM((8, rows, model), BF),
        pltpu.VMEM((4, rows, model), BF),
        pltpu.VMEM((4, rows, model), BF),
        pltpu.VMEM((6, rows // 2, model), BF),
    ]
    scratch = [pltpu.VMEM((rows, model), F32)]
    scratch += [
        pltpu.VMEM(shape, BF),
        pltpu.VMEM((8, rows, model), BF),
        pltpu.VMEM((8, rows, model), BF),
        pltpu.VMEM((8, rows, width), F32),
        pltpu.VMEM((8 * rows, width), BF),
        pltpu.VMEM((8 * rows, width), BF),
        pltpu.VMEM(shape, BF),
    ] + group
    if before:
        scratch += [pltpu.VMEM(shape, BF)] + line
    scratch += buffers(GATHER_COPIES + SCATTER_COPIES + line_copies(ways), 6)
    scratch += [pltpu.VMEM(leaf.shape, leaf.dtype) for leaf in [attention_weights, *saved]]
    scratch += [
        pltpu.VMEM((4, rows, model), BF),
        pltpu.VMEM((heads, 4 * rows, HEAD_DIM), BF),
        pltpu.VMEM((heads, 4 * rows, HEAD_DIM), BF),
        pltpu.VMEM((4 * rows, cut), BF),
        pltpu.VMEM((8 * rows, 2 * cut), BF),
        pltpu.VMEM((2 * heads, 8 * rows, HEAD_DIM), F32),
        pltpu.VMEM(shape, BF),
    ] + group
    if hop:
        scratch += line
    if before:
        scratch.append(pltpu.VMEM((2, *shard), BF))
    scratch += buffers(PAIR_COPIES + SCATTER_COPIES + line_copies(ways) + 2, 10)
    result = pl.pallas_call(
        functools.partial(layer_backward_kernel, ways, before),
        out_shape=outs,
        in_specs=[VMEM] * 4 + [ANY] * 3 + [VMEM] * 2 + [ANY] * (7 + 2 * before),
        out_specs=specs,
        scratch_shapes=scratch,
        compiler_params=pltpu.CompilerParams(collective_id=number, has_side_effects=True),
        name="layer_backward",
    )(grad, mods, *feed_in, *attention_in, *(prior if before else ()))
    grad, small_feed, small_attention, dw_feed, dw_attention, *rest = result
    shard_before = rest.pop(0) if before else None
    shard_feed = rest.pop(0) if hop else None
    swapped = rest.pop(0) if before else None
    return grad, small_feed, small_attention, dw_feed, dw_attention, shard_before, shard_feed, swapped


def exchange_kernel(ways, modes, pieces, by_tp, by_x, has_block, has_sums, swaps, *refs):
    count = len(modes)
    stacked = [number for number in range(count) if pieces[number] > 1]
    extra_in, extra_out = int(has_sums) + swaps, int(has_sums) + int(swaps > 0)
    extra_scratch = 4 * int(has_sums) + int(swaps > 0)
    block = int(has_block)
    parts, block_in, ex_in, outs, block_out, ex_out, scratch, stack_buf, block_buf, ex_scratch, sems = (
        split_refs(
            refs,
            sum(pieces),
            block,
            extra_in,
            count,
            block,
            extra_out,
            3 * count,
            len(stacked),
            block,
            extra_scratch,
            3,
        )
    )
    held, arrived, far = scratch[:count], scratch[count : 2 * count], scratch[2 * count :]
    local, send, recv = sems
    sums_src, swap_src, ex = take_extra(has_sums, swaps, ex_in, ex_out, ex_scratch)
    stages = 2 * int(by_tp) + int(by_x)
    used = count * (stages + ways - 1)
    extra = Extra(ways, sums_src, swap_src, ex, local, 1, send, recv, used)
    if has_sums:
        used += line_copies(ways)
    used += swaps
    extra.begin()
    ctx, row, core = place()
    tp = row * 2 + core
    at = lax.axis_index("shard")
    barrier = pltpu.get_barrier_semaphore()
    sides = [{"tp": row * 2 + 1 - core}, {"tp": (tp + 2) % 4}] if by_tp else []
    if by_x:
        sides.append({"ctx": 1 - ctx})
    greeted = sides if by_x or not swaps else sides + [{"ctx": 1 - ctx}]
    for where in greeted:
        pl.semaphore_signal(barrier, inc=1, device_id=where, device_id_type=MESH)
    for away in range(1, ways):
        pl.semaphore_signal(
            barrier, inc=1, device_id={"shard": (at + away) % ways}, device_id_type=MESH
        )
    pl.semaphore_wait(barrier, len(greeted) + ways - 1)
    copies = []
    now, taken = [], 0
    for number in range(count):
        given = parts[taken : taken + pieces[number]]
        taken += pieces[number]
        if number in stacked:
            into, first = stack_buf[stacked.index(number)], 0
            for ref in given:
                into[first : first + ref.shape[0]] = ref[...]
                first += ref.shape[0]
            given = [into]
        now.append(given[0])
    for stage, where in enumerate(sides):
        here = []
        for number in range(count):
            here.append(
                remote(
                    number * stages + stage,
                    now[number],
                    arrived[number].at[stage],
                    send,
                    recv,
                    **where,
                )
            )
            here[-1].start()
        if stage == 0:
            if has_block:
                line = LineGather(
                    ways, block_in[0], block_buf[0], local.at[0], send, recv, used
                )
                line.start()
            extra.start()
            extra.start_swap()
        for number in range(count):
            here[number].wait_recv()
            both = now[number][...].astype(F32) + arrived[number][stage].astype(F32)
            held[number][stage] = both.astype(held[number].dtype)
            now[number] = held[number].at[stage]
        copies += here
    if has_block:
        line.step(2)
    base = count * stages
    for number, mode in enumerate(modes):
        if mode == "gather":
            far[number][at] = now[number][...].astype(far[number].dtype)
            now[number] = far[number].at[at]
    waits = []
    for number, mode in enumerate(modes):
        for away in range(1, ways):
            to = (at + away) % ways
            copy = remote(
                base + number * (ways - 1) + away - 1,
                now[number].at[to] if mode == "scatter" else now[number],
                far[number].at[at],
                send,
                recv,
                shard=to,
            )
            copy.start()
            waits.append(copy)
        if mode != "gather":
            far[number][at] = now[number][at] if mode == "scatter" else now[number][...]
    extra.step(2)
    for k in range(3, ways):
        if has_block:
            line.step(k)
        extra.step(k)
    for copy in waits:
        copy.wait_recv()
    for number, mode in enumerate(modes):
        if mode == "gather":
            outs[number][...] = far[number][...].astype(F32)
            continue
        total = far[number][0].astype(F32)
        for index in range(1, ways):
            total = total + far[number][index].astype(F32)
        outs[number][...] = total
    for copy in copies + waits:
        copy.wait_send()
    extra.finish()
    if has_block:
        line.finish()
        keep = pltpu.make_async_copy(block_buf[0], block_out[0], local.at[0])
        keep.start()
        keep.wait()


def stacked_shape(arrays):
    return (sum(array.shape[0] for array in arrays), *arrays[0].shape[1:])


def exchange(parts, number, by_tp=True, by_x=False, block=None, grads=None, swaps=()):
    ways = lax.axis_size("shard")
    if ways > HOP_WAYS:
        return exchange_plain(parts, by_tp, by_x)
    stages = 2 * int(by_tp) + int(by_x)
    modes, pieces = [mode for _, mode in parts], [len(arrays) for arrays, _ in parts]
    outs, held, arrived, far, stacks, given = [], [], [], [], [], []
    for arrays, mode in parts:
        whole, dtype = stacked_shape(arrays), arrays[0].dtype
        one = whole[1:] if mode == "scatter" else whole
        full = (ways, *one)
        given += list(arrays)
        outs.append(sds(full if mode == "gather" else one, F32))
        held.append(pltpu.VMEM((max(stages, 1), *whole), dtype))
        arrived.append(pltpu.VMEM((max(stages, 1), *whole), dtype))
        far.append(pltpu.VMEM(full, BF if mode == "gather" else dtype))
        if len(arrays) > 1:
            stacks.append(pltpu.VMEM(whole, dtype))
    specs = [VMEM] * len(outs)
    block_specs, block_scratch, inputs = [], [], len(given)
    copies = len(parts) * (stages + ways - 1)
    if block is not None:
        shape = (ways * block.shape[0], block.shape[1])
        given.append(block)
        block_specs.append(ANY)
        block_scratch.append(pltpu.VMEM(shape, BF))
        outs.append(sds(shape, BF))
        copies += line_copies(ways)
    more, more_outs, more_specs, more_scratch, more_copies = extra_shapes(ways, grads, swaps)
    copies += more_copies
    return pl.pallas_call(
        functools.partial(
            exchange_kernel,
            ways,
            tuple(modes),
            tuple(pieces),
            by_tp,
            by_x,
            block is not None,
            grads is not None,
            len(swaps),
        ),
        out_shape=outs + more_outs,
        in_specs=[VMEM] * inputs + block_specs + [ANY] * len(more),
        out_specs=specs + block_specs + more_specs,
        scratch_shapes=held
        + arrived
        + far
        + stacks
        + block_scratch
        + more_scratch
        + [
            pltpu.SemaphoreType.DMA((3,)),
            pltpu.SemaphoreType.DMA((copies,)),
            pltpu.SemaphoreType.DMA((copies,)),
        ],
        compiler_params=pltpu.CompilerParams(collective_id=number, has_side_effects=True),
        name="exchange",
    )(*given, *more)


def exchange_plain(parts, by_tp, by_x):
    near = (("ctx",) if by_x else ()) + (("tp",) if by_tp else ())
    outs = []
    for arrays, mode in parts:
        wide = jnp.concatenate(arrays, 0).astype(F32)
        if mode == "gather":
            outs.append(lax.all_gather(lax.psum(wide, near), "shard", axis=0))
        elif mode == "scatter":
            total = lax.psum_scatter(wide, "shard", scatter_dimension=0, tiled=True)
            outs.append(lax.psum(total, near)[0])
        else:
            outs.append(lax.psum(wide, ("shard",) + near))
    return outs


def spread(values, at, axis_size):
    full = jnp.zeros((*values.shape[:-1], axis_size), values.dtype)
    return lax.dynamic_update_slice_in_dim(full, values, at, values.ndim - 1)


def silu_grad(values):
    gate = jax.nn.sigmoid(values)
    return gate * (1.0 + values * (1.0 - gate))


def local(
    noised,
    velocity,
    labels,
    time_ids,
    stem,
    stem_mean,
    stem_square,
    modulation,
    modulation_mean,
    modulation_square,
    attention_in,
    attention_in_mean,
    attention_in_square,
    attention_out,
    attention_out_mean,
    attention_out_square,
    feedforward,
    feedforward_mean,
    feedforward_square,
):
    tensor_ways = lax.axis_size("tp")
    shard_ways = lax.axis_size("shard")
    own_latent = lax.axis_index("shard")
    own_ctx = lax.axis_index("ctx")
    own_tp = lax.axis_index("tp")
    owned = stem.shape[1]
    first_owned = (own_latent * tensor_ways + lax.axis_index("tp")) * owned

    def own_columns(values):
        return lax.dynamic_slice_in_dim(values, first_owned, owned, values.ndim - 1)

    stem_low = stem.astype(jnp.bfloat16)
    class_own, time_in_own, time_out_own, shift_own, scale_own, patch_own, head_own = split_stem(
        stem_low
    )
    modulation_low = modulation.astype(jnp.bfloat16)
    mine = (jnp.arange(shard_ways) == own_latent).astype(jnp.float32)[:, None]
    packed_ids = mine * jnp.concatenate([labels, time_ids]).astype(jnp.float32)[None, :]
    ids_wide = jnp.pad(packed_ids, ((0, 0), (0, 126)))
    (ids_all,) = exchange([([ids_wide], "sum")], 10, by_tp=False)
    all_labels, all_times = ids_all[:, 0].astype(jnp.int32), ids_all[:, 1].astype(jnp.int32)
    latents = all_labels.shape[0]
    features = time_features(all_times).astype(jnp.bfloat16)
    time_pre = jnp.dot(features, time_in_own, preferred_element_type=jnp.float32)
    time_hidden_own = jax.nn.silu(time_pre).astype(jnp.bfloat16)
    hidden_half = feedforward.shape[3] // lax.axis_size("ctx")
    feed_low = lax.dynamic_slice_in_dim(feedforward, own_ctx * hidden_half, hidden_half, 3).astype(
        jnp.bfloat16
    )
    in_low, out_low = attention_in.astype(jnp.bfloat16), attention_out.astype(jnp.bfloat16)
    hops = shard_ways <= HOP_WAYS
    own_blocks, blocks = [], []
    for layer_at in range(LAYERS):
        parts = [in_low[layer_at, 0], out_low[layer_at], in_low[layer_at, 1], in_low[layer_at, 2]]
        own_blocks.append(jnp.concatenate(parts, 1))
        own_blocks.append(jnp.concatenate([feed_low[layer_at, 0], feed_low[layer_at, 1]], 1))
    to_send = jnp.concatenate([time_hidden_own, patch_own, head_own], 0)
    half_rows = own_blocks[0].shape[0] // 2
    exchanged = exchange(
        [([spread(to_send, first_owned, D)], "sum")], 11, block=own_blocks[0][:half_rows]
    )
    packed = exchanged[0].astype(jnp.bfloat16)
    time_hidden = packed[:latents]
    patch_in, head_rows = packed[latents : latents + PDIM], packed[latents + PDIM :]
    onehot = (all_labels[:, None] == jnp.arange(CLASSES)[None, :]).astype(jnp.bfloat16)
    condition = jnp.dot(time_hidden, time_out_own, preferred_element_type=jnp.float32) + jnp.dot(
        onehot, class_own, preferred_element_type=jnp.float32
    )
    gated_own = jax.nn.silu(condition).astype(jnp.bfloat16)
    mod_part = jnp.einsum(
        "bd,lde->ble", gated_own, modulation_low, preferred_element_type=jnp.float32
    )
    first_half = exchanged[1:]
    mod_part = mod_part.reshape(latents, LAYERS * 6, D)
    exchanged = exchange(
        [([mod_part], "scatter"), ([spread(gated_own, first_owned, D)], "sum")],
        12,
        block=own_blocks[0][half_rows:],
    )
    layer_mods = exchanged[0].reshape(LAYERS, 6, D)
    gated = exchanged[1].astype(jnp.bfloat16)
    if hops:
        both = [part.reshape(shard_ways, half_rows, -1) for part in (first_half[0], exchanged[2])]
        blocks.append(jnp.concatenate(both, 1).reshape(shard_ways * 2 * half_rows, -1))
    else:
        for block in own_blocks:
            blocks.append(lax.all_gather(block, "shard", axis=0, tiled=True))
    end_own = jnp.stack(
        [
            jnp.dot(gated, shift_own, preferred_element_type=jnp.float32),
            jnp.dot(gated, scale_own, preferred_element_type=jnp.float32),
        ],
        1,
    )
    (end_mods,) = exchange([([spread(end_own, first_owned, D)], "scatter")], 13)
    end_shift, end_scale = end_mods[0:1], end_mods[1:2]

    pieces = patchify(noised)[0]
    rows_here = noised.shape[2] // PATCH
    first_row = (own_ctx * tensor_ways + lax.axis_index("tp")) * rows_here
    embedded = jnp.dot(pieces, patch_in, preferred_element_type=jnp.float32)
    hidden = embedded + positions(first_row, rows_here, noised.shape[3] // PATCH, D)
    saved, weights = [], blocks[0]
    for layer_at in range(LAYERS):
        final = layer_at + 1 == LAYERS
        feed_own, ahead, feed_weights = None, None, None
        if hops:
            feed_own = own_blocks[2 * layer_at + 1]
            ahead = None if final else own_blocks[2 * layer_at + 2]
        else:
            weights, feed_weights = blocks[2 * layer_at : 2 * layer_at + 2]
        hidden, kept_attention, kept_feed, feed_weights, following = layer_forward(
            hidden, layer_mods[layer_at], weights, feed_weights, feed_own, ahead, 2 + int(final)
        )
        saved.append((kept_attention, kept_feed, (weights, feed_weights)))
        weights = following

    final_normed = modulate(hidden, end_shift, end_scale).astype(jnp.bfloat16)
    predicted = jnp.einsum(
        "pd,cd->pc", final_normed, head_rows, preferred_element_type=jnp.float32
    )
    target_rows = patchify(velocity)[0].astype(jnp.float32)
    weighting = 0.5 + time_ids.astype(jnp.float32)[0] / STEPS
    misfit = predicted - target_rows
    loss_scale = 1.0 / (shard_ways * PATCHES * PDIM)
    loss_local = jnp.sum(weighting * misfit * misfit) * loss_scale
    grad_pred = (2.0 * loss_scale * weighting * misfit).astype(jnp.bfloat16)
    grad_head = jnp.einsum("pc,pd->cd", grad_pred, final_normed, preferred_element_type=jnp.float32)
    grad_normed = jnp.dot(grad_pred, head_rows, preferred_element_type=jnp.float32)
    grad_hidden, grad_end_shift, grad_end_scale = jax.vjp(modulate, hidden, end_shift, end_scale)[
        1
    ](grad_normed)

    small = [None] * (2 * LAYERS)
    shards, others = [None] * (2 * LAYERS), [None] * (2 * LAYERS)
    prior = None
    for layer_at in reversed(range(LAYERS)):
        kept_attention, kept_feed, pair = saved[layer_at]
        one, two = 2 * layer_at, 2 * layer_at + 1
        (
            grad_hidden,
            small[two],
            small[one],
            feed_grads,
            grads,
            shard_before,
            shards[two],
            swapped,
        ) = layer_backward(
            grad_hidden,
            layer_mods[layer_at],
            pair,
            kept_attention,
            kept_feed,
            prior,
            5 + int(prior is None),
        )
        if prior is not None:
            shards[one + 2] = shard_before
            others[two + 2], others[one + 2] = swapped[0], swapped[1]
        if hops:
            prior = (grads, shards[two])
        else:
            for half, local_grads in ((one, grads), (two, feed_grads)):
                shards[half] = lax.psum_scatter(
                    local_grads, "shard", scatter_dimension=0, tiled=True
                )
                others[half] = lax.ppermute(shards[half], "ctx", [(0, 1), (1, 0)])
    grad_embed = grad_hidden.astype(jnp.bfloat16)
    grad_patch = jnp.einsum("pf,pd->fd", pieces, grad_embed, preferred_element_type=jnp.float32)

    pixel = jnp.concatenate([grad_patch, grad_head], 0).astype(jnp.bfloat16)
    pixel = pixel.reshape(2 * PDIM, shard_ways, -1).transpose(1, 0, 2)
    result = exchange(
        [(small + [grad_end_shift, grad_end_scale], "gather"), ([pixel], "scatter")],
        14,
        by_x=True,
        grads=grads,
        swaps=[shards[1]],
    )
    small, pixel = result[0], result[1]
    if hops:
        shards[0], others[1] = result[2], result[3][0]
    grad_mod = small[:, : 6 * LAYERS].reshape(latents, LAYERS, 6 * D)
    grad_ends = small[:, 6 * LAYERS :]
    ends_here = own_columns(grad_ends)
    gated_part = jnp.dot(
        ends_here[:, 0], shift_own.astype(jnp.float32).T, precision=highest
    ) + jnp.dot(ends_here[:, 1], scale_own.astype(jnp.float32).T, precision=highest)
    result = exchange([([gated_part], "sum")], 15, swaps=[shards[0]])
    if hops:
        others[0] = result[1][0]
    grad_gated = own_columns(result[0]) + jnp.einsum(
        "ble,lde->bd", grad_mod, modulation_low.astype(jnp.float32), precision=highest
    )
    grad_condition = grad_gated * silu_grad(condition)
    time_part = jnp.dot(grad_condition, time_out_own.astype(jnp.float32).T, precision=highest)
    (grad_time_hidden,) = exchange([([time_part], "sum")], 16)
    grad_time_hidden = own_columns(grad_time_hidden)
    grad_time_pre = grad_time_hidden * silu_grad(time_pre)
    gated_wide = gated.astype(jnp.float32)
    grad_ends_own = lax.dynamic_slice_in_dim(pixel, own_tp * owned, owned, 1)
    shard_stem = jnp.concatenate(
        [
            jnp.dot(onehot.astype(jnp.float32).T, grad_condition, precision=highest),
            jnp.dot(features.astype(jnp.float32).T, grad_time_pre, precision=highest),
            jnp.dot(time_hidden.astype(jnp.float32).T, grad_condition, precision=highest),
            jnp.dot(gated_wide.T, ends_here[:, 0], precision=highest),
            jnp.dot(gated_wide.T, ends_here[:, 1], precision=highest),
            grad_ends_own,
        ],
        0,
    )
    shard_modulation = jnp.einsum(
        "bd,ble->lde", gated_own.astype(jnp.float32), grad_mod, precision=highest
    )
    cut = attention_in.shape[3]
    shard_in, shard_out, shard_hidden = [], [], []
    for layer_at in range(LAYERS):
        own, other = shards[2 * layer_at], others[2 * layer_at]
        both = own.astype(jnp.float32) + other.astype(jnp.float32)
        shard_out.append(both[:, cut : 2 * cut])
        shard_in.append(
            jnp.stack([both[:, number * cut : (number + 1) * cut] for number in (0, 2, 3)])
        )
        own, other = shards[2 * layer_at + 1], others[2 * layer_at + 1]
        low, high = jnp.where(own_ctx == 0, own, other), jnp.where(own_ctx == 0, other, own)
        shard_hidden.append(
            jnp.stack(
                [
                    jnp.concatenate([low[:, :hidden_half], high[:, :hidden_half]], 1),
                    jnp.concatenate([low[:, hidden_half:], high[:, hidden_half:]], 1),
                ]
            )
        )
    shard_in, shard_out = jnp.stack(shard_in), jnp.stack(shard_out)
    shard_hidden = jnp.stack(shard_hidden).astype(jnp.float32)
    squares = (
        jnp.sum(shard_stem * shard_stem)
        + jnp.sum(shard_modulation * shard_modulation)
        + jnp.sum(shard_in * shard_in)
        + jnp.sum(shard_out * shard_out)
        + jnp.sum(shard_hidden * shard_hidden)
    )
    squares = jnp.where(own_ctx == 0, squares, jnp.zeros((), jnp.float32))
    sums = jnp.stack([squares, loss_local])[:, None] * jnp.ones((1, 128), jnp.float32)
    (sums,) = exchange([([sums], "sum")], 17, by_x=True)
    square_total, train_loss = sums[0, 0], sums[1, 0]
    total_norm = jnp.sqrt(square_total)
    factor = clip_level / jnp.maximum(total_norm, clip_level)
    stem_out = adam_update(stem, stem_mean, stem_square, shard_stem, factor)
    mod_out = adam_update(modulation, modulation_mean, modulation_square, shard_modulation, factor)
    in_out = adam_update(attention_in, attention_in_mean, attention_in_square, shard_in, factor)
    proj_out = adam_update(
        attention_out, attention_out_mean, attention_out_square, shard_out, factor
    )
    feed_out = adam_update(feedforward, feedforward_mean, feedforward_square, shard_hidden, factor)
    return (
        train_loss,
        total_norm,
        stem_out[0],
        stem_out[1],
        stem_out[2],
        stem_out[3],
        mod_out[0],
        mod_out[1],
        mod_out[2],
        mod_out[3],
        in_out[0],
        in_out[1],
        in_out[2],
        in_out[3],
        proj_out[0],
        proj_out[1],
        proj_out[2],
        proj_out[3],
        feed_out[0],
        feed_out[1],
        feed_out[2],
        feed_out[3],
    )


def solution(mesh):
    placed = (
        P("shard", None, ("ctx", "tp"), None),
        P("shard", None, ("ctx", "tp"), None),
        P("shard"),
        P("shard"),
        P(None, ("shard", "tp")),
        P(None, ("shard", "tp")),
        P(None, ("shard", "tp")),
        P(None, ("shard", "tp"), None),
        P(None, ("shard", "tp"), None),
        P(None, ("shard", "tp"), None),
        P(None, None, "shard", "tp"),
        P(None, None, "shard", "tp"),
        P(None, None, "shard", "tp"),
        P(None, "shard", "tp"),
        P(None, "shard", "tp"),
        P(None, "shard", "tp"),
        P(None, None, "shard", "tp"),
        P(None, None, "shard", "tp"),
        P(None, None, "shard", "tp"),
    )
    return jax.shard_map(
        local,
        mesh=mesh,
        in_specs=placed,
        out_specs=(
            P(),
            P(),
            P(None, ("shard", "tp")),
            P(None, ("shard", "tp")),
            P(None, ("shard", "tp")),
            P(None, ("shard", "tp")),
            P(None, ("shard", "tp"), None),
            P(None, ("shard", "tp"), None),
            P(None, ("shard", "tp"), None),
            P(None, ("shard", "tp"), None),
            P(None, None, "shard", "tp"),
            P(None, None, "shard", "tp"),
            P(None, None, "shard", "tp"),
            P(None, None, "shard", "tp"),
            P(None, "shard", "tp"),
            P(None, "shard", "tp"),
            P(None, "shard", "tp"),
            P(None, "shard", "tp"),
            P(None, None, "shard", "tp"),
            P(None, None, "shard", "tp"),
            P(None, None, "shard", "tp"),
            P(None, None, "shard", "tp"),
        ),
        check_vma=False,
    )
```

```python
import functools
import math

import jax
import jax.numpy as jnp
from jax import lax
from jax.experimental import pallas as pl
from jax.experimental.pallas import tpu as pltpu
from jax.sharding import PartitionSpec as P

D = 768
HEAD_DIM = 64
CLASSES = 1000
FREQ = 256
PATCH = 2
STEPS = 1000
LAYERS = 4
PATCHES = 1024
PDIM = 16


norm_eps = 1e-06
clip_level = 0.5
learn_rate = 0.01
beta_first = 0.5
beta_second = 0.5
adam_eps = 1e-08
weight_decay = 0.1
bias_fix = 0.875
highest = lax.Precision.HIGHEST


def layer_norm(values):
    centre = values - jnp.mean(values, -1, keepdims=True)
    spread = jnp.mean(centre * centre, -1, keepdims=True)
    return centre * lax.rsqrt(spread + norm_eps)


def modulate(values, shift_rows, scale_rows):
    return layer_norm(values) * (1.0 + scale_rows) + shift_rows


def gelu_tanh(values):
    return jax.nn.gelu(values, approximate=True)


def patchify(image_in):
    latent_count, channels, height, columns = image_in.shape
    shaped = image_in.reshape(
        latent_count, channels, height // PATCH, PATCH, columns // PATCH, PATCH
    )
    shaped = shaped.transpose(0, 2, 4, 3, 5, 1)
    return shaped.reshape(
        latent_count, height // PATCH * (columns // PATCH), PATCH * PATCH * channels
    )


def positions(first_row, height, columns, model_width):
    quarter = model_width // 4
    omegas = jnp.exp(-math.log(10000.0) * jnp.arange(quarter).astype(jnp.float32) / quarter)
    row_angle = (first_row + jnp.arange(height)).astype(jnp.float32)[:, None] * omegas[None, :]
    col_angle = jnp.arange(columns).astype(jnp.float32)[:, None] * omegas[None, :]
    row_part = jnp.concatenate([jnp.sin(row_angle), jnp.cos(row_angle)], -1)
    col_part = jnp.concatenate([jnp.sin(col_angle), jnp.cos(col_angle)], -1)
    grid_table = jnp.concatenate(
        [
            jnp.broadcast_to(col_part[None], (height, columns, 2 * quarter)),
            jnp.broadcast_to(row_part[:, None], (height, columns, 2 * quarter)),
        ],
        -1,
    )
    return grid_table.reshape(height * columns, model_width)


def time_features(step_ids):
    half_width = FREQ // 2
    frequencies = jnp.exp(
        -math.log(10000.0) * jnp.arange(half_width).astype(jnp.float32) / half_width
    )
    angles = step_ids.astype(jnp.float32)[:, None] * frequencies[None, :]
    return jnp.concatenate([jnp.cos(angles), jnp.sin(angles)], -1)


def split_stem(stem_rows):
    bounds = [CLASSES, FREQ, D, D, D, PDIM, PDIM]
    pieces_out = []
    offset = 0
    for extent in bounds:
        pieces_out.append(stem_rows[offset : offset + extent])
        offset = offset + extent
    return pieces_out


def adam_update(master, first_moment, second_moment, gradient, factor):
    clipped = gradient * factor
    first_new = beta_first * first_moment + (1.0 - beta_first) * clipped
    second_new = beta_second * second_moment + (1.0 - beta_second) * clipped * clipped
    direction = first_new / bias_fix / (jnp.sqrt(second_new / bias_fix) + adam_eps)
    master_new = master - learn_rate * (direction + weight_decay * master)
    return (master_new, first_new, second_new, master_new.astype(jnp.bfloat16))


GROUP = ("ctx", "tp")
OWNERS = ("shard", "tp")
EVERY = ("shard", "ctx", "tp")
HOP_WAYS = 4


MESH = pl.DeviceIdType.MESH
BF = jnp.bfloat16
F32 = jnp.float32
SCORE_SCALE = HEAD_DIM**-0.5


def place():
    ctx, tp = lax.axis_index("ctx"), lax.axis_index("tp")
    core = tp % 2
    row = tp // 2
    return ctx, row, core


def square(ctx, row, core):
    return ctx * 4 + row * 2 + core


def remote(index, src, dst, send, recv, **where):
    return pltpu.make_async_remote_copy(
        src_ref=src,
        dst_ref=dst,
        send_sem=send.at[index],
        recv_sem=recv.at[index],
        device_id=where,
        device_id_type=MESH,
    )


def greet_signal(shard_ways):
    ctx, row, core = place()
    barrier = pltpu.get_barrier_semaphore()
    tp = row * 2 + core
    pl.semaphore_signal(barrier, inc=1, device_id={"ctx": 1 - ctx}, device_id_type=MESH)
    pl.semaphore_signal(barrier, inc=1, device_id={"tp": (tp + 2) % 4}, device_id_type=MESH)
    pl.semaphore_signal(
        barrier, inc=1, device_id={"tp": row * 2 + 1 - core}, device_id_type=MESH
    )
    if shard_ways > 1:
        line_signal(shard_ways)


def line_signal(ways):
    barrier = pltpu.get_barrier_semaphore()
    at = lax.axis_index("shard")
    for away in (1, 2):

        @pl.when(at >= away)
        def _():
            pl.semaphore_signal(
                barrier, inc=1, device_id={"shard": at - away}, device_id_type=MESH
            )

        @pl.when(at < ways - away)
        def _():
            pl.semaphore_signal(
                barrier, inc=1, device_id={"shard": at + away}, device_id_type=MESH
            )


def greet_wait(shard_ways):
    barrier = pltpu.get_barrier_semaphore()
    if shard_ways == 1:
        pl.semaphore_wait(barrier, 3)
        return
    at = lax.axis_index("shard")
    for own in range(shard_ways):
        near = min(own, 2) + min(shard_ways - 1 - own, 2)

        @pl.when(at == own)
        def _():
            pl.semaphore_wait(barrier, 3 + near)


GATHER_COPIES = 13


class GroupGather:
    def __init__(self, buf, send, recv):
        ctx, row, core = place()
        half = buf.shape[1] // 2
        tp = row * 2 + core
        across, along = {"ctx": 1 - ctx}, {"tp": (tp + 2) % 4}
        beside = {"tp": row * 2 + 1 - core}
        own = square(ctx, row, core)
        self.by_x, self.by_y = square(1 - ctx, row, core), square(ctx, 1 - row, core)
        self.far = square(1 - ctx, 1 - row, core)

        def piece(block, which):
            if which is None:
                return buf.at[block]
            return buf.at[block, pl.ds(which * half, half)]

        def make(index, block, which, where):
            return remote(index, piece(block, which), piece(block, which), send, recv, **where)

        self.first = [
            make(0, own, 0, across),
            make(1, own, 1, along),
            make(2, own, None, beside),
            make(3, own, 1, across),
            make(4, own, 0, along),
        ]
        self.second = [
            (0, make(5, self.by_x, 0, along)),
            (0, make(6, self.by_x, 0, beside)),
            (1, make(7, self.by_y, 1, across)),
            (1, make(8, self.by_y, 1, beside)),
            (3, make(9, self.by_x, 1, beside)),
            (4, make(10, self.by_y, 0, beside)),
        ]
        self.third = [
            (5, make(11, self.far, 0, beside)),
            (7, make(12, self.far, 1, beside)),
        ]
        self.all = self.first + [c for _, c in self.second] + [c for _, c in self.third]

    def start(self):
        for copy in self.first:
            copy.start()

    def relay(self):
        waited = set()
        for needs, copy in self.second:
            if needs not in waited:
                self.all[needs].wait_recv()
                waited.add(needs)
            copy.start()

    def relay_far(self):
        for needs, copy in self.third:
            self.all[needs].wait_recv()
            copy.start()

    def wait_chip(self, which):
        for index in {"own": (2,), "x": (6, 9), "y": (8, 10), "far": (11, 12)}[which]:
            self.all[index].wait_recv()

    def finish(self):
        for copy in self.all:
            copy.wait_send()


SCATTER_COPIES = 10


class GroupScatter:
    def __init__(self, part, beside_in, summed, turn_in, send, recv, base):
        ctx, row, core = place()
        half = part.shape[1] // 2
        tp = row * 2 + core
        across, along = {"ctx": 1 - ctx}, {"tp": (tp + 2) % 4}
        beside = {"tp": row * 2 + 1 - core}
        self.part, self.beside_in, self.summed, self.turn_in = part, beside_in, summed, turn_in
        self.core, self.half = core, half
        self.chips = {
            "far": (1 - ctx, 1 - row),
            "x": (1 - ctx, row),
            "y": (ctx, 1 - row),
            "own": (ctx, row),
        }
        self.slot = {name: a * 2 + b for name, (a, b) in self.chips.items()}
        self.order = ["far", "x", "y", "own"]
        self.pair = {}
        for number, name in enumerate(self.order):
            a, b = self.chips[name]
            self.pair[name] = remote(
                base + number,
                part.at[square(a, b, 1 - core)],
                beside_in.at[self.slot[name]],
                send,
                recv,
                **beside,
            )

        def turn(index, name, which, place_at, where):
            return remote(
                base + index,
                summed.at[self.slot[name], pl.ds(which * half, half)],
                turn_in.at[place_at],
                send,
                recv,
                **where,
            )

        self.far_x = turn(4, "far", 0, 0, across)
        self.far_y = turn(5, "far", 1, 1, along)
        self.near_x = turn(6, "x", 0, 2, across)
        self.near_y = turn(7, "y", 1, 3, along)
        self.last_y = turn(8, "y", 0, 4, along)
        self.last_x = turn(9, "x", 1, 5, across)
        self.all = list(self.pair.values()) + [
            self.far_x,
            self.far_y,
            self.near_x,
            self.near_y,
            self.last_y,
            self.last_x,
        ]

    def send_pair(self, name):
        self.pair[name].start()

    def add_pair(self, name):
        self.pair[name].wait_recv()
        a, b = self.chips[name]
        mine = self.part[square(a, b, self.core)].astype(F32)
        slot = self.slot[name]
        self.summed[slot] = (mine + self.beside_in[slot].astype(F32)).astype(BF)
        if name == "far":
            self.far_x.start()
            self.far_y.start()
        if name == "x":
            self.near_x.start()
        if name == "y":
            self.near_y.start()

    def turn_corner(self):
        half = self.half
        low, high = pl.ds(0, half), pl.ds(half, half)
        self.far_x.wait_recv()
        slot = self.slot["y"]
        kept = self.summed[slot, low].astype(F32) + self.turn_in[0].astype(F32)
        self.summed[slot, low] = kept.astype(BF)
        self.last_y.start()
        self.far_y.wait_recv()
        slot = self.slot["x"]
        kept = self.summed[slot, high].astype(F32) + self.turn_in[1].astype(F32)
        self.summed[slot, high] = kept.astype(BF)
        self.last_x.start()

    def total(self):
        half = self.half
        slot = self.slot["own"]
        for copy in (self.near_x, self.near_y, self.last_y, self.last_x):
            copy.wait_recv()
        low = (
            self.summed[slot, pl.ds(0, half)].astype(F32)
            + self.turn_in[2].astype(F32)
            + self.turn_in[4].astype(F32)
        )
        high = (
            self.summed[slot, pl.ds(half, half)].astype(F32)
            + self.turn_in[3].astype(F32)
            + self.turn_in[5].astype(F32)
        )
        return jnp.concatenate([low, high], 0)

    def finish(self):
        for copy in self.all:
            copy.wait_send()


class LineGather:
    def __init__(self, ways, src, buf, local_sem, send, recv, base):
        self.ways, self.at = ways, lax.axis_index("shard")
        at = self.at
        rows = src.shape[0]
        self.own = pltpu.make_async_copy(src, buf.at[pl.ds(at * rows, rows)], local_sem)

        def hop(index, block, first, to):
            target = buf.at[pl.ds(jnp.clip(block, 0, ways - 1) * rows, rows)]
            to = jnp.clip(to, 0, ways - 1)
            return remote(base + index, src if first else target, target, send, recv, shard=to)

        self.direct, self.passed = [], []
        for side, sign in ((0, 1), (1, -1)):
            place_at = at if side == 0 else ways - 1 - at
            for away in (2, 1):
                if away < ways:
                    copy = hop(3 * side + away - 1, at, True, at + sign * away)
                    self.direct.append((copy, place_at < ways - away, place_at >= away))
            if ways > 3:
                copy = hop(3 * side + 2, at - 2 * sign, False, at + sign)
                passes = (place_at >= 2) & (place_at < ways - 1)
                self.passed.append((copy, passes, place_at >= 3, self.direct[2 * side]))

    def start(self):
        self.own.start()
        for number in (0, 2, 1, 3):
            if number < len(self.direct):
                copy, sends, _ = self.direct[number]
                pl.when(sends)(copy.start)

    def step(self, k):
        if k != 2:
            return
        for copy, passes, _, needed in self.passed:

            @pl.when(passes)
            def _():
                needed[0].wait_recv()
                copy.start()

    def finish(self):
        waited = [passes for _, passes, _, _ in self.passed]
        for number, (copy, sends, receives) in enumerate(self.direct):
            if waited and number % 2 == 0:
                receives = receives & jnp.logical_not(waited[number // 2])
            pl.when(receives)(copy.wait_recv)
            pl.when(sends)(copy.wait_send)
        for copy, passes, receives, _ in self.passed:
            pl.when(receives)(copy.wait_recv)
            pl.when(passes)(copy.wait_send)
        self.own.wait()


def norm_rows(values):
    centre = values - jnp.mean(values, -1, keepdims=True)
    spread = jnp.mean(centre * centre, -1, keepdims=True)
    return centre, lax.rsqrt(spread + norm_eps)


def dot(left, right):
    return lax.dot_general(left, right, (((1,), (0,)), ((), ())), preferred_element_type=F32)


def dot_wide(left, right):
    return lax.dot_general(left, right, (((1,), (1,)), ((), ())), preferred_element_type=F32)


def dot_tall(left, right):
    return lax.dot_general(left, right, (((0,), (0,)), ((), ())), preferred_element_type=F32)


def gelu_parts(values):
    inner = math.sqrt(2.0 / math.pi) * (values + 0.044715 * (values * values * values))
    return jnp.tanh(inner)


def feed_forward_kernel(
    ways,
    gate,
    ready,
    hidden_ref,
    mods_ref,
    weights_hbm,
    *rest,
):
    if ways > 1:
        next_src, *rest = rest
    hidden_out, branch_out, normed_hbm, pre_hbm, *rest = rest
    if ways > 1:
        next_hbm, *rest = rest
    weights, gathered, pre, part, beside_in, summed, turn_in, *rest = rest
    if ways > 1:
        next_buf, *rest = rest
    local, send, recv = rest
    rows = hidden_ref.shape[0]
    if gate is not None:
        greet_signal(gate)
    if not ready:
        load = pltpu.make_async_copy(weights_hbm, weights, local.at[0])
        load.start()
    centre, scale_by = norm_rows(hidden_ref[...])
    normed = centre * scale_by * (1.0 + mods_ref[4:5, :]) + mods_ref[3:4, :]
    ctx, row, core = place()
    gathered[square(ctx, row, core)] = normed.astype(BF)
    gather = GroupGather(gathered, send, recv)
    scatter = GroupScatter(part, beside_in, summed, turn_in, send, recv, GATHER_COPIES)
    if gate is not None:
        greet_wait(gate)
    gather.start()
    if ways > 1:
        line = LineGather(
            ways, next_src, next_buf, local.at[3], send, recv, GATHER_COPIES + SCATTER_COPIES
        )
        line.start()
    if not ready:
        load.wait()
    width = pre.shape[-1]

    def up(name):
        a, b = scatter.chips[name]
        first = square(a, b, 0)
        rows_here = gathered[pl.ds(first, 2)].reshape(2 * rows, gathered.shape[2])
        value = dot(rows_here, weights[:, :width])
        pre[pl.ds(first, 2)] = value.reshape(2, rows, width)

    def down(name):
        a, b = scatter.chips[name]
        first = square(a, b, 0)
        value = pre[pl.ds(first, 2)].reshape(2 * rows, width)
        act = (0.5 * value * (1.0 + gelu_parts(value))).astype(BF)
        out = dot_wide(act, weights[:, width:]).astype(BF)
        part[pl.ds(first, 2)] = out.reshape(2, rows, out.shape[1])

    gather.wait_chip("own")
    up("own")
    gather.relay()
    gather.wait_chip("x")
    up("x")
    gather.wait_chip("y")
    up("y")
    gather.relay_far()
    gather.wait_chip("far")
    keep_normed = pltpu.make_async_copy(gathered, normed_hbm, local.at[1])
    keep_normed.start()
    up("far")
    if ways > 1:
        line.step(2)
    keep_pre = pltpu.make_async_copy(pre, pre_hbm, local.at[2])
    keep_pre.start()
    down("far")
    scatter.send_pair("far")
    down("x")
    scatter.send_pair("x")
    scatter.add_pair("far")
    down("y")
    scatter.send_pair("y")
    scatter.add_pair("x")
    down("own")
    scatter.send_pair("own")
    scatter.add_pair("y")
    scatter.add_pair("own")
    scatter.turn_corner()
    branch = scatter.total()
    branch_out[...] = branch
    hidden_out[...] = hidden_ref[...] + mods_ref[5:6, :] * branch
    gather.finish()
    scatter.finish()
    keep_normed.wait()
    keep_pre.wait()
    if ways > 1:
        line.finish()
        keep_next = pltpu.make_async_copy(next_buf, next_hbm, local.at[0])
        keep_next.start()
        keep_next.wait()


ANY = pl.BlockSpec(memory_space=pl.ANY)
VMEM = pl.BlockSpec(memory_space=pltpu.VMEM)


def line_copies(ways):
    return 6 if ways > 1 else 0


def sds(shape, dtype):
    return jax.ShapeDtypeStruct(shape, dtype)


PAIR_COPIES = 3


class RowScatter:
    def __init__(self, part, beside_in, summed, turn_in, send, recv, base):
        ctx, row, core = place()
        tp = row * 2 + core
        beside = {"tp": row * 2 + 1 - core}
        self.part, self.beside_in, self.summed, self.turn_in = part, beside_in, summed, turn_in
        self.core = core
        self.chip = {"y": 1 - row, "own": row}
        self.pair = {}
        for number, name in enumerate(("y", "own")):
            self.pair[name] = remote(
                base + number,
                part.at[self.chip[name] * 2 + 1 - core],
                beside_in.at[number],
                send,
                recv,
                **beside,
            )
        self.turn = remote(base + 2, summed, turn_in, send, recv, tp=(tp + 2) % 4)
        self.all = list(self.pair.values()) + [self.turn]

    def send_pair(self, name):
        self.pair[name].start()

    def add_pair(self, name):
        number = 0 if name == "y" else 1
        self.pair[name].wait_recv()
        mine = self.part[self.chip[name] * 2 + self.core].astype(F32)
        return mine + self.beside_in[number].astype(F32)

    def send_far(self):
        self.summed[...] = self.add_pair("y").astype(BF)
        self.turn.start()

    def total(self):
        own = self.add_pair("own")
        self.turn.wait_recv()
        return own + self.turn_in[...].astype(F32)

    def finish(self):
        for copy in self.all:
            copy.wait_send()


def attention_forward_kernel(ways, gate, hidden_ref, mods_ref, weights_hbm, *rest):
    if ways > 1:
        next_src, *rest = rest
    hidden_out, branch_out, normed_hbm, q_hbm, k_hbm, v_hbm, lse_hbm, mixed_hbm, *rest = rest
    if ways > 1:
        next_hbm, *rest = rest
    weights, gathered, q, k, v, lse, mixed, part, beside_in, summed, turn_in, *rest = rest
    if ways > 1:
        next_buf, *rest = rest
    local, send, recv = rest
    rows, model = hidden_ref.shape
    heads = q.shape[0]
    cut = heads * HEAD_DIM
    greet_signal(gate)
    load = pltpu.make_async_copy(weights_hbm, weights, local.at[0])
    load.start()
    centre, scale_by = norm_rows(hidden_ref[...])
    normed = centre * scale_by * (1.0 + mods_ref[1:2, :]) + mods_ref[0:1, :]
    ctx, row, core = place()
    gathered[square(ctx, row, core)] = normed.astype(BF)
    gather = GroupGather(gathered, send, recv)
    scatter = RowScatter(part, beside_in, summed, turn_in, send, recv, GATHER_COPIES)
    greet_wait(gate)
    gather.start()
    if ways > 1:
        line = LineGather(
            ways, next_src, next_buf, local.at[8], send, recv, GATHER_COPIES + PAIR_COPIES
        )
        line.start()
    load.wait()
    chips = {
        "own": (ctx, row),
        "x": (1 - ctx, row),
        "y": (ctx, 1 - row),
        "far": (1 - ctx, 1 - row),
    }

    def project(name):
        a, b = chips[name]
        first = square(a, b, 0)
        here = gathered[pl.ds(first, 2)].reshape(2 * rows, model)
        span = pl.ds(pl.multiple_of(first * rows, 2 * rows), 2 * rows)
        pair = dot(here, weights[:, 2 * cut :]).astype(BF)
        for head in range(heads):
            k[head, span] = pair[:, head * HEAD_DIM : (head + 1) * HEAD_DIM]
            v[head, span] = pair[:, cut + head * HEAD_DIM : cut + (head + 1) * HEAD_DIM]
        if name in ("own", "y"):
            query = (dot(here, weights[:, :cut]) * SCORE_SCALE).astype(BF)
            span = pl.ds(pl.multiple_of(b * 2 * rows, 2 * rows), 2 * rows)
            for head in range(heads):
                q[head, span] = query[:, head * HEAD_DIM : (head + 1) * HEAD_DIM]

    gather.wait_chip("own")
    project("own")
    gather.relay()
    gather.wait_chip("x")
    project("x")
    gather.wait_chip("y")
    project("y")
    gather.relay_far()
    gather.wait_chip("far")
    keep = [pltpu.make_async_copy(gathered, normed_hbm, local.at[1])]
    keep[0].start()
    project("far")
    if ways > 1:
        line.step(2)
    for number, (src, dst) in enumerate(((q, q_hbm), (k, k_hbm), (v, v_hbm))):
        keep.append(pltpu.make_async_copy(src, dst, local.at[2 + number]))
        keep[-1].start()

    def attend(name):
        b = chips[name][1]
        span = pl.ds(pl.multiple_of(b * 2 * rows, 2 * rows), 2 * rows)
        for head in range(heads):
            scores = dot_wide(q[head, span], k[head])
            top = jnp.max(scores, -1, keepdims=True)
            exponent = jnp.exp(scores - top)
            total = jnp.sum(exponent, -1, keepdims=True)
            out = dot(exponent.astype(BF), v[head]) / total
            mixed[span, head * HEAD_DIM : (head + 1) * HEAD_DIM] = out.astype(BF)
            logs = top + jnp.log(total)
            for half in range(2):
                wide = jnp.broadcast_to(logs[half * rows : (half + 1) * rows], (rows, rows))
                lse[head, pl.ds(b * 2 + half, 1)] = wide.T[0:1]

        @pl.loop(0, 2)
        def _(step):
            at = b * 2 + step
            span = pl.ds(pl.multiple_of(at * rows, rows), rows)
            part[at] = dot_wide(mixed[span, :], weights[:, cut : 2 * cut]).astype(BF)

    attend("y")
    scatter.send_pair("y")
    attend("own")
    scatter.send_pair("own")
    scatter.send_far()
    for number, (src, dst) in enumerate(((lse, lse_hbm), (mixed, mixed_hbm))):
        keep.append(pltpu.make_async_copy(src, dst, local.at[5 + number]))
        keep[-1].start()
    branch = scatter.total()
    branch_out[...] = branch
    hidden_out[...] = hidden_ref[...] + mods_ref[2:3, :] * branch
    gather.finish()
    scatter.finish()
    for copy in keep:
        copy.wait()
    if ways > 1:
        line.finish()
        keep_next = pltpu.make_async_copy(next_buf, next_hbm, local.at[0])
        keep_next.start()
        keep_next.wait()


def layer_forward_kernel(ways, last, *refs):
    hop, more = int(ways > 1), int(ways > 1 and not last)
    (
        (hidden, mods, weights),
        feed_weights,
        feed_own,
        ahead,
        outs,
        feed_block,
        feed_outs,
        ahead_block,
        scratch,
        feed_buf,
        sems,
        feed_scratch,
        ahead_buf,
        feed_sems,
    ) = split_refs(refs, 3, 1 - hop, hop, more, 8, hop, 4, more, 11, 1, 3, 6, more, 3)
    attention_forward_kernel(
        ways,
        ways,
        hidden,
        mods,
        weights,
        *feed_own,
        *outs,
        *feed_block,
        *scratch,
        *(feed_buf if hop else ()),
        *sems,
    )
    feed_forward_kernel(
        ways if more else 1,
        None,
        hop == 1,
        outs[0],
        mods,
        *(feed_weights or (None,)),
        *ahead,
        *feed_outs,
        *ahead_block,
        *feed_buf,
        *feed_scratch,
        *ahead_buf,
        *feed_sems,
    )


def layer_forward(hidden, mods, weights, feed_weights, feed_own, ahead, number):
    rows, model = hidden.shape
    cut = weights.shape[1] // 4
    heads = cut // HEAD_DIM
    ways = 1 if feed_own is None else lax.axis_size("shard")
    hop, last = ways > 1, ahead is None
    kept = [
        sds((8, rows, model), BF),
        sds((heads, 4 * rows, HEAD_DIM), BF),
        sds((heads, 8 * rows, HEAD_DIM), BF),
        sds((heads, 8 * rows, HEAD_DIM), BF),
        sds((heads, 4, rows), F32),
        sds((4 * rows, cut), BF),
    ]
    wide = sds(weights.shape, BF)
    width = weights.shape[1] // 2
    row_pair = [sds((rows, model), F32), sds((rows, model), F32)]
    feed_kept = [sds((8, rows, model), BF), sds((8, rows, width), F32)]
    outs = row_pair + kept + [wide] * hop + row_pair + feed_kept + [wide] * (hop and not last)
    out_specs = [VMEM, VMEM] + [ANY] * (len(kept) + hop)
    out_specs += [VMEM, VMEM] + [ANY] * (2 + (hop and not last))

    def buffers(copies, locals_used):
        return [
            pltpu.SemaphoreType.DMA((locals_used,)),
            pltpu.SemaphoreType.DMA((copies,)),
            pltpu.SemaphoreType.DMA((copies,)),
        ]

    scratch = [pltpu.VMEM(weights.shape, BF)]
    scratch += [pltpu.VMEM(leaf.shape, leaf.dtype) for leaf in kept]
    scratch += [
        pltpu.VMEM((4, rows, model), BF),
        pltpu.VMEM((2, rows, model), BF),
        pltpu.VMEM((rows, model), BF),
        pltpu.VMEM((rows, model), BF),
        pltpu.VMEM(weights.shape, BF),
    ]
    scratch += buffers(GATHER_COPIES + PAIR_COPIES + line_copies(ways), 9)
    scratch += [
        pltpu.VMEM((8, rows, model), BF),
        pltpu.VMEM((8, rows, width), F32),
        pltpu.VMEM((8, rows, model), BF),
        pltpu.VMEM((4, rows, model), BF),
        pltpu.VMEM((4, rows, model), BF),
        pltpu.VMEM((6, rows // 2, model), BF),
    ]
    if hop and not last:
        scratch.append(pltpu.VMEM(weights.shape, BF))
    scratch += buffers(GATHER_COPIES + SCATTER_COPIES + line_copies(ways), 4)
    given = [weights] + ([feed_own] if hop else [feed_weights]) + [ahead] * (hop and not last)
    result = pl.pallas_call(
        functools.partial(layer_forward_kernel, ways, last),
        out_shape=outs,
        in_specs=[VMEM, VMEM] + [ANY] * len(given),
        out_specs=out_specs,
        scratch_shapes=scratch,
        compiler_params=pltpu.CompilerParams(collective_id=number, has_side_effects=True),
        name="layer_forward",
    )(hidden, mods, *given)
    middle, branch, *rest = result
    saved, rest = rest[:6], rest[6:]
    if hop:
        feed_weights, rest = rest[0], rest[1:]
    hidden_new, feed_branch, normed, pre, *rest = rest
    kept_attention = (hidden, branch, *saved)
    kept_feed = (middle, normed, pre, feed_branch)
    return hidden_new, kept_attention, kept_feed, feed_weights, rest[0] if rest else None


class LineScatter:
    def __init__(self, ways, src, arrived, sums, total, send, recv, base):
        self.ways, self.at, self.src = ways, lax.axis_index("shard"), src
        self.arrived, self.sums, self.total = arrived, sums, total
        self.rows = total.shape[0]
        at = self.at

        def hop(index, part, to):
            return pltpu.make_async_remote_copy(
                src_ref=part,
                dst_ref=arrived.at[index],
                send_sem=send.at[base + index],
                recv_sem=recv.at[base + index],
                device_id={"shard": jnp.clip(to, 0, ways - 1)},
                device_id_type=MESH,
            )

        self.far, self.near, self.two, self.summed = [], [], [], []
        for side, sign in ((0, 1), (1, -1)):
            place_at = at if side == 0 else ways - 1 - at
            first = 3 * side
            passes = (place_at >= 1) & (place_at < ways - 2)
            if ways > 3:
                copy = hop(first + 2, self.block(at + 3 * sign), at + sign)
                self.far.append((copy, place_at < ways - 3, passes))
            copy = hop(first, self.block(at + sign), at + sign)
            self.near.append((copy, place_at < ways - 1, place_at >= 1))
            if ways > 2:
                plain = place_at < ways - 2
                if ways > 3:
                    plain = plain & (place_at < 1)
                    copy = hop(first + 1, sums.at[side], at + 2 * sign)
                    self.summed.append((copy, passes, first + 2, at + 2 * sign))
                copy = hop(first + 1, self.block(at + 2 * sign), at + 2 * sign)
                self.two.append((copy, plain, place_at < ways - 2, place_at >= 2))

    def block(self, number):
        return self.src.at[pl.ds(jnp.clip(number, 0, self.ways - 1) * self.rows, self.rows)]

    def step(self, k):
        if k == 1:
            for copy, sends, _ in self.far:
                pl.when(sends)(copy.start)
            for copy, sends, _, _ in self.two:
                pl.when(sends)(copy.start)
            for copy, sends, _ in self.near:
                pl.when(sends)(copy.start)
        if k == 2:
            for side, (copy, sends, slot, owner) in enumerate(self.summed):

                @pl.when(sends)
                def _():
                    self.far[side][0].wait_recv()
                    mine = self.block(owner)[...].astype(F32)
                    self.sums[side] = (mine + self.arrived[slot].astype(F32)).astype(BF)
                    copy.start()

    def finish(self):
        self.total[...] = self.block(self.at)[...].astype(F32)
        for side in range(2):
            copy, _, receives = self.near[side]

            @pl.when(receives)
            def _():
                copy.wait_recv()
                self.total[...] = self.total[...] + self.arrived[3 * side].astype(F32)

            if self.two:
                pair, _, _, receives = self.two[side]

                @pl.when(receives)
                def _():
                    pair.wait_recv()
                    self.total[...] = self.total[...] + self.arrived[3 * side + 1].astype(F32)

        for copy, sends, _ in self.far + self.near:
            pl.when(sends)(copy.wait_send)
        for copy, _, sends, _ in self.two:
            pl.when(sends)(copy.wait_send)


class Extra:
    def __init__(self, ways, sums_src, swap_src, refs, local, first_local, send, recv, base):
        self.ways = ways
        self.sums_hbm, self.swap_hbm = sums_src, swap_src
        self.refs, self.local, self.at = refs, local, first_local
        self.ready = sums_src is not None and sums_src is refs["src"]
        if sums_src is not None and not self.ready:
            self.load = pltpu.make_async_copy(sums_src, refs["src"], local.at[first_local])
        if sums_src is not None:
            self.line = LineScatter(
                ways, refs["src"], refs["arrived"], refs["sums"], refs["total"], send, recv, base
            )
            base = base + line_copies(ways)
        if swap_src is not None:
            ctx = lax.axis_index("ctx")
            self.swaps = [
                remote(base + number, src, refs["swap"].at[number], send, recv, ctx=1 - ctx)
                for number, src in enumerate(swap_src)
            ]

    def begin(self):
        if self.sums_hbm is not None and not self.ready:
            self.load.start()

    def start(self):
        if self.sums_hbm is not None:
            if not self.ready:
                self.load.wait()
            self.line.step(1)

    def start_swap(self):
        if self.swap_hbm is not None:
            for copy in self.swaps:
                copy.start()

    def step(self, k):
        if self.sums_hbm is not None and k < self.ways:
            self.line.step(k)

    def finish(self):
        keep = []
        if self.swap_hbm is not None:
            for number, copy in enumerate(self.swaps):
                copy.wait_recv()
                copy.wait_send()
            keep.append(
                pltpu.make_async_copy(
                    self.refs["swap"], self.refs["swap_out"], self.local.at[self.at + 1]
                )
            )
            keep[-1].start()
        if self.sums_hbm is not None:
            self.line.finish()
            self.refs["shard_out"][...] = self.refs["total"][...].astype(BF)
        for copy in keep:
            copy.wait()


def extra_shapes(ways, grads, swaps):
    given, outs, specs, scratch, copies = [], [], [], [], 0
    if grads is not None:
        rows, width = grads.shape[0] // ways, grads.shape[1]
        given.append(grads)
        outs.append(sds((rows, width), BF))
        specs.append(VMEM)
        scratch += [
            pltpu.VMEM(grads.shape, BF),
            pltpu.VMEM((line_copies(ways), rows, width), BF),
            pltpu.VMEM((2, rows, width), BF),
            pltpu.VMEM((rows, width), F32),
        ]
        copies += line_copies(ways)
    if swaps:
        given += list(swaps)
        shape = (len(swaps), *swaps[0].shape)
        outs.append(sds(shape, BF))
        specs.append(ANY)
        scratch.append(pltpu.VMEM(shape, BF))
        copies += len(swaps)
    return given, outs, specs, scratch, copies


def take_extra(has_sums, swaps, ins, outs, scratch):
    refs = {}
    ins, outs, scratch = list(ins), list(outs), list(scratch)
    sums_src = swap_src = None
    if has_sums:
        sums_src = ins.pop(0)
        refs["shard_out"] = outs.pop(0)
        for name in ("src", "arrived", "sums", "total"):
            refs[name] = scratch.pop(0)
    if swaps:
        swap_src = [ins.pop(0) for _ in range(swaps)]
        refs["swap_out"] = outs.pop(0)
        refs["swap"] = scratch.pop(0)
    return sums_src, swap_src, refs


def modulate_backward(grad, hidden, scale, step_ref, small_ref):
    centre, scale_by = norm_rows(hidden)
    normed = centre * scale_by
    both = grad * normed
    small_ref[0:1, :] = jnp.sum(grad, 0, keepdims=True)
    small_ref[1:2, :] = jnp.sum(both, 0, keepdims=True)
    inner = grad * (1.0 + scale)
    mean = jnp.mean(inner, -1, keepdims=True)
    along = jnp.mean(inner * normed, -1, keepdims=True)
    step_ref[...] = step_ref[...] + (inner - mean - normed * along) * scale_by


def split_refs(refs, *counts):
    out, at = [], 0
    for count in counts:
        out.append(refs[at : at + count])
        at += count
    return out


def feed_backward_kernel(ways, gate, has_sums, swaps, *refs):
    extra_in, extra_out = int(has_sums) + swaps, int(has_sums) + int(swaps > 0)
    extra_scratch = 4 * int(has_sums) + int(swaps > 0)
    ins, ex_in, outs, ex_out, scratch, ex_scratch, sems = split_refs(
        refs, 7, extra_in, 3, extra_out, 11, extra_scratch, 3
    )
    grad_ref, hidden_ref, branch_ref, mods_ref, weights_hbm, normed_hbm, pre_hbm = ins
    grad_out, small_out, dw_hbm = outs
    weights, gathered, normed, pre, act, dpre, dw, part, beside_in, summed, turn_in = scratch
    local, send, recv = sems
    rows, model = grad_ref.shape
    width = pre.shape[-1]
    greet_signal(gate)
    loads = [
        pltpu.make_async_copy(src, dst, local.at[number])
        for number, (src, dst) in enumerate(
            ((weights_hbm, weights), (pre_hbm, pre), (normed_hbm, normed))
        )
    ]
    for copy in loads:
        copy.start()
    sums_src, swap_src, ex = take_extra(has_sums, swaps, ex_in, ex_out, ex_scratch)
    extra = Extra(
        ways, sums_src, swap_src, ex, local, 4, send, recv, GATHER_COPIES + SCATTER_COPIES
    )
    extra.begin()
    ctx, row, core = place()
    grad = grad_ref[...]
    gathered[square(ctx, row, core)] = (mods_ref[5:6, :] * grad).astype(BF)
    gather = GroupGather(gathered, send, recv)
    scatter = GroupScatter(part, beside_in, summed, turn_in, send, recv, GATHER_COPIES)
    greet_wait(gate)
    gather.start()
    extra.start()
    extra.start_swap()
    small_out[2:3, :] = jnp.sum(grad * branch_ref[...], 0, keepdims=True)
    loads[0].wait()
    loads[1].wait()

    def span_of(name):
        a, b = scatter.chips[name]
        return pl.ds(pl.multiple_of(square(a, b, 0) * rows, 2 * rows), 2 * rows)

    def back(name):
        a, b = scatter.chips[name]
        here = gathered[pl.ds(square(a, b, 0), 2)].reshape(2 * rows, model)
        value = pre[pl.ds(square(a, b, 0), 2)].reshape(2 * rows, width)
        grad_act = dot(here, weights[:, width:])
        root = math.sqrt(2.0 / math.pi)
        bend = gelu_parts(value)
        act[span_of(name), :] = (0.5 * value * (1.0 + bend)).astype(BF)
        slope = 0.5 * (1.0 + bend) + 0.5 * value * (1.0 - bend * bend) * root * (
            1.0 + 3.0 * 0.044715 * value * value
        )
        dpre[span_of(name), :] = (grad_act * slope).astype(BF)

    def down(name):
        a, b = scatter.chips[name]
        out = dot_wide(dpre[span_of(name), :], weights[:, :width]).astype(BF)
        part[pl.ds(square(a, b, 0), 2)] = out.reshape(2, rows, model)

    gather.wait_chip("own")
    back("own")
    gather.relay()
    gather.wait_chip("x")
    back("x")
    gather.wait_chip("y")
    back("y")
    extra.step(2)
    gather.relay_far()
    gather.wait_chip("far")
    back("far")
    down("far")
    scatter.send_pair("far")
    down("x")
    scatter.send_pair("x")
    scatter.add_pair("far")
    down("y")
    scatter.send_pair("y")
    scatter.add_pair("x")
    down("own")
    scatter.send_pair("own")
    scatter.add_pair("y")
    scatter.add_pair("own")
    loads[2].wait()
    tile = 256

    def wide_rows(ref, at):
        return ref[:, :, pl.ds(pl.multiple_of(at * tile, tile), tile)].reshape(8 * rows, tile)

    def out_rows(at):
        return pl.ds(pl.multiple_of(at * tile, tile), tile)

    @pl.loop(0, model // tile)
    def _(at):
        dw[out_rows(at), :width] = dot_tall(wide_rows(normed, at), dpre[...]).astype(BF)

    scatter.turn_corner()

    @pl.loop(0, model // tile)
    def _(at):
        dw[out_rows(at), width:] = dot_tall(wide_rows(gathered, at), act[...]).astype(BF)

    keep = pltpu.make_async_copy(dw, dw_hbm, local.at[3])
    keep.start()
    grad_out[...] = grad
    modulate_backward(scatter.total(), hidden_ref[...], mods_ref[4:5, :], grad_out, small_out)
    gather.finish()
    scatter.finish()
    extra.finish()
    keep.wait()


class RowGather:
    def __init__(self, buf, send, recv):
        ctx, row, core = place()
        tp = row * 2 + core
        along, beside = {"tp": (tp + 2) % 4}, {"tp": row * 2 + 1 - core}
        other = (1 - row) * 2 + core
        self.to_y = remote(0, buf.at[tp], buf.at[tp], send, recv, **along)
        self.to_core = remote(1, buf.at[tp], buf.at[tp], send, recv, **beside)
        self.passed = remote(2, buf.at[other], buf.at[other], send, recv, **beside)

    def start(self):
        self.to_y.start()
        self.to_core.start()

    def relay(self):
        self.to_y.wait_recv()
        self.passed.start()

    def finish(self):
        for copy in (self.to_y, self.to_core, self.passed):
            copy.wait_send()


def attention_backward_kernel(ways, has_sums, swaps, *refs):
    extra_in, extra_out = int(has_sums) + swaps, int(has_sums) + int(swaps > 0)
    extra_scratch = 4 * int(has_sums) + int(swaps > 0)
    ins, ex_in, outs, ex_out, scratch, ex_scratch, sems = split_refs(
        refs, 11, extra_in, 3, extra_out, 18, extra_scratch, 3
    )
    grad_ref, hidden_ref, branch_ref, mods_ref = ins[:4]
    grad_out, small_out, dw_hbm = outs
    weights, normed, q, k, v, lse, mixed = scratch[:7]
    gathered, dmixed, dqh, dq, dkv, dk, dw, part, beside_in, summed, turn_in = scratch[7:]
    local, send, recv = sems
    rows, model = grad_ref.shape
    heads = q.shape[0]
    cut = heads * HEAD_DIM
    loads = [
        pltpu.make_async_copy(src, dst, local.at[number])
        for number, (src, dst) in enumerate(zip(ins[4:], scratch[:7]))
    ]
    for copy in loads:
        copy.start()
    sums_src, swap_src, ex = take_extra(has_sums, swaps, ex_in, ex_out, ex_scratch)
    extra = Extra(
        ways, sums_src, swap_src, ex, local, 8, send, recv, PAIR_COPIES + SCATTER_COPIES
    )
    extra.begin()
    ctx, row, core = place()
    grad = grad_ref[...]
    gathered[row * 2 + core] = (mods_ref[2:3, :] * grad).astype(BF)
    gather = RowGather(gathered, send, recv)
    scatter = GroupScatter(part, beside_in, summed, turn_in, send, recv, PAIR_COPIES)
    gather.start()
    extra.start()
    extra.start_swap()
    small_out[2:3, :] = jnp.sum(grad * branch_ref[...], 0, keepdims=True)
    for copy in loads:
        copy.wait()

    def attend(name, first):
        b = scatter.chips[name][1]
        span = pl.ds(pl.multiple_of(b * 2 * rows, 2 * rows), 2 * rows)
        here = gathered[pl.ds(b * 2, 2)].reshape(2 * rows, model)
        out = dot(here, weights[:, cut : 2 * cut]).astype(BF)
        for head in range(heads):
            dmixed[head, span] = out[:, head * HEAD_DIM : (head + 1) * HEAD_DIM]

        @pl.loop(0, heads)
        def _(head):
            query, upper = q[head, span], dmixed[head, span]
            scores = dot_wide(k[head], query)
            top = jnp.concatenate(
                [lse[head, pl.ds(b * 2, 1)], lse[head, pl.ds(b * 2 + 1, 1)]], 1
            )
            weight = jnp.exp(scores - top)
            grad_prob = dot_wide(v[head], upper)
            inner = jnp.sum(weight * grad_prob, 0, keepdims=True)
            grad_score = (weight * (grad_prob - inner)).astype(BF)
            grad_value = dot(weight.astype(BF), upper)
            grad_key = dot(grad_score, query)
            grad_query = dot_tall(grad_score, k[head])
            dqh[head, span] = (grad_query * SCORE_SCALE).astype(BF)
            if first:
                dk[head] = grad_key
                dk[heads + head] = grad_value
            else:
                dk[head] = dk[head] + grad_key
                dk[heads + head] = dk[heads + head] + grad_value

    gather.to_core.wait_recv()
    attend("own", True)
    gather.relay()
    extra.step(2)
    gather.passed.wait_recv()
    attend("y", False)
    for head in range(heads):
        dq[:, head * HEAD_DIM : (head + 1) * HEAD_DIM] = dqh[head]
    for head in range(2 * heads):
        dkv[:, head * HEAD_DIM : (head + 1) * HEAD_DIM] = dk[head].astype(BF)

    def span_of(name):
        a, b = scatter.chips[name]
        return pl.ds(pl.multiple_of(square(a, b, 0) * rows, 2 * rows), 2 * rows)

    def down(name):
        a, b = scatter.chips[name]
        out = dot_wide(dkv[span_of(name), :], weights[:, 2 * cut :])
        if name in ("own", "y"):
            span = pl.ds(pl.multiple_of(b * 2 * rows, 2 * rows), 2 * rows)
            out = out + dot_wide(dq[span, :], weights[:, :cut])
        part[pl.ds(square(a, b, 0), 2)] = out.astype(BF).reshape(2, rows, model)

    down("far")
    scatter.send_pair("far")
    down("x")
    scatter.send_pair("x")
    scatter.add_pair("far")
    down("y")
    scatter.send_pair("y")
    scatter.add_pair("x")
    down("own")
    scatter.send_pair("own")
    scatter.add_pair("y")
    scatter.add_pair("own")
    tile = 256

    def out_rows(at):
        return pl.ds(pl.multiple_of(at * tile, tile), tile)

    @pl.loop(0, model // tile)
    def _(at):
        lanes = out_rows(at)
        all_rows = normed[:, :, lanes].reshape(8 * rows, tile)
        dw[out_rows(at), 2 * cut :] = dot_tall(all_rows, dkv[...]).astype(BF)

    scatter.turn_corner()

    @pl.loop(0, model // tile)
    def _(at):
        lanes = out_rows(at)
        mine = normed[pl.ds(ctx * 4, 4), :, lanes].reshape(4 * rows, tile)
        dw[out_rows(at), :cut] = dot_tall(mine, dq[...]).astype(BF)
        upper = gathered[:, :, lanes].reshape(4 * rows, tile)
        dw[out_rows(at), cut : 2 * cut] = dot_tall(upper, mixed[...]).astype(BF)

    keep = pltpu.make_async_copy(dw, dw_hbm, local.at[7])
    keep.start()
    grad_out[...] = grad
    modulate_backward(scatter.total(), hidden_ref[...], mods_ref[1:2, :], grad_out, small_out)
    gather.finish()
    scatter.finish()
    extra.finish()
    keep.wait()


def layer_backward_kernel(ways, prior, *refs):
    hop, before = int(ways > 1), int(ways > 1 and prior)
    (
        (grad, mods),
        feed_in,
        attention_in,
        prior_grads,
        prior_shard,
        (grad_out, small_feed, small_attention, dw_feed, dw_attention),
        shard_before,
        shard_feed,
        swap_out,
        (middle,),
        feed_scratch,
        feed_extra,
        feed_sems,
        scratch,
        hops,
        swap_buf,
        sems,
    ) = split_refs(
        refs, 2, 5, 9, before, before, 5, before, hop, before, 1, 11, 4 * before, 3, 18, 3 * hop,
        before, 3,
    )
    hidden, branch, *rest = feed_in
    feed_backward_kernel(
        ways,
        ways,
        before == 1,
        0,
        grad,
        hidden,
        branch,
        mods,
        *rest,
        *prior_grads,
        middle,
        small_feed,
        dw_feed,
        *shard_before,
        *feed_scratch,
        *feed_extra,
        *feed_sems,
    )
    hidden, branch, *rest = attention_in
    dw = feed_scratch[6]
    sources = ((dw,) if hop else ()) + tuple(prior_shard) + tuple(shard_before)
    attention_backward_kernel(
        ways,
        hop == 1,
        2 * before,
        middle,
        hidden,
        branch,
        mods,
        *rest,
        *sources,
        grad_out,
        small_attention,
        dw_attention,
        *shard_feed,
        *swap_out,
        *scratch,
        *((dw,) if hop else ()),
        *hops,
        *swap_buf,
        *sems,
    )


def layer_backward(grad, mods, blocks, kept_attention, kept_feed, prior, number):
    rows, model = grad.shape
    attention_weights, feed_weights = blocks
    shape = attention_weights.shape
    cut, width = shape[1] // 4, shape[1] // 2
    heads = cut // HEAD_DIM
    ways = lax.axis_size("shard")
    if ways > HOP_WAYS:
        ways = 1
    hop, before = ways > 1, prior is not None
    shard = (shape[0] // ways, shape[1])
    hidden, normed, pre, branch = kept_feed
    feed_in = [hidden, branch, feed_weights, normed, pre]
    hidden, branch, *saved = kept_attention
    attention_in = [hidden, branch, attention_weights, *saved]
    outs = [sds((rows, model), F32), sds((3, model), F32), sds((3, model), F32)]
    outs += [sds(shape, BF)] * 2
    specs = [VMEM, VMEM, VMEM, ANY, ANY]
    outs += [sds(shard, BF)] * (before + hop) + [sds((2, *shard), BF)] * before
    specs += [VMEM] * (before + hop) + [ANY] * before
    line = [
        pltpu.VMEM((max(line_copies(ways), 1), *shard), BF),
        pltpu.VMEM((2, *shard), BF),
        pltpu.VMEM(shard, F32),
    ]

    def buffers(copies, locals_used):
        return [
            pltpu.SemaphoreType.DMA((locals_used,)),
            pltpu.SemaphoreType.DMA((copies,)),
            pltpu.SemaphoreType.DMA((copies,)),
        ]

    group = [
        pltpu.VMEM((8, rows, model), BF),
        pltpu.VMEM((4, rows, model), BF),
        pltpu.VMEM((4, rows, model), BF),
        pltpu.VMEM((6, rows // 2, model), BF),
    ]
    scratch = [pltpu.VMEM((rows, model), F32)]
    scratch += [
        pltpu.VMEM(shape, BF),
        pltpu.VMEM((8, rows, model), BF),
        pltpu.VMEM((8, rows, model), BF),
        pltpu.VMEM((8, rows, width), F32),
        pltpu.VMEM((8 * rows, width), BF),
        pltpu.VMEM((8 * rows, width), BF),
        pltpu.VMEM(shape, BF),
    ] + group
    if before:
        scratch += [pltpu.VMEM(shape, BF)] + line
    scratch += buffers(GATHER_COPIES + SCATTER_COPIES + line_copies(ways), 6)
    scratch += [pltpu.VMEM(leaf.shape, leaf.dtype) for leaf in [attention_weights, *saved]]
    scratch += [
        pltpu.VMEM((4, rows, model), BF),
        pltpu.VMEM((heads, 4 * rows, HEAD_DIM), BF),
        pltpu.VMEM((heads, 4 * rows, HEAD_DIM), BF),
        pltpu.VMEM((4 * rows, cut), BF),
        pltpu.VMEM((8 * rows, 2 * cut), BF),
        pltpu.VMEM((2 * heads, 8 * rows, HEAD_DIM), F32),
        pltpu.VMEM(shape, BF),
    ] + group
    if hop:
        scratch += line
    if before:
        scratch.append(pltpu.VMEM((2, *shard), BF))
    scratch += buffers(PAIR_COPIES + SCATTER_COPIES + line_copies(ways) + 2, 10)
    result = pl.pallas_call(
        functools.partial(layer_backward_kernel, ways, before),
        out_shape=outs,
        in_specs=[VMEM] * 4 + [ANY] * 3 + [VMEM] * 2 + [ANY] * (7 + 2 * before),
        out_specs=specs,
        scratch_shapes=scratch,
        compiler_params=pltpu.CompilerParams(collective_id=number, has_side_effects=True),
        name="layer_backward",
    )(grad, mods, *feed_in, *attention_in, *(prior if before else ()))
    grad, small_feed, small_attention, dw_feed, dw_attention, *rest = result
    shard_before = rest.pop(0) if before else None
    shard_feed = rest.pop(0) if hop else None
    swapped = rest.pop(0) if before else None
    return grad, small_feed, small_attention, dw_feed, dw_attention, shard_before, shard_feed, swapped


def exchange_kernel(ways, modes, pieces, by_tp, by_x, has_block, has_sums, swaps, *refs):
    count = len(modes)
    stacked = [number for number in range(count) if pieces[number] > 1]
    extra_in, extra_out = int(has_sums) + swaps, int(has_sums) + int(swaps > 0)
    extra_scratch = 4 * int(has_sums) + int(swaps > 0)
    block = int(has_block)
    parts, block_in, ex_in, outs, block_out, ex_out, scratch, stack_buf, block_buf, ex_scratch, sems = (
        split_refs(
            refs,
            sum(pieces),
            block,
            extra_in,
            count,
            block,
            extra_out,
            3 * count,
            len(stacked),
            block,
            extra_scratch,
            3,
        )
    )
    held, arrived, far = scratch[:count], scratch[count : 2 * count], scratch[2 * count :]
    local, send, recv = sems
    sums_src, swap_src, ex = take_extra(has_sums, swaps, ex_in, ex_out, ex_scratch)
    stages = 2 * int(by_tp) + int(by_x)
    used = count * (stages + ways - 1)
    extra = Extra(ways, sums_src, swap_src, ex, local, 1, send, recv, used)
    if has_sums:
        used += line_copies(ways)
    used += swaps
    extra.begin()
    ctx, row, core = place()
    tp = row * 2 + core
    at = lax.axis_index("shard")
    barrier = pltpu.get_barrier_semaphore()
    sides = [{"tp": row * 2 + 1 - core}, {"tp": (tp + 2) % 4}] if by_tp else []
    if by_x:
        sides.append({"ctx": 1 - ctx})
    greeted = sides if by_x or not swaps else sides + [{"ctx": 1 - ctx}]
    for where in greeted:
        pl.semaphore_signal(barrier, inc=1, device_id=where, device_id_type=MESH)
    for away in range(1, ways):
        pl.semaphore_signal(
            barrier, inc=1, device_id={"shard": (at + away) % ways}, device_id_type=MESH
        )
    pl.semaphore_wait(barrier, len(greeted) + ways - 1)
    copies = []
    now, taken = [], 0
    for number in range(count):
        given = parts[taken : taken + pieces[number]]
        taken += pieces[number]
        if number in stacked:
            into, first = stack_buf[stacked.index(number)], 0
            for ref in given:
                into[first : first + ref.shape[0]] = ref[...]
                first += ref.shape[0]
            given = [into]
        now.append(given[0])
    for stage, where in enumerate(sides):
        here = []
        for number in range(count):
            here.append(
                remote(
                    number * stages + stage,
                    now[number],
                    arrived[number].at[stage],
                    send,
                    recv,
                    **where,
                )
            )
            here[-1].start()
        if stage == 0:
            if has_block:
                line = LineGather(
                    ways, block_in[0], block_buf[0], local.at[0], send, recv, used
                )
                line.start()
            extra.start()
            extra.start_swap()
        for number in range(count):
            here[number].wait_recv()
            both = now[number][...].astype(F32) + arrived[number][stage].astype(F32)
            held[number][stage] = both.astype(held[number].dtype)
            now[number] = held[number].at[stage]
        copies += here
        if stage == 1:
            extra.step(2)
    if has_block:
        line.step(2)
    base = count * stages
    for number, mode in enumerate(modes):
        if mode == "gather":
            far[number][at] = now[number][...].astype(far[number].dtype)
            now[number] = far[number].at[at]
    waits = []
    for number, mode in enumerate(modes):
        for away in range(1, ways):
            to = (at + away) % ways
            copy = remote(
                base + number * (ways - 1) + away - 1,
                now[number].at[to] if mode == "scatter" else now[number],
                far[number].at[at],
                send,
                recv,
                shard=to,
            )
            copy.start()
            waits.append(copy)
        if mode != "gather":
            far[number][at] = now[number][at] if mode == "scatter" else now[number][...]
    for k in range(3, ways):
        if has_block:
            line.step(k)
        extra.step(k)
    for copy in waits:
        copy.wait_recv()
    for number, mode in enumerate(modes):
        if mode == "gather":
            outs[number][...] = far[number][...].astype(F32)
            continue
        total = far[number][0].astype(F32)
        for index in range(1, ways):
            total = total + far[number][index].astype(F32)
        outs[number][...] = total
    for copy in copies + waits:
        copy.wait_send()
    extra.finish()
    if has_block:
        line.finish()
        keep = pltpu.make_async_copy(block_buf[0], block_out[0], local.at[0])
        keep.start()
        keep.wait()


def stacked_shape(arrays):
    return (sum(array.shape[0] for array in arrays), *arrays[0].shape[1:])


def exchange(parts, number, by_tp=True, by_x=False, block=None, grads=None, swaps=()):
    ways = lax.axis_size("shard")
    if ways > HOP_WAYS:
        return exchange_plain(parts, by_tp, by_x)
    stages = 2 * int(by_tp) + int(by_x)
    modes, pieces = [mode for _, mode in parts], [len(arrays) for arrays, _ in parts]
    outs, held, arrived, far, stacks, given = [], [], [], [], [], []
    for arrays, mode in parts:
        whole, dtype = stacked_shape(arrays), arrays[0].dtype
        one = whole[1:] if mode == "scatter" else whole
        full = (ways, *one)
        given += list(arrays)
        outs.append(sds(full if mode == "gather" else one, F32))
        held.append(pltpu.VMEM((max(stages, 1), *whole), dtype))
        arrived.append(pltpu.VMEM((max(stages, 1), *whole), dtype))
        far.append(pltpu.VMEM(full, BF if mode == "gather" else dtype))
        if len(arrays) > 1:
            stacks.append(pltpu.VMEM(whole, dtype))
    specs = [VMEM] * len(outs)
    block_specs, block_scratch, inputs = [], [], len(given)
    copies = len(parts) * (stages + ways - 1)
    if block is not None:
        shape = (ways * block.shape[0], block.shape[1])
        given.append(block)
        block_specs.append(ANY)
        block_scratch.append(pltpu.VMEM(shape, BF))
        outs.append(sds(shape, BF))
        copies += line_copies(ways)
    more, more_outs, more_specs, more_scratch, more_copies = extra_shapes(ways, grads, swaps)
    copies += more_copies
    return pl.pallas_call(
        functools.partial(
            exchange_kernel,
            ways,
            tuple(modes),
            tuple(pieces),
            by_tp,
            by_x,
            block is not None,
            grads is not None,
            len(swaps),
        ),
        out_shape=outs + more_outs,
        in_specs=[VMEM] * inputs + block_specs + [ANY] * len(more),
        out_specs=specs + block_specs + more_specs,
        scratch_shapes=held
        + arrived
        + far
        + stacks
        + block_scratch
        + more_scratch
        + [
            pltpu.SemaphoreType.DMA((3,)),
            pltpu.SemaphoreType.DMA((copies,)),
            pltpu.SemaphoreType.DMA((copies,)),
        ],
        compiler_params=pltpu.CompilerParams(collective_id=number, has_side_effects=True),
        name="exchange",
    )(*given, *more)


def exchange_plain(parts, by_tp, by_x):
    near = (("ctx",) if by_x else ()) + (("tp",) if by_tp else ())
    outs = []
    for arrays, mode in parts:
        wide = jnp.concatenate(arrays, 0).astype(F32)
        if mode == "gather":
            outs.append(lax.all_gather(lax.psum(wide, near), "shard", axis=0))
        elif mode == "scatter":
            total = lax.psum_scatter(wide, "shard", scatter_dimension=0, tiled=True)
            outs.append(lax.psum(total, near)[0])
        else:
            outs.append(lax.psum(wide, ("shard",) + near))
    return outs


def loss_kernel(
    loss_scale,
    hidden_ref,
    ends_ref,
    head_ref,
    target_ref,
    weight_ref,
    grad_out,
    small_out,
    head_out,
    loss_out,
):
    hidden, head = hidden_ref[...], head_ref[...]
    shift, scale = ends_ref[0:1, :], ends_ref[1:2, :]
    centre, scale_by = norm_rows(hidden)
    normed = (centre * scale_by * (1.0 + scale) + shift).astype(BF)
    misfit = dot_wide(normed, head) - target_ref[...]
    weighted = weight_ref[...] * misfit
    rows = jnp.sum(weighted * misfit, 1, keepdims=True)
    loss_out[...] = jnp.sum(rows, 0, keepdims=True) * loss_scale
    grad_pred = (2.0 * loss_scale * weighted).astype(BF)
    head_out[...] = dot_tall(grad_pred, normed)
    grad_out[...] = jnp.zeros_like(grad_out)
    modulate_backward(dot(grad_pred, head), hidden, scale, grad_out, small_out)


def loss_and_grad(hidden, ends, head_rows, target, weight, loss_scale):
    rows, model = hidden.shape
    return pl.pallas_call(
        functools.partial(loss_kernel, loss_scale),
        out_shape=[
            sds((rows, model), F32),
            sds((2, model), F32),
            sds(head_rows.shape, F32),
            sds((1, 1), F32),
        ],
        in_specs=[VMEM] * 5,
        out_specs=[VMEM] * 4,
        name="loss_and_grad",
    )(hidden, ends, head_rows, target, weight)


def spread(values, at, axis_size):
    full = jnp.zeros((*values.shape[:-1], axis_size), values.dtype)
    return lax.dynamic_update_slice_in_dim(full, values, at, values.ndim - 1)


def silu_grad(values):
    gate = jax.nn.sigmoid(values)
    return gate * (1.0 + values * (1.0 - gate))


def local(
    noised,
    velocity,
    labels,
    time_ids,
    stem,
    stem_mean,
    stem_square,
    modulation,
    modulation_mean,
    modulation_square,
    attention_in,
    attention_in_mean,
    attention_in_square,
    attention_out,
    attention_out_mean,
    attention_out_square,
    feedforward,
    feedforward_mean,
    feedforward_square,
):
    tensor_ways = lax.axis_size("tp")
    shard_ways = lax.axis_size("shard")
    own_latent = lax.axis_index("shard")
    own_ctx = lax.axis_index("ctx")
    own_tp = lax.axis_index("tp")
    owned = stem.shape[1]
    first_owned = (own_latent * tensor_ways + lax.axis_index("tp")) * owned

    def own_columns(values):
        return lax.dynamic_slice_in_dim(values, first_owned, owned, values.ndim - 1)

    stem_low = stem.astype(jnp.bfloat16)
    class_own, time_in_own, time_out_own, shift_own, scale_own, patch_own, head_own = split_stem(
        stem_low
    )
    modulation_low = modulation.astype(jnp.bfloat16)
    mine = (jnp.arange(shard_ways) == own_latent).astype(jnp.float32)[:, None]
    packed_ids = mine * jnp.concatenate([labels, time_ids]).astype(jnp.float32)[None, :]
    ids_wide = jnp.pad(packed_ids, ((0, 0), (0, 126)))
    (ids_all,) = exchange([([ids_wide], "sum")], 10, by_tp=False)
    all_labels, all_times = ids_all[:, 0].astype(jnp.int32), ids_all[:, 1].astype(jnp.int32)
    latents = all_labels.shape[0]
    features = time_features(all_times).astype(jnp.bfloat16)
    time_pre = jnp.dot(features, time_in_own, preferred_element_type=jnp.float32)
    time_hidden_own = jax.nn.silu(time_pre).astype(jnp.bfloat16)
    hidden_half = feedforward.shape[3] // lax.axis_size("ctx")
    feed_low = lax.dynamic_slice_in_dim(feedforward, own_ctx * hidden_half, hidden_half, 3).astype(
        jnp.bfloat16
    )
    in_low, out_low = attention_in.astype(jnp.bfloat16), attention_out.astype(jnp.bfloat16)
    hops = shard_ways <= HOP_WAYS
    own_blocks, blocks = [], []
    for layer_at in range(LAYERS):
        parts = [in_low[layer_at, 0], out_low[layer_at], in_low[layer_at, 1], in_low[layer_at, 2]]
        own_blocks.append(jnp.concatenate(parts, 1))
        own_blocks.append(jnp.concatenate([feed_low[layer_at, 0], feed_low[layer_at, 1]], 1))
    to_send = jnp.concatenate([time_hidden_own, patch_own, head_own], 0)
    half_rows = own_blocks[0].shape[0] // 2
    exchanged = exchange(
        [([spread(to_send, first_owned, D)], "sum")], 11, block=own_blocks[0][:half_rows]
    )
    packed = exchanged[0].astype(jnp.bfloat16)
    time_hidden = packed[:latents]
    patch_in, head_rows = packed[latents : latents + PDIM], packed[latents + PDIM :]
    onehot = (all_labels[:, None] == jnp.arange(CLASSES)[None, :]).astype(jnp.bfloat16)
    condition = jnp.dot(time_hidden, time_out_own, preferred_element_type=jnp.float32) + jnp.dot(
        onehot, class_own, preferred_element_type=jnp.float32
    )
    gated_own = jax.nn.silu(condition).astype(jnp.bfloat16)
    mod_part = jnp.einsum(
        "bd,lde->ble", gated_own, modulation_low, preferred_element_type=jnp.float32
    )
    first_half = exchanged[1:]
    mod_part = mod_part.reshape(latents, LAYERS * 6, D)
    exchanged = exchange(
        [([mod_part], "scatter"), ([spread(gated_own, first_owned, D)], "sum")],
        12,
        block=own_blocks[0][half_rows:],
    )
    layer_mods = exchanged[0].reshape(LAYERS, 6, D)
    gated = exchanged[1].astype(jnp.bfloat16)
    if hops:
        both = [part.reshape(shard_ways, half_rows, -1) for part in (first_half[0], exchanged[2])]
        blocks.append(jnp.concatenate(both, 1).reshape(shard_ways * 2 * half_rows, -1))
    else:
        for block in own_blocks:
            blocks.append(lax.all_gather(block, "shard", axis=0, tiled=True))
    end_own = jnp.stack(
        [
            jnp.dot(gated, shift_own, preferred_element_type=jnp.float32),
            jnp.dot(gated, scale_own, preferred_element_type=jnp.float32),
        ],
        1,
    )
    (end_mods,) = exchange([([spread(end_own, first_owned, D)], "scatter")], 13)

    pieces = patchify(noised)[0]
    rows_here = noised.shape[2] // PATCH
    first_row = (own_ctx * tensor_ways + lax.axis_index("tp")) * rows_here
    embedded = jnp.dot(pieces, patch_in, preferred_element_type=jnp.float32)
    hidden = embedded + positions(first_row, rows_here, noised.shape[3] // PATCH, D)
    saved, weights = [], blocks[0]
    for layer_at in range(LAYERS):
        final = layer_at + 1 == LAYERS
        feed_own, ahead, feed_weights = None, None, None
        if hops:
            feed_own = own_blocks[2 * layer_at + 1]
            ahead = None if final else own_blocks[2 * layer_at + 2]
        else:
            weights, feed_weights = blocks[2 * layer_at : 2 * layer_at + 2]
        hidden, kept_attention, kept_feed, feed_weights, following = layer_forward(
            hidden, layer_mods[layer_at], weights, feed_weights, feed_own, ahead, 2 + int(final)
        )
        saved.append((kept_attention, kept_feed, (weights, feed_weights)))
        weights = following

    target_rows = patchify(velocity)[0].astype(jnp.float32)
    weighting = 0.5 + time_ids.astype(jnp.float32)[:, None] / STEPS
    loss_scale = 1.0 / (shard_ways * PATCHES * PDIM)
    grad_hidden, grad_ends, grad_head, loss_local = loss_and_grad(
        hidden, end_mods, head_rows, target_rows, weighting, loss_scale
    )
    loss_local = loss_local[0, 0]

    small = [None] * (2 * LAYERS)
    shards, others = [None] * (2 * LAYERS), [None] * (2 * LAYERS)
    prior = None
    for layer_at in reversed(range(LAYERS)):
        kept_attention, kept_feed, pair = saved[layer_at]
        one, two = 2 * layer_at, 2 * layer_at + 1
        (
            grad_hidden,
            small[two],
            small[one],
            feed_grads,
            grads,
            shard_before,
            shards[two],
            swapped,
        ) = layer_backward(
            grad_hidden,
            layer_mods[layer_at],
            pair,
            kept_attention,
            kept_feed,
            prior,
            5 + int(prior is None),
        )
        if prior is not None:
            shards[one + 2] = shard_before
            others[two + 2], others[one + 2] = swapped[0], swapped[1]
        if hops:
            prior = (grads, shards[two])
        else:
            for half, local_grads in ((one, grads), (two, feed_grads)):
                shards[half] = lax.psum_scatter(
                    local_grads, "shard", scatter_dimension=0, tiled=True
                )
                others[half] = lax.ppermute(shards[half], "ctx", [(0, 1), (1, 0)])
    grad_embed = grad_hidden.astype(jnp.bfloat16)
    grad_patch = jnp.einsum("pf,pd->fd", pieces, grad_embed, preferred_element_type=jnp.float32)

    pixel = jnp.concatenate([grad_patch, grad_head], 0).astype(jnp.bfloat16)
    pixel = pixel.reshape(2 * PDIM, shard_ways, -1).transpose(1, 0, 2)
    result = exchange(
        [(small + [grad_ends], "gather"), ([pixel], "scatter")],
        14,
        by_x=True,
        grads=grads,
        swaps=[shards[1]],
    )
    small, pixel = result[0], result[1]
    if hops:
        shards[0], others[1] = result[2], result[3][0]
    grad_mod = small[:, : 6 * LAYERS].reshape(latents, LAYERS, 6 * D)
    grad_ends = small[:, 6 * LAYERS :]
    ends_here = own_columns(grad_ends)
    gated_part = jnp.dot(
        ends_here[:, 0], shift_own.astype(jnp.float32).T, precision=highest
    ) + jnp.dot(ends_here[:, 1], scale_own.astype(jnp.float32).T, precision=highest)
    result = exchange([([gated_part], "sum")], 15, swaps=[shards[0]])
    if hops:
        others[0] = result[1][0]
    grad_gated = own_columns(result[0]) + jnp.einsum(
        "ble,lde->bd", grad_mod, modulation_low.astype(jnp.float32), precision=highest
    )
    grad_condition = grad_gated * silu_grad(condition)
    time_part = jnp.dot(grad_condition, time_out_own.astype(jnp.float32).T, precision=highest)
    (grad_time_hidden,) = exchange([([time_part], "sum")], 16)
    grad_time_hidden = own_columns(grad_time_hidden)
    grad_time_pre = grad_time_hidden * silu_grad(time_pre)
    gated_wide = gated.astype(jnp.float32)
    grad_ends_own = lax.dynamic_slice_in_dim(pixel, own_tp * owned, owned, 1)
    shard_stem = jnp.concatenate(
        [
            jnp.dot(onehot.astype(jnp.float32).T, grad_condition, precision=highest),
            jnp.dot(features.astype(jnp.float32).T, grad_time_pre, precision=highest),
            jnp.dot(time_hidden.astype(jnp.float32).T, grad_condition, precision=highest),
            jnp.dot(gated_wide.T, ends_here[:, 0], precision=highest),
            jnp.dot(gated_wide.T, ends_here[:, 1], precision=highest),
            grad_ends_own,
        ],
        0,
    )
    shard_modulation = jnp.einsum(
        "bd,ble->lde", gated_own.astype(jnp.float32), grad_mod, precision=highest
    )
    cut = attention_in.shape[3]
    shard_in, shard_out, shard_hidden = [], [], []
    for layer_at in range(LAYERS):
        own, other = shards[2 * layer_at], others[2 * layer_at]
        both = own.astype(jnp.float32) + other.astype(jnp.float32)
        shard_out.append(both[:, cut : 2 * cut])
        shard_in.append(
            jnp.stack([both[:, number * cut : (number + 1) * cut] for number in (0, 2, 3)])
        )
        own, other = shards[2 * layer_at + 1], others[2 * layer_at + 1]
        low, high = jnp.where(own_ctx == 0, own, other), jnp.where(own_ctx == 0, other, own)
        shard_hidden.append(
            jnp.stack(
                [
                    jnp.concatenate([low[:, :hidden_half], high[:, :hidden_half]], 1),
                    jnp.concatenate([low[:, hidden_half:], high[:, hidden_half:]], 1),
                ]
            )
        )
    shard_in, shard_out = jnp.stack(shard_in), jnp.stack(shard_out)
    shard_hidden = jnp.stack(shard_hidden).astype(jnp.float32)
    flat_mod = grad_mod.reshape(latents, -1)
    wide_own = gated_own.astype(jnp.float32)
    modulation_square_sum = jnp.sum(
        jnp.dot(wide_own, wide_own.T, precision=highest)
        * jnp.dot(flat_mod, flat_mod.T, precision=highest)
    )
    squares = (
        jnp.sum(shard_stem * shard_stem)
        + modulation_square_sum
        + jnp.sum(shard_in * shard_in)
        + jnp.sum(shard_out * shard_out)
        + jnp.sum(shard_hidden * shard_hidden)
    )
    squares = jnp.where(own_ctx == 0, squares, jnp.zeros((), jnp.float32))
    sums = jnp.stack([squares, loss_local])[:, None] * jnp.ones((1, 128), jnp.float32)
    (sums,) = exchange([([sums], "sum")], 17, by_x=True)
    square_total, train_loss = sums[0, 0], sums[1, 0]
    total_norm = jnp.sqrt(square_total)
    factor = clip_level / jnp.maximum(total_norm, clip_level)
    stem_out = adam_update(stem, stem_mean, stem_square, shard_stem, factor)
    mod_out = adam_update(modulation, modulation_mean, modulation_square, shard_modulation, factor)
    in_out = adam_update(attention_in, attention_in_mean, attention_in_square, shard_in, factor)
    proj_out = adam_update(
        attention_out, attention_out_mean, attention_out_square, shard_out, factor
    )
    feed_out = adam_update(feedforward, feedforward_mean, feedforward_square, shard_hidden, factor)
    return (
        train_loss,
        total_norm,
        stem_out[0],
        stem_out[1],
        stem_out[2],
        stem_out[3],
        mod_out[0],
        mod_out[1],
        mod_out[2],
        mod_out[3],
        in_out[0],
        in_out[1],
        in_out[2],
        in_out[3],
        proj_out[0],
        proj_out[1],
        proj_out[2],
        proj_out[3],
        feed_out[0],
        feed_out[1],
        feed_out[2],
        feed_out[3],
    )


def solution(mesh):
    placed = (
        P("shard", None, ("ctx", "tp"), None),
        P("shard", None, ("ctx", "tp"), None),
        P("shard"),
        P("shard"),
        P(None, ("shard", "tp")),
        P(None, ("shard", "tp")),
        P(None, ("shard", "tp")),
        P(None, ("shard", "tp"), None),
        P(None, ("shard", "tp"), None),
        P(None, ("shard", "tp"), None),
        P(None, None, "shard", "tp"),
        P(None, None, "shard", "tp"),
        P(None, None, "shard", "tp"),
        P(None, "shard", "tp"),
        P(None, "shard", "tp"),
        P(None, "shard", "tp"),
        P(None, None, "shard", "tp"),
        P(None, None, "shard", "tp"),
        P(None, None, "shard", "tp"),
    )
    return jax.shard_map(
        local,
        mesh=mesh,
        in_specs=placed,
        out_specs=(
            P(),
            P(),
            P(None, ("shard", "tp")),
            P(None, ("shard", "tp")),
            P(None, ("shard", "tp")),
            P(None, ("shard", "tp")),
            P(None, ("shard", "tp"), None),
            P(None, ("shard", "tp"), None),
            P(None, ("shard", "tp"), None),
            P(None, ("shard", "tp"), None),
            P(None, None, "shard", "tp"),
            P(None, None, "shard", "tp"),
            P(None, None, "shard", "tp"),
            P(None, None, "shard", "tp"),
            P(None, "shard", "tp"),
            P(None, "shard", "tp"),
            P(None, "shard", "tp"),
            P(None, "shard", "tp"),
            P(None, None, "shard", "tp"),
            P(None, None, "shard", "tp"),
            P(None, None, "shard", "tp"),
            P(None, None, "shard", "tp"),
        ),
        check_vma=False,
    )
```

```python
import functools
import math

import jax
import jax.numpy as jnp
from jax import lax
from jax.experimental import pallas as pl
from jax.experimental.pallas import tpu as pltpu
from jax.sharding import PartitionSpec as P

D = 768
HEAD_DIM = 64
CLASSES = 1000
FREQ = 256
PATCH = 2
STEPS = 1000
LAYERS = 4
PATCHES = 1024
PDIM = 16


norm_eps = 1e-06
clip_level = 0.5
learn_rate = 0.01
beta_first = 0.5
beta_second = 0.5
adam_eps = 1e-08
weight_decay = 0.1
bias_fix = 0.875
highest = lax.Precision.HIGHEST


def layer_norm(values):
    centre = values - jnp.mean(values, -1, keepdims=True)
    spread = jnp.mean(centre * centre, -1, keepdims=True)
    return centre * lax.rsqrt(spread + norm_eps)


def modulate(values, shift_rows, scale_rows):
    return layer_norm(values) * (1.0 + scale_rows) + shift_rows


def gelu_tanh(values):
    return jax.nn.gelu(values, approximate=True)


def patchify(image_in):
    latent_count, channels, height, columns = image_in.shape
    shaped = image_in.reshape(
        latent_count, channels, height // PATCH, PATCH, columns // PATCH, PATCH
    )
    shaped = shaped.transpose(0, 2, 4, 3, 5, 1)
    return shaped.reshape(
        latent_count, height // PATCH * (columns // PATCH), PATCH * PATCH * channels
    )


def positions(first_row, height, columns, model_width):
    quarter = model_width // 4
    omegas = jnp.exp(-math.log(10000.0) * jnp.arange(quarter).astype(jnp.float32) / quarter)
    row_angle = (first_row + jnp.arange(height)).astype(jnp.float32)[:, None] * omegas[None, :]
    col_angle = jnp.arange(columns).astype(jnp.float32)[:, None] * omegas[None, :]
    row_part = jnp.concatenate([jnp.sin(row_angle), jnp.cos(row_angle)], -1)
    col_part = jnp.concatenate([jnp.sin(col_angle), jnp.cos(col_angle)], -1)
    grid_table = jnp.concatenate(
        [
            jnp.broadcast_to(col_part[None], (height, columns, 2 * quarter)),
            jnp.broadcast_to(row_part[:, None], (height, columns, 2 * quarter)),
        ],
        -1,
    )
    return grid_table.reshape(height * columns, model_width)


def time_features(step_ids):
    half_width = FREQ // 2
    frequencies = jnp.exp(
        -math.log(10000.0) * jnp.arange(half_width).astype(jnp.float32) / half_width
    )
    angles = step_ids.astype(jnp.float32)[:, None] * frequencies[None, :]
    return jnp.concatenate([jnp.cos(angles), jnp.sin(angles)], -1)


def split_stem(stem_rows):
    bounds = [CLASSES, FREQ, D, D, D, PDIM, PDIM]
    pieces_out = []
    offset = 0
    for extent in bounds:
        pieces_out.append(stem_rows[offset : offset + extent])
        offset = offset + extent
    return pieces_out


def adam_update(master, first_moment, second_moment, gradient, factor):
    clipped = gradient * factor
    first_new = beta_first * first_moment + (1.0 - beta_first) * clipped
    second_new = beta_second * second_moment + (1.0 - beta_second) * clipped * clipped
    direction = first_new / bias_fix / (jnp.sqrt(second_new / bias_fix) + adam_eps)
    master_new = master - learn_rate * (direction + weight_decay * master)
    return (master_new, first_new, second_new, master_new.astype(jnp.bfloat16))


GROUP = ("ctx", "tp")
OWNERS = ("shard", "tp")
EVERY = ("shard", "ctx", "tp")
HOP_WAYS = 4


MESH = pl.DeviceIdType.MESH
BF = jnp.bfloat16
F32 = jnp.float32
SCORE_SCALE = HEAD_DIM**-0.5


def place():
    ctx, tp = lax.axis_index("ctx"), lax.axis_index("tp")
    core = tp % 2
    row = tp // 2
    return ctx, row, core


def square(ctx, row, core):
    return ctx * 4 + row * 2 + core


def remote(index, src, dst, send, recv, **where):
    return pltpu.make_async_remote_copy(
        src_ref=src,
        dst_ref=dst,
        send_sem=send.at[index],
        recv_sem=recv.at[index],
        device_id=where,
        device_id_type=MESH,
    )


def greet_signal(shard_ways):
    ctx, row, core = place()
    barrier = pltpu.get_barrier_semaphore()
    tp = row * 2 + core
    pl.semaphore_signal(barrier, inc=1, device_id={"ctx": 1 - ctx}, device_id_type=MESH)
    pl.semaphore_signal(barrier, inc=1, device_id={"tp": (tp + 2) % 4}, device_id_type=MESH)
    pl.semaphore_signal(
        barrier, inc=1, device_id={"tp": row * 2 + 1 - core}, device_id_type=MESH
    )
    if shard_ways > 1:
        line_signal(shard_ways)


def line_signal(ways):
    barrier = pltpu.get_barrier_semaphore()
    at = lax.axis_index("shard")
    for away in (1, 2):

        @pl.when(at >= away)
        def _():
            pl.semaphore_signal(
                barrier, inc=1, device_id={"shard": at - away}, device_id_type=MESH
            )

        @pl.when(at < ways - away)
        def _():
            pl.semaphore_signal(
                barrier, inc=1, device_id={"shard": at + away}, device_id_type=MESH
            )


def greet_wait(shard_ways):
    barrier = pltpu.get_barrier_semaphore()
    if shard_ways == 1:
        pl.semaphore_wait(barrier, 3)
        return
    at = lax.axis_index("shard")
    for own in range(shard_ways):
        near = min(own, 2) + min(shard_ways - 1 - own, 2)

        @pl.when(at == own)
        def _():
            pl.semaphore_wait(barrier, 3 + near)


GATHER_COPIES = 13


class GroupGather:
    def __init__(self, buf, send, recv):
        ctx, row, core = place()
        half = buf.shape[1] // 2
        tp = row * 2 + core
        across, along = {"ctx": 1 - ctx}, {"tp": (tp + 2) % 4}
        beside = {"tp": row * 2 + 1 - core}
        own = square(ctx, row, core)
        self.by_x, self.by_y = square(1 - ctx, row, core), square(ctx, 1 - row, core)
        self.far = square(1 - ctx, 1 - row, core)

        def piece(block, which):
            if which is None:
                return buf.at[block]
            return buf.at[block, pl.ds(which * half, half)]

        def make(index, block, which, where):
            return remote(index, piece(block, which), piece(block, which), send, recv, **where)

        self.first = [
            make(0, own, 0, across),
            make(1, own, 1, along),
            make(2, own, None, beside),
            make(3, own, 1, across),
            make(4, own, 0, along),
        ]
        self.second = [
            (0, make(5, self.by_x, 0, along)),
            (0, make(6, self.by_x, 0, beside)),
            (1, make(7, self.by_y, 1, across)),
            (1, make(8, self.by_y, 1, beside)),
            (3, make(9, self.by_x, 1, beside)),
            (4, make(10, self.by_y, 0, beside)),
        ]
        self.third = [
            (5, make(11, self.far, 0, beside)),
            (7, make(12, self.far, 1, beside)),
        ]
        self.all = self.first + [c for _, c in self.second] + [c for _, c in self.third]

    def start(self):
        for copy in self.first:
            copy.start()

    def relay(self):
        waited = set()
        for needs, copy in self.second:
            if needs not in waited:
                self.all[needs].wait_recv()
                waited.add(needs)
            copy.start()

    def relay_far(self):
        for needs, copy in self.third:
            self.all[needs].wait_recv()
            copy.start()

    def wait_chip(self, which):
        for index in {"own": (2,), "x": (6, 9), "y": (8, 10), "far": (11, 12)}[which]:
            self.all[index].wait_recv()

    def finish(self):
        for copy in self.all:
            copy.wait_send()


SCATTER_COPIES = 10


class GroupScatter:
    def __init__(self, part, beside_in, summed, turn_in, send, recv, base):
        ctx, row, core = place()
        half = part.shape[1] // 2
        tp = row * 2 + core
        across, along = {"ctx": 1 - ctx}, {"tp": (tp + 2) % 4}
        beside = {"tp": row * 2 + 1 - core}
        self.part, self.beside_in, self.summed, self.turn_in = part, beside_in, summed, turn_in
        self.core, self.half = core, half
        self.chips = {
            "far": (1 - ctx, 1 - row),
            "x": (1 - ctx, row),
            "y": (ctx, 1 - row),
            "own": (ctx, row),
        }
        self.slot = {name: a * 2 + b for name, (a, b) in self.chips.items()}
        self.order = ["far", "x", "y", "own"]
        self.pair = {}
        for number, name in enumerate(self.order):
            a, b = self.chips[name]
            self.pair[name] = remote(
                base + number,
                part.at[square(a, b, 1 - core)],
                beside_in.at[self.slot[name]],
                send,
                recv,
                **beside,
            )

        def turn(index, name, which, place_at, where):
            return remote(
                base + index,
                summed.at[self.slot[name], pl.ds(which * half, half)],
                turn_in.at[place_at],
                send,
                recv,
                **where,
            )

        self.far_x = turn(4, "far", 0, 0, across)
        self.far_y = turn(5, "far", 1, 1, along)
        self.near_x = turn(6, "x", 0, 2, across)
        self.near_y = turn(7, "y", 1, 3, along)
        self.last_y = turn(8, "y", 0, 4, along)
        self.last_x = turn(9, "x", 1, 5, across)
        self.all = list(self.pair.values()) + [
            self.far_x,
            self.far_y,
            self.near_x,
            self.near_y,
            self.last_y,
            self.last_x,
        ]

    def send_pair(self, name):
        self.pair[name].start()

    def add_pair(self, name):
        self.pair[name].wait_recv()
        a, b = self.chips[name]
        mine = self.part[square(a, b, self.core)].astype(F32)
        slot = self.slot[name]
        self.summed[slot] = (mine + self.beside_in[slot].astype(F32)).astype(BF)
        if name == "far":
            self.far_x.start()
            self.far_y.start()
        if name == "x":
            self.near_x.start()
        if name == "y":
            self.near_y.start()

    def turn_corner(self):
        half = self.half
        low, high = pl.ds(0, half), pl.ds(half, half)
        self.far_x.wait_recv()
        slot = self.slot["y"]
        kept = self.summed[slot, low].astype(F32) + self.turn_in[0].astype(F32)
        self.summed[slot, low] = kept.astype(BF)
        self.last_y.start()
        self.far_y.wait_recv()
        slot = self.slot["x"]
        kept = self.summed[slot, high].astype(F32) + self.turn_in[1].astype(F32)
        self.summed[slot, high] = kept.astype(BF)
        self.last_x.start()

    def total(self):
        half = self.half
        slot = self.slot["own"]
        for copy in (self.near_x, self.near_y, self.last_y, self.last_x):
            copy.wait_recv()
        low = (
            self.summed[slot, pl.ds(0, half)].astype(F32)
            + self.turn_in[2].astype(F32)
            + self.turn_in[4].astype(F32)
        )
        high = (
            self.summed[slot, pl.ds(half, half)].astype(F32)
            + self.turn_in[3].astype(F32)
            + self.turn_in[5].astype(F32)
        )
        return jnp.concatenate([low, high], 0)

    def finish(self):
        for copy in self.all:
            copy.wait_send()


class LineGather:
    def __init__(self, ways, src, buf, local_sem, send, recv, base):
        self.ways, self.at = ways, lax.axis_index("shard")
        at = self.at
        rows = src.shape[0]
        self.own = pltpu.make_async_copy(src, buf.at[pl.ds(at * rows, rows)], local_sem)

        def hop(index, block, first, to):
            target = buf.at[pl.ds(jnp.clip(block, 0, ways - 1) * rows, rows)]
            to = jnp.clip(to, 0, ways - 1)
            return remote(base + index, src if first else target, target, send, recv, shard=to)

        self.direct, self.passed = [], []
        for side, sign in ((0, 1), (1, -1)):
            place_at = at if side == 0 else ways - 1 - at
            for away in (2, 1):
                if away < ways:
                    copy = hop(3 * side + away - 1, at, True, at + sign * away)
                    self.direct.append((copy, place_at < ways - away, place_at >= away))
            if ways > 3:
                copy = hop(3 * side + 2, at - 2 * sign, False, at + sign)
                passes = (place_at >= 2) & (place_at < ways - 1)
                self.passed.append((copy, passes, place_at >= 3, self.direct[2 * side]))

    def start(self):
        self.own.start()
        for number in (0, 2, 1, 3):
            if number < len(self.direct):
                copy, sends, _ = self.direct[number]
                pl.when(sends)(copy.start)

    def step(self, k):
        if k != 2:
            return
        for copy, passes, _, needed in self.passed:

            @pl.when(passes)
            def _():
                needed[0].wait_recv()
                copy.start()

    def finish(self):
        waited = [passes for _, passes, _, _ in self.passed]
        for number, (copy, sends, receives) in enumerate(self.direct):
            if waited and number % 2 == 0:
                receives = receives & jnp.logical_not(waited[number // 2])
            pl.when(receives)(copy.wait_recv)
            pl.when(sends)(copy.wait_send)
        for copy, passes, receives, _ in self.passed:
            pl.when(receives)(copy.wait_recv)
            pl.when(passes)(copy.wait_send)
        self.own.wait()


def norm_rows(values):
    centre = values - jnp.mean(values, -1, keepdims=True)
    spread = jnp.mean(centre * centre, -1, keepdims=True)
    return centre, lax.rsqrt(spread + norm_eps)


def dot(left, right):
    return lax.dot_general(left, right, (((1,), (0,)), ((), ())), preferred_element_type=F32)


def dot_wide(left, right):
    return lax.dot_general(left, right, (((1,), (1,)), ((), ())), preferred_element_type=F32)


def dot_tall(left, right):
    return lax.dot_general(left, right, (((0,), (0,)), ((), ())), preferred_element_type=F32)


def gelu_parts(values):
    inner = math.sqrt(2.0 / math.pi) * (values + 0.044715 * (values * values * values))
    return jnp.tanh(inner)


def feed_forward_kernel(
    ways,
    gate,
    ready,
    hidden_ref,
    mods_ref,
    weights_hbm,
    *rest,
):
    if ways > 1:
        next_src, *rest = rest
    hidden_out, branch_out, normed_hbm, pre_hbm, *rest = rest
    if ways > 1:
        next_hbm, *rest = rest
    weights, gathered, pre, part, beside_in, summed, turn_in, *rest = rest
    if ways > 1:
        next_buf, *rest = rest
    local, send, recv = rest
    rows = hidden_ref.shape[0]
    if gate is not None:
        greet_signal(gate)
    if not ready:
        load = pltpu.make_async_copy(weights_hbm, weights, local.at[0])
        load.start()
    centre, scale_by = norm_rows(hidden_ref[...])
    normed = centre * scale_by * (1.0 + mods_ref[4:5, :]) + mods_ref[3:4, :]
    ctx, row, core = place()
    gathered[square(ctx, row, core)] = normed.astype(BF)
    gather = GroupGather(gathered, send, recv)
    scatter = GroupScatter(part, beside_in, summed, turn_in, send, recv, GATHER_COPIES)
    if gate is not None:
        greet_wait(gate)
    gather.start()
    if ways > 1:
        line = LineGather(
            ways, next_src, next_buf, local.at[3], send, recv, GATHER_COPIES + SCATTER_COPIES
        )
        line.start()
    if not ready:
        load.wait()
    width = pre.shape[-1]

    def up(name):
        a, b = scatter.chips[name]
        first = square(a, b, 0)
        rows_here = gathered[pl.ds(first, 2)].reshape(2 * rows, gathered.shape[2])
        value = dot(rows_here, weights[:, :width])
        pre[pl.ds(first, 2)] = value.reshape(2, rows, width)

    def down(name):
        a, b = scatter.chips[name]
        first = square(a, b, 0)
        value = pre[pl.ds(first, 2)].reshape(2 * rows, width)
        act = (0.5 * value * (1.0 + gelu_parts(value))).astype(BF)
        out = dot_wide(act, weights[:, width:]).astype(BF)
        part[pl.ds(first, 2)] = out.reshape(2, rows, out.shape[1])

    gather.wait_chip("own")
    up("own")
    gather.relay()
    gather.wait_chip("x")
    up("x")
    gather.wait_chip("y")
    up("y")
    gather.relay_far()
    gather.wait_chip("far")
    keep_normed = pltpu.make_async_copy(gathered, normed_hbm, local.at[1])
    keep_normed.start()
    up("far")
    if ways > 1:
        line.step(2)
    keep_pre = pltpu.make_async_copy(pre, pre_hbm, local.at[2])
    keep_pre.start()
    down("far")
    scatter.send_pair("far")
    down("x")
    scatter.send_pair("x")
    scatter.add_pair("far")
    down("y")
    scatter.send_pair("y")
    scatter.add_pair("x")
    down("own")
    scatter.send_pair("own")
    scatter.add_pair("y")
    scatter.add_pair("own")
    scatter.turn_corner()
    branch = scatter.total()
    branch_out[...] = branch
    hidden_out[...] = hidden_ref[...] + mods_ref[5:6, :] * branch
    gather.finish()
    scatter.finish()
    keep_normed.wait()
    keep_pre.wait()
    if ways > 1:
        line.finish()
        keep_next = pltpu.make_async_copy(next_buf, next_hbm, local.at[0])
        keep_next.start()
        keep_next.wait()


ANY = pl.BlockSpec(memory_space=pl.ANY)
VMEM = pl.BlockSpec(memory_space=pltpu.VMEM)


def line_copies(ways):
    return 6 if ways > 1 else 0


def sds(shape, dtype):
    return jax.ShapeDtypeStruct(shape, dtype)


PAIR_COPIES = 3


class RowScatter:
    def __init__(self, part, beside_in, summed, turn_in, send, recv, base):
        ctx, row, core = place()
        tp = row * 2 + core
        beside = {"tp": row * 2 + 1 - core}
        self.part, self.beside_in, self.summed, self.turn_in = part, beside_in, summed, turn_in
        self.core = core
        self.chip = {"y": 1 - row, "own": row}
        self.pair = {}
        for number, name in enumerate(("y", "own")):
            self.pair[name] = remote(
                base + number,
                part.at[self.chip[name] * 2 + 1 - core],
                beside_in.at[number],
                send,
                recv,
                **beside,
            )
        self.turn = remote(base + 2, summed, turn_in, send, recv, tp=(tp + 2) % 4)
        self.all = list(self.pair.values()) + [self.turn]

    def send_pair(self, name):
        self.pair[name].start()

    def add_pair(self, name):
        number = 0 if name == "y" else 1
        self.pair[name].wait_recv()
        mine = self.part[self.chip[name] * 2 + self.core].astype(F32)
        return mine + self.beside_in[number].astype(F32)

    def send_far(self):
        self.summed[...] = self.add_pair("y").astype(BF)
        self.turn.start()

    def total(self):
        own = self.add_pair("own")
        self.turn.wait_recv()
        return own + self.turn_in[...].astype(F32)

    def finish(self):
        for copy in self.all:
            copy.wait_send()


def attention_forward_kernel(ways, gate, hidden_ref, mods_ref, weights_hbm, *rest):
    if ways > 1:
        next_src, *rest = rest
    hidden_out, branch_out, normed_hbm, q_hbm, k_hbm, v_hbm, lse_hbm, mixed_hbm, *rest = rest
    if ways > 1:
        next_hbm, *rest = rest
    weights, gathered, q, k, v, lse, mixed, part, beside_in, summed, turn_in, *rest = rest
    if ways > 1:
        next_buf, *rest = rest
    local, send, recv = rest
    rows, model = hidden_ref.shape
    heads = q.shape[0]
    cut = heads * HEAD_DIM
    greet_signal(gate)
    load = pltpu.make_async_copy(weights_hbm, weights, local.at[0])
    load.start()
    centre, scale_by = norm_rows(hidden_ref[...])
    normed = centre * scale_by * (1.0 + mods_ref[1:2, :]) + mods_ref[0:1, :]
    ctx, row, core = place()
    gathered[square(ctx, row, core)] = normed.astype(BF)
    gather = GroupGather(gathered, send, recv)
    scatter = RowScatter(part, beside_in, summed, turn_in, send, recv, GATHER_COPIES)
    greet_wait(gate)
    gather.start()
    if ways > 1:
        line = LineGather(
            ways, next_src, next_buf, local.at[8], send, recv, GATHER_COPIES + PAIR_COPIES
        )
        line.start()
    load.wait()
    chips = {
        "own": (ctx, row),
        "x": (1 - ctx, row),
        "y": (ctx, 1 - row),
        "far": (1 - ctx, 1 - row),
    }

    def project(name):
        a, b = chips[name]
        first = square(a, b, 0)
        here = gathered[pl.ds(first, 2)].reshape(2 * rows, model)
        span = pl.ds(pl.multiple_of(first * rows, 2 * rows), 2 * rows)
        pair = dot(here, weights[:, 2 * cut :]).astype(BF)
        for head in range(heads):
            k[head, span] = pair[:, head * HEAD_DIM : (head + 1) * HEAD_DIM]
            v[head, span] = pair[:, cut + head * HEAD_DIM : cut + (head + 1) * HEAD_DIM]
        if name in ("own", "y"):
            query = (dot(here, weights[:, :cut]) * SCORE_SCALE).astype(BF)
            span = pl.ds(pl.multiple_of(b * 2 * rows, 2 * rows), 2 * rows)
            for head in range(heads):
                q[head, span] = query[:, head * HEAD_DIM : (head + 1) * HEAD_DIM]

    gather.wait_chip("own")
    project("own")
    gather.relay()
    gather.wait_chip("x")
    project("x")
    gather.wait_chip("y")
    project("y")
    gather.relay_far()
    gather.wait_chip("far")
    keep = [pltpu.make_async_copy(gathered, normed_hbm, local.at[1])]
    keep[0].start()
    project("far")
    if ways > 1:
        line.step(2)
    for number, (src, dst) in enumerate(((q, q_hbm), (k, k_hbm), (v, v_hbm))):
        keep.append(pltpu.make_async_copy(src, dst, local.at[2 + number]))
        keep[-1].start()

    def attend(name):
        b = chips[name][1]
        span = pl.ds(pl.multiple_of(b * 2 * rows, 2 * rows), 2 * rows)
        for head in range(heads):
            scores = dot_wide(q[head, span], k[head])
            top = jnp.max(scores, -1, keepdims=True)
            exponent = jnp.exp(scores - top)
            total = jnp.sum(exponent, -1, keepdims=True)
            out = dot(exponent.astype(BF), v[head]) / total
            mixed[span, head * HEAD_DIM : (head + 1) * HEAD_DIM] = out.astype(BF)
            logs = top + jnp.log(total)
            for half in range(2):
                wide = jnp.broadcast_to(logs[half * rows : (half + 1) * rows], (rows, rows))
                lse[head, pl.ds(b * 2 + half, 1)] = wide.T[0:1]

        @pl.loop(0, 2)
        def _(step):
            at = b * 2 + step
            span = pl.ds(pl.multiple_of(at * rows, rows), rows)
            part[at] = dot_wide(mixed[span, :], weights[:, cut : 2 * cut]).astype(BF)

    attend("y")
    scatter.send_pair("y")
    attend("own")
    scatter.send_pair("own")
    scatter.send_far()
    for number, (src, dst) in enumerate(((lse, lse_hbm), (mixed, mixed_hbm))):
        keep.append(pltpu.make_async_copy(src, dst, local.at[5 + number]))
        keep[-1].start()
    branch = scatter.total()
    branch_out[...] = branch
    hidden_out[...] = hidden_ref[...] + mods_ref[2:3, :] * branch
    gather.finish()
    scatter.finish()
    for copy in keep:
        copy.wait()
    if ways > 1:
        line.finish()
        keep_next = pltpu.make_async_copy(next_buf, next_hbm, local.at[0])
        keep_next.start()
        keep_next.wait()


def layer_forward_kernel(ways, last, *refs):
    hop, more = int(ways > 1), int(ways > 1 and not last)
    (
        (hidden, mods, weights),
        feed_weights,
        feed_own,
        ahead,
        outs,
        feed_block,
        feed_outs,
        ahead_block,
        scratch,
        feed_buf,
        sems,
        feed_scratch,
        ahead_buf,
        feed_sems,
    ) = split_refs(refs, 3, 1 - hop, hop, more, 8, hop, 4, more, 11, 1, 3, 6, more, 3)
    attention_forward_kernel(
        ways,
        ways,
        hidden,
        mods,
        weights,
        *feed_own,
        *outs,
        *feed_block,
        *scratch,
        *(feed_buf if hop else ()),
        *sems,
    )
    feed_forward_kernel(
        ways if more else 1,
        None,
        hop == 1,
        outs[0],
        mods,
        *(feed_weights or (None,)),
        *ahead,
        *feed_outs,
        *ahead_block,
        *feed_buf,
        *feed_scratch,
        *ahead_buf,
        *feed_sems,
    )


def layer_forward(hidden, mods, weights, feed_weights, feed_own, ahead, number):
    rows, model = hidden.shape
    cut = weights.shape[1] // 4
    heads = cut // HEAD_DIM
    ways = 1 if feed_own is None else lax.axis_size("shard")
    hop, last = ways > 1, ahead is None
    kept = [
        sds((8, rows, model), BF),
        sds((heads, 4 * rows, HEAD_DIM), BF),
        sds((heads, 8 * rows, HEAD_DIM), BF),
        sds((heads, 8 * rows, HEAD_DIM), BF),
        sds((heads, 4, rows), F32),
        sds((4 * rows, cut), BF),
    ]
    wide = sds(weights.shape, BF)
    width = weights.shape[1] // 2
    row_pair = [sds((rows, model), F32), sds((rows, model), F32)]
    feed_kept = [sds((8, rows, model), BF), sds((8, rows, width), F32)]
    outs = row_pair + kept + [wide] * hop + row_pair + feed_kept + [wide] * (hop and not last)
    out_specs = [VMEM, VMEM] + [ANY] * (len(kept) + hop)
    out_specs += [VMEM, VMEM] + [ANY] * (2 + (hop and not last))

    def buffers(copies, locals_used):
        return [
            pltpu.SemaphoreType.DMA((locals_used,)),
            pltpu.SemaphoreType.DMA((copies,)),
            pltpu.SemaphoreType.DMA((copies,)),
        ]

    scratch = [pltpu.VMEM(weights.shape, BF)]
    scratch += [pltpu.VMEM(leaf.shape, leaf.dtype) for leaf in kept]
    scratch += [
        pltpu.VMEM((4, rows, model), BF),
        pltpu.VMEM((2, rows, model), BF),
        pltpu.VMEM((rows, model), BF),
        pltpu.VMEM((rows, model), BF),
        pltpu.VMEM(weights.shape, BF),
    ]
    scratch += buffers(GATHER_COPIES + PAIR_COPIES + line_copies(ways), 9)
    scratch += [
        pltpu.VMEM((8, rows, model), BF),
        pltpu.VMEM((8, rows, width), F32),
        pltpu.VMEM((8, rows, model), BF),
        pltpu.VMEM((4, rows, model), BF),
        pltpu.VMEM((4, rows, model), BF),
        pltpu.VMEM((6, rows // 2, model), BF),
    ]
    if hop and not last:
        scratch.append(pltpu.VMEM(weights.shape, BF))
    scratch += buffers(GATHER_COPIES + SCATTER_COPIES + line_copies(ways), 4)
    given = [weights] + ([feed_own] if hop else [feed_weights]) + [ahead] * (hop and not last)
    result = pl.pallas_call(
        functools.partial(layer_forward_kernel, ways, last),
        out_shape=outs,
        in_specs=[VMEM, VMEM] + [ANY] * len(given),
        out_specs=out_specs,
        scratch_shapes=scratch,
        compiler_params=pltpu.CompilerParams(collective_id=number, has_side_effects=True),
        name="layer_forward",
    )(hidden, mods, *given)
    middle, branch, *rest = result
    saved, rest = rest[:6], rest[6:]
    if hop:
        feed_weights, rest = rest[0], rest[1:]
    hidden_new, feed_branch, normed, pre, *rest = rest
    kept_attention = (hidden, branch, *saved)
    kept_feed = (middle, normed, pre, feed_branch)
    return hidden_new, kept_attention, kept_feed, feed_weights, rest[0] if rest else None


class LineScatter:
    def __init__(self, ways, src, arrived, sums, total, send, recv, base):
        self.ways, self.at, self.src = ways, lax.axis_index("shard"), src
        self.arrived, self.sums, self.total = arrived, sums, total
        self.rows = total.shape[0]
        at = self.at

        def hop(index, part, to):
            return pltpu.make_async_remote_copy(
                src_ref=part,
                dst_ref=arrived.at[index],
                send_sem=send.at[base + index],
                recv_sem=recv.at[base + index],
                device_id={"shard": jnp.clip(to, 0, ways - 1)},
                device_id_type=MESH,
            )

        self.far, self.near, self.two, self.summed = [], [], [], []
        for side, sign in ((0, 1), (1, -1)):
            place_at = at if side == 0 else ways - 1 - at
            first = 3 * side
            passes = (place_at >= 1) & (place_at < ways - 2)
            if ways > 3:
                copy = hop(first + 2, self.block(at + 3 * sign), at + sign)
                self.far.append((copy, place_at < ways - 3, passes))
            copy = hop(first, self.block(at + sign), at + sign)
            self.near.append((copy, place_at < ways - 1, place_at >= 1))
            if ways > 2:
                plain = place_at < ways - 2
                if ways > 3:
                    plain = plain & (place_at < 1)
                    copy = hop(first + 1, sums.at[side], at + 2 * sign)
                    self.summed.append((copy, passes, first + 2, at + 2 * sign))
                copy = hop(first + 1, self.block(at + 2 * sign), at + 2 * sign)
                self.two.append((copy, plain, place_at < ways - 2, place_at >= 2))

    def block(self, number):
        return self.src.at[pl.ds(jnp.clip(number, 0, self.ways - 1) * self.rows, self.rows)]

    def step(self, k):
        if k == 1:
            for copy, sends, _ in self.far:
                pl.when(sends)(copy.start)
            for copy, sends, _, _ in self.two:
                pl.when(sends)(copy.start)
            for copy, sends, _ in self.near:
                pl.when(sends)(copy.start)
        if k == 2:
            for side, (copy, sends, slot, owner) in enumerate(self.summed):

                @pl.when(sends)
                def _():
                    self.far[side][0].wait_recv()
                    mine = self.block(owner)[...].astype(F32)
                    self.sums[side] = (mine + self.arrived[slot].astype(F32)).astype(BF)
                    copy.start()

    def finish(self):
        self.total[...] = self.block(self.at)[...].astype(F32)
        for side in range(2):
            copy, _, receives = self.near[side]

            @pl.when(receives)
            def _():
                copy.wait_recv()
                self.total[...] = self.total[...] + self.arrived[3 * side].astype(F32)

            if self.two:
                pair, _, _, receives = self.two[side]

                @pl.when(receives)
                def _():
                    pair.wait_recv()
                    self.total[...] = self.total[...] + self.arrived[3 * side + 1].astype(F32)

        for copy, sends, _ in self.far + self.near:
            pl.when(sends)(copy.wait_send)
        for copy, _, sends, _ in self.two:
            pl.when(sends)(copy.wait_send)


class Extra:
    def __init__(self, ways, sums_src, swap_src, refs, local, first_local, send, recv, base):
        self.ways = ways
        self.sums_hbm, self.swap_hbm = sums_src, swap_src
        self.refs, self.local, self.at = refs, local, first_local
        self.ready = sums_src is not None and sums_src is refs["src"]
        if sums_src is not None and not self.ready:
            self.load = pltpu.make_async_copy(sums_src, refs["src"], local.at[first_local])
        if sums_src is not None:
            self.line = LineScatter(
                ways, refs["src"], refs["arrived"], refs["sums"], refs["total"], send, recv, base
            )
            base = base + line_copies(ways)
        if swap_src is not None:
            ctx = lax.axis_index("ctx")
            self.swaps = [
                remote(base + number, src, refs["swap"].at[number], send, recv, ctx=1 - ctx)
                for number, src in enumerate(swap_src)
            ]

    def begin(self):
        if self.sums_hbm is not None and not self.ready:
            self.load.start()

    def start(self):
        if self.sums_hbm is not None:
            if not self.ready:
                self.load.wait()
            self.line.step(1)

    def start_swap(self):
        if self.swap_hbm is not None:
            for copy in self.swaps:
                copy.start()

    def step(self, k):
        if self.sums_hbm is not None and k < self.ways:
            self.line.step(k)

    def finish(self):
        keep = []
        if self.swap_hbm is not None:
            for number, copy in enumerate(self.swaps):
                copy.wait_recv()
                copy.wait_send()
            keep.append(
                pltpu.make_async_copy(
                    self.refs["swap"], self.refs["swap_out"], self.local.at[self.at + 1]
                )
            )
            keep[-1].start()
        if self.sums_hbm is not None:
            self.line.finish()
            self.refs["shard_out"][...] = self.refs["total"][...].astype(BF)
        for copy in keep:
            copy.wait()


def extra_shapes(ways, grads, swaps):
    given, outs, specs, scratch, copies = [], [], [], [], 0
    if grads is not None:
        rows, width = grads.shape[0] // ways, grads.shape[1]
        given.append(grads)
        outs.append(sds((rows, width), BF))
        specs.append(VMEM)
        scratch += [
            pltpu.VMEM(grads.shape, BF),
            pltpu.VMEM((line_copies(ways), rows, width), BF),
            pltpu.VMEM((2, rows, width), BF),
            pltpu.VMEM((rows, width), F32),
        ]
        copies += line_copies(ways)
    if swaps:
        given += list(swaps)
        shape = (len(swaps), *swaps[0].shape)
        outs.append(sds(shape, BF))
        specs.append(ANY)
        scratch.append(pltpu.VMEM(shape, BF))
        copies += len(swaps)
    return given, outs, specs, scratch, copies


def take_extra(has_sums, swaps, ins, outs, scratch):
    refs = {}
    ins, outs, scratch = list(ins), list(outs), list(scratch)
    sums_src = swap_src = None
    if has_sums:
        sums_src = ins.pop(0)
        refs["shard_out"] = outs.pop(0)
        for name in ("src", "arrived", "sums", "total"):
            refs[name] = scratch.pop(0)
    if swaps:
        swap_src = [ins.pop(0) for _ in range(swaps)]
        refs["swap_out"] = outs.pop(0)
        refs["swap"] = scratch.pop(0)
    return sums_src, swap_src, refs


def modulate_backward(grad, hidden, scale, step_ref, small_ref):
    centre, scale_by = norm_rows(hidden)
    normed = centre * scale_by
    both = grad * normed
    small_ref[0:1, :] = jnp.sum(grad, 0, keepdims=True)
    small_ref[1:2, :] = jnp.sum(both, 0, keepdims=True)
    inner = grad * (1.0 + scale)
    mean = jnp.mean(inner, -1, keepdims=True)
    along = jnp.mean(inner * normed, -1, keepdims=True)
    step_ref[...] = step_ref[...] + (inner - mean - normed * along) * scale_by


def split_refs(refs, *counts):
    out, at = [], 0
    for count in counts:
        out.append(refs[at : at + count])
        at += count
    return out


def feed_backward_kernel(ways, gate, has_sums, swaps, *refs):
    extra_in, extra_out = int(has_sums) + swaps, int(has_sums) + int(swaps > 0)
    extra_scratch = 4 * int(has_sums) + int(swaps > 0)
    ins, ex_in, outs, ex_out, scratch, ex_scratch, sems = split_refs(
        refs, 7, extra_in, 3, extra_out, 11, extra_scratch, 3
    )
    grad_ref, hidden_ref, branch_ref, mods_ref, weights_hbm, normed_hbm, pre_hbm = ins
    grad_out, small_out, dw_hbm = outs
    weights, gathered, normed, pre, act, dpre, dw, part, beside_in, summed, turn_in = scratch
    local, send, recv = sems
    rows, model = grad_ref.shape
    width = pre.shape[-1]
    greet_signal(gate)
    loads = [
        pltpu.make_async_copy(src, dst, local.at[number])
        for number, (src, dst) in enumerate(
            ((weights_hbm, weights), (pre_hbm, pre), (normed_hbm, normed))
        )
    ]
    for copy in loads:
        copy.start()
    sums_src, swap_src, ex = take_extra(has_sums, swaps, ex_in, ex_out, ex_scratch)
    extra = Extra(
        ways, sums_src, swap_src, ex, local, 4, send, recv, GATHER_COPIES + SCATTER_COPIES
    )
    extra.begin()
    ctx, row, core = place()
    grad = grad_ref[...]
    gathered[square(ctx, row, core)] = (mods_ref[5:6, :] * grad).astype(BF)
    gather = GroupGather(gathered, send, recv)
    scatter = GroupScatter(part, beside_in, summed, turn_in, send, recv, GATHER_COPIES)
    greet_wait(gate)
    gather.start()
    extra.start()
    extra.start_swap()
    small_out[2:3, :] = jnp.sum(grad * branch_ref[...], 0, keepdims=True)
    loads[0].wait()
    loads[1].wait()

    def span_of(name):
        a, b = scatter.chips[name]
        return pl.ds(pl.multiple_of(square(a, b, 0) * rows, 2 * rows), 2 * rows)

    def back(name):
        a, b = scatter.chips[name]
        here = gathered[pl.ds(square(a, b, 0), 2)].reshape(2 * rows, model)
        value = pre[pl.ds(square(a, b, 0), 2)].reshape(2 * rows, width)
        grad_act = dot(here, weights[:, width:])
        root = math.sqrt(2.0 / math.pi)
        bend = gelu_parts(value)
        act[span_of(name), :] = (0.5 * value * (1.0 + bend)).astype(BF)
        slope = 0.5 * (1.0 + bend) + 0.5 * value * (1.0 - bend * bend) * root * (
            1.0 + 3.0 * 0.044715 * value * value
        )
        dpre[span_of(name), :] = (grad_act * slope).astype(BF)

    def down(name):
        a, b = scatter.chips[name]
        out = dot_wide(dpre[span_of(name), :], weights[:, :width]).astype(BF)
        part[pl.ds(square(a, b, 0), 2)] = out.reshape(2, rows, model)

    gather.wait_chip("own")
    back("own")
    gather.relay()
    gather.wait_chip("x")
    back("x")
    gather.wait_chip("y")
    back("y")
    extra.step(2)
    gather.relay_far()
    gather.wait_chip("far")
    back("far")
    down("far")
    scatter.send_pair("far")
    down("x")
    scatter.send_pair("x")
    scatter.add_pair("far")
    down("y")
    scatter.send_pair("y")
    scatter.add_pair("x")
    down("own")
    scatter.send_pair("own")
    scatter.add_pair("y")
    scatter.add_pair("own")
    loads[2].wait()
    tile = 256

    def wide_rows(ref, at):
        return ref[:, :, pl.ds(pl.multiple_of(at * tile, tile), tile)].reshape(8 * rows, tile)

    def out_rows(at):
        return pl.ds(pl.multiple_of(at * tile, tile), tile)

    @pl.loop(0, model // tile)
    def _(at):
        dw[out_rows(at), :width] = dot_tall(wide_rows(normed, at), dpre[...]).astype(BF)

    scatter.turn_corner()

    @pl.loop(0, model // tile)
    def _(at):
        dw[out_rows(at), width:] = dot_tall(wide_rows(gathered, at), act[...]).astype(BF)

    keep = pltpu.make_async_copy(dw, dw_hbm, local.at[3])
    keep.start()
    grad_out[...] = grad
    modulate_backward(scatter.total(), hidden_ref[...], mods_ref[4:5, :], grad_out, small_out)
    gather.finish()
    scatter.finish()
    extra.finish()
    keep.wait()


class RowGather:
    def __init__(self, buf, send, recv):
        ctx, row, core = place()
        tp = row * 2 + core
        along, beside = {"tp": (tp + 2) % 4}, {"tp": row * 2 + 1 - core}
        other = (1 - row) * 2 + core
        self.to_y = remote(0, buf.at[tp], buf.at[tp], send, recv, **along)
        self.to_core = remote(1, buf.at[tp], buf.at[tp], send, recv, **beside)
        self.passed = remote(2, buf.at[other], buf.at[other], send, recv, **beside)

    def start(self):
        self.to_y.start()
        self.to_core.start()

    def relay(self):
        self.to_y.wait_recv()
        self.passed.start()

    def finish(self):
        for copy in (self.to_y, self.to_core, self.passed):
            copy.wait_send()


def attention_backward_kernel(ways, has_sums, swaps, *refs):
    extra_in, extra_out = int(has_sums) + swaps, int(has_sums) + int(swaps > 0)
    extra_scratch = 4 * int(has_sums) + int(swaps > 0)
    ins, ex_in, outs, ex_out, scratch, ex_scratch, sems = split_refs(
        refs, 11, extra_in, 3, extra_out, 18, extra_scratch, 3
    )
    grad_ref, hidden_ref, branch_ref, mods_ref = ins[:4]
    grad_out, small_out, dw_hbm = outs
    weights, normed, q, k, v, lse, mixed = scratch[:7]
    gathered, dmixed, dqh, dq, dkv, dk, dw, part, beside_in, summed, turn_in = scratch[7:]
    local, send, recv = sems
    rows, model = grad_ref.shape
    heads = q.shape[0]
    cut = heads * HEAD_DIM
    loads = [
        pltpu.make_async_copy(src, dst, local.at[number])
        for number, (src, dst) in enumerate(zip(ins[4:], scratch[:7]))
    ]
    for copy in loads:
        copy.start()
    sums_src, swap_src, ex = take_extra(has_sums, swaps, ex_in, ex_out, ex_scratch)
    extra = Extra(
        ways, sums_src, swap_src, ex, local, 8, send, recv, PAIR_COPIES + SCATTER_COPIES
    )
    extra.begin()
    ctx, row, core = place()
    grad = grad_ref[...]
    gathered[row * 2 + core] = (mods_ref[2:3, :] * grad).astype(BF)
    gather = RowGather(gathered, send, recv)
    scatter = GroupScatter(part, beside_in, summed, turn_in, send, recv, PAIR_COPIES)
    gather.start()
    extra.start()
    extra.start_swap()
    small_out[2:3, :] = jnp.sum(grad * branch_ref[...], 0, keepdims=True)
    for copy in loads:
        copy.wait()

    def attend(name, first):
        b = scatter.chips[name][1]
        span = pl.ds(pl.multiple_of(b * 2 * rows, 2 * rows), 2 * rows)
        here = gathered[pl.ds(b * 2, 2)].reshape(2 * rows, model)
        out = dot(here, weights[:, cut : 2 * cut]).astype(BF)
        for head in range(heads):
            dmixed[head, span] = out[:, head * HEAD_DIM : (head + 1) * HEAD_DIM]

        @pl.loop(0, heads)
        def _(head):
            query, upper = q[head, span], dmixed[head, span]
            scores = dot_wide(k[head], query)
            top = jnp.concatenate(
                [lse[head, pl.ds(b * 2, 1)], lse[head, pl.ds(b * 2 + 1, 1)]], 1
            )
            weight = jnp.exp(scores - top)
            grad_prob = dot_wide(v[head], upper)
            inner = jnp.sum(weight * grad_prob, 0, keepdims=True)
            grad_score = (weight * (grad_prob - inner)).astype(BF)
            grad_value = dot(weight.astype(BF), upper)
            grad_key = dot(grad_score, query)
            grad_query = dot_tall(grad_score, k[head])
            dqh[head, span] = (grad_query * SCORE_SCALE).astype(BF)
            if first:
                dk[head] = grad_key
                dk[heads + head] = grad_value
            else:
                dk[head] = dk[head] + grad_key
                dk[heads + head] = dk[heads + head] + grad_value

    gather.to_core.wait_recv()
    attend("own", True)
    gather.relay()
    extra.step(2)
    gather.passed.wait_recv()
    attend("y", False)
    for head in range(heads):
        dq[:, head * HEAD_DIM : (head + 1) * HEAD_DIM] = dqh[head]
    for head in range(2 * heads):
        dkv[:, head * HEAD_DIM : (head + 1) * HEAD_DIM] = dk[head].astype(BF)

    def span_of(name):
        a, b = scatter.chips[name]
        return pl.ds(pl.multiple_of(square(a, b, 0) * rows, 2 * rows), 2 * rows)

    def down(name):
        a, b = scatter.chips[name]
        out = dot_wide(dkv[span_of(name), :], weights[:, 2 * cut :])
        if name in ("own", "y"):
            span = pl.ds(pl.multiple_of(b * 2 * rows, 2 * rows), 2 * rows)
            out = out + dot_wide(dq[span, :], weights[:, :cut])
        part[pl.ds(square(a, b, 0), 2)] = out.astype(BF).reshape(2, rows, model)

    down("far")
    scatter.send_pair("far")
    down("x")
    scatter.send_pair("x")
    scatter.add_pair("far")
    down("y")
    scatter.send_pair("y")
    scatter.add_pair("x")
    down("own")
    scatter.send_pair("own")
    scatter.add_pair("y")
    scatter.add_pair("own")
    tile = 256

    def out_rows(at):
        return pl.ds(pl.multiple_of(at * tile, tile), tile)

    @pl.loop(0, model // tile)
    def _(at):
        lanes = out_rows(at)
        all_rows = normed[:, :, lanes].reshape(8 * rows, tile)
        dw[out_rows(at), 2 * cut :] = dot_tall(all_rows, dkv[...]).astype(BF)

    scatter.turn_corner()

    @pl.loop(0, model // tile)
    def _(at):
        lanes = out_rows(at)
        mine = normed[pl.ds(ctx * 4, 4), :, lanes].reshape(4 * rows, tile)
        dw[out_rows(at), :cut] = dot_tall(mine, dq[...]).astype(BF)
        upper = gathered[:, :, lanes].reshape(4 * rows, tile)
        dw[out_rows(at), cut : 2 * cut] = dot_tall(upper, mixed[...]).astype(BF)

    keep = pltpu.make_async_copy(dw, dw_hbm, local.at[7])
    keep.start()
    grad_out[...] = grad
    modulate_backward(scatter.total(), hidden_ref[...], mods_ref[1:2, :], grad_out, small_out)
    gather.finish()
    scatter.finish()
    extra.finish()
    keep.wait()


def layer_backward_kernel(ways, prior, *refs):
    hop, before = int(ways > 1), int(ways > 1 and prior)
    (
        (grad, mods),
        feed_in,
        attention_in,
        prior_grads,
        prior_shard,
        (grad_out, small_feed, small_attention, dw_feed, dw_attention),
        shard_before,
        shard_feed,
        swap_out,
        (middle,),
        feed_scratch,
        feed_extra,
        feed_sems,
        scratch,
        hops,
        swap_buf,
        sems,
    ) = split_refs(
        refs, 2, 5, 9, before, before, 5, before, hop, before, 1, 11, 4 * before, 3, 18, 3 * hop,
        before, 3,
    )
    hidden, branch, *rest = feed_in
    feed_backward_kernel(
        ways,
        ways,
        before == 1,
        0,
        grad,
        hidden,
        branch,
        mods,
        *rest,
        *prior_grads,
        middle,
        small_feed,
        dw_feed,
        *shard_before,
        *feed_scratch,
        *feed_extra,
        *feed_sems,
    )
    hidden, branch, *rest = attention_in
    dw = feed_scratch[6]
    sources = ((dw,) if hop else ()) + tuple(prior_shard) + tuple(shard_before)
    attention_backward_kernel(
        ways,
        hop == 1,
        2 * before,
        middle,
        hidden,
        branch,
        mods,
        *rest,
        *sources,
        grad_out,
        small_attention,
        dw_attention,
        *shard_feed,
        *swap_out,
        *scratch,
        *((dw,) if hop else ()),
        *hops,
        *swap_buf,
        *sems,
    )


def layer_backward(grad, mods, blocks, kept_attention, kept_feed, prior, number):
    rows, model = grad.shape
    attention_weights, feed_weights = blocks
    shape = attention_weights.shape
    cut, width = shape[1] // 4, shape[1] // 2
    heads = cut // HEAD_DIM
    ways = lax.axis_size("shard")
    if ways > HOP_WAYS:
        ways = 1
    hop, before = ways > 1, prior is not None
    shard = (shape[0] // ways, shape[1])
    hidden, normed, pre, branch = kept_feed
    feed_in = [hidden, branch, feed_weights, normed, pre]
    hidden, branch, *saved = kept_attention
    attention_in = [hidden, branch, attention_weights, *saved]
    outs = [sds((rows, model), F32), sds((3, model), F32), sds((3, model), F32)]
    outs += [sds(shape, BF)] * 2
    specs = [VMEM, VMEM, VMEM, ANY, ANY]
    outs += [sds(shard, BF)] * (before + hop) + [sds((2, *shard), BF)] * before
    specs += [VMEM] * (before + hop) + [ANY] * before
    line = [
        pltpu.VMEM((max(line_copies(ways), 1), *shard), BF),
        pltpu.VMEM((2, *shard), BF),
        pltpu.VMEM(shard, F32),
    ]

    def buffers(copies, locals_used):
        return [
            pltpu.SemaphoreType.DMA((locals_used,)),
            pltpu.SemaphoreType.DMA((copies,)),
            pltpu.SemaphoreType.DMA((copies,)),
        ]

    group = [
        pltpu.VMEM((8, rows, model), BF),
        pltpu.VMEM((4, rows, model), BF),
        pltpu.VMEM((4, rows, model), BF),
        pltpu.VMEM((6, rows // 2, model), BF),
    ]
    scratch = [pltpu.VMEM((rows, model), F32)]
    scratch += [
        pltpu.VMEM(shape, BF),
        pltpu.VMEM((8, rows, model), BF),
        pltpu.VMEM((8, rows, model), BF),
        pltpu.VMEM((8, rows, width), F32),
        pltpu.VMEM((8 * rows, width), BF),
        pltpu.VMEM((8 * rows, width), BF),
        pltpu.VMEM(shape, BF),
    ] + group
    if before:
        scratch += [pltpu.VMEM(shape, BF)] + line
    scratch += buffers(GATHER_COPIES + SCATTER_COPIES + line_copies(ways), 6)
    scratch += [pltpu.VMEM(leaf.shape, leaf.dtype) for leaf in [attention_weights, *saved]]
    scratch += [
        pltpu.VMEM((4, rows, model), BF),
        pltpu.VMEM((heads, 4 * rows, HEAD_DIM), BF),
        pltpu.VMEM((heads, 4 * rows, HEAD_DIM), BF),
        pltpu.VMEM((4 * rows, cut), BF),
        pltpu.VMEM((8 * rows, 2 * cut), BF),
        pltpu.VMEM((2 * heads, 8 * rows, HEAD_DIM), F32),
        pltpu.VMEM(shape, BF),
    ] + group
    if hop:
        scratch += line
    if before:
        scratch.append(pltpu.VMEM((2, *shard), BF))
    scratch += buffers(PAIR_COPIES + SCATTER_COPIES + line_copies(ways) + 2, 10)
    result = pl.pallas_call(
        functools.partial(layer_backward_kernel, ways, before),
        out_shape=outs,
        in_specs=[VMEM] * 4 + [ANY] * 3 + [VMEM] * 2 + [ANY] * (7 + 2 * before),
        out_specs=specs,
        scratch_shapes=scratch,
        compiler_params=pltpu.CompilerParams(collective_id=number, has_side_effects=True),
        name="layer_backward",
    )(grad, mods, *feed_in, *attention_in, *(prior if before else ()))
    grad, small_feed, small_attention, dw_feed, dw_attention, *rest = result
    shard_before = rest.pop(0) if before else None
    shard_feed = rest.pop(0) if hop else None
    swapped = rest.pop(0) if before else None
    return grad, small_feed, small_attention, dw_feed, dw_attention, shard_before, shard_feed, swapped


def exchange_kernel(ways, modes, pieces, by_tp, by_x, has_block, has_sums, swaps, *refs):
    count = len(modes)
    stacked = [number for number in range(count) if pieces[number] > 1]
    extra_in, extra_out = int(has_sums) + swaps, int(has_sums) + int(swaps > 0)
    extra_scratch = 4 * int(has_sums) + int(swaps > 0)
    block = int(has_block)
    parts, block_in, ex_in, outs, block_out, ex_out, scratch, stack_buf, block_buf, ex_scratch, sems = (
        split_refs(
            refs,
            sum(pieces),
            block,
            extra_in,
            count,
            block,
            extra_out,
            3 * count,
            len(stacked),
            block,
            extra_scratch,
            3,
        )
    )
    held, arrived, far = scratch[:count], scratch[count : 2 * count], scratch[2 * count :]
    local, send, recv = sems
    sums_src, swap_src, ex = take_extra(has_sums, swaps, ex_in, ex_out, ex_scratch)
    stages = 2 * int(by_tp) + int(by_x)
    used = count * (stages + ways - 1)
    extra = Extra(ways, sums_src, swap_src, ex, local, 1, send, recv, used)
    if has_sums:
        used += line_copies(ways)
    used += swaps
    extra.begin()
    ctx, row, core = place()
    tp = row * 2 + core
    at = lax.axis_index("shard")
    barrier = pltpu.get_barrier_semaphore()
    sides = [{"tp": row * 2 + 1 - core}, {"tp": (tp + 2) % 4}] if by_tp else []
    if by_x:
        sides.append({"ctx": 1 - ctx})
    greeted = sides if by_x or not swaps else sides + [{"ctx": 1 - ctx}]
    for where in greeted:
        pl.semaphore_signal(barrier, inc=1, device_id=where, device_id_type=MESH)
    for away in range(1, ways):
        pl.semaphore_signal(
            barrier, inc=1, device_id={"shard": (at + away) % ways}, device_id_type=MESH
        )
    pl.semaphore_wait(barrier, len(greeted) + ways - 1)
    copies = []
    now, taken = [], 0
    for number in range(count):
        given = parts[taken : taken + pieces[number]]
        taken += pieces[number]
        if number in stacked:
            into, first = stack_buf[stacked.index(number)], 0
            for ref in given:
                into[first : first + ref.shape[0]] = ref[...]
                first += ref.shape[0]
            given = [into]
        now.append(given[0])
    for stage, where in enumerate(sides):
        here = []
        for number in range(count):
            here.append(
                remote(
                    number * stages + stage,
                    now[number],
                    arrived[number].at[stage],
                    send,
                    recv,
                    **where,
                )
            )
            here[-1].start()
        if stage == 0:
            if has_block:
                line = LineGather(
                    ways, block_in[0], block_buf[0], local.at[0], send, recv, used
                )
                line.start()
            extra.start()
            extra.start_swap()
        for number in range(count):
            here[number].wait_recv()
            both = now[number][...].astype(F32) + arrived[number][stage].astype(F32)
            held[number][stage] = both.astype(held[number].dtype)
            now[number] = held[number].at[stage]
        copies += here
        if stage == 1:
            extra.step(2)
    if has_block:
        line.step(2)
    base = count * stages
    for number, mode in enumerate(modes):
        if mode == "gather":
            far[number][at] = now[number][...].astype(far[number].dtype)
            now[number] = far[number].at[at]
    waits = []
    for number, mode in enumerate(modes):
        for away in range(1, ways):
            to = (at + away) % ways
            copy = remote(
                base + number * (ways - 1) + away - 1,
                now[number].at[to] if mode == "scatter" else now[number],
                far[number].at[at],
                send,
                recv,
                shard=to,
            )
            copy.start()
            waits.append(copy)
        if mode != "gather":
            far[number][at] = now[number][at] if mode == "scatter" else now[number][...]
    for k in range(3, ways):
        if has_block:
            line.step(k)
        extra.step(k)
    for copy in waits:
        copy.wait_recv()
    for number, mode in enumerate(modes):
        if mode == "gather":
            outs[number][...] = far[number][...].astype(F32)
            continue
        total = far[number][0].astype(F32)
        for index in range(1, ways):
            total = total + far[number][index].astype(F32)
        outs[number][...] = total
    for copy in copies + waits:
        copy.wait_send()
    extra.finish()
    if has_block:
        line.finish()
        keep = pltpu.make_async_copy(block_buf[0], block_out[0], local.at[0])
        keep.start()
        keep.wait()


def stacked_shape(arrays):
    return (sum(array.shape[0] for array in arrays), *arrays[0].shape[1:])


def exchange(parts, number, by_tp=True, by_x=False, block=None, grads=None, swaps=()):
    ways = lax.axis_size("shard")
    if ways > HOP_WAYS:
        return exchange_plain(parts, by_tp, by_x)
    stages = 2 * int(by_tp) + int(by_x)
    modes, pieces = [mode for _, mode in parts], [len(arrays) for arrays, _ in parts]
    outs, held, arrived, far, stacks, given = [], [], [], [], [], []
    for arrays, mode in parts:
        whole, dtype = stacked_shape(arrays), arrays[0].dtype
        one = whole[1:] if mode == "scatter" else whole
        full = (ways, *one)
        given += list(arrays)
        outs.append(sds(full if mode == "gather" else one, F32))
        held.append(pltpu.VMEM((max(stages, 1), *whole), dtype))
        arrived.append(pltpu.VMEM((max(stages, 1), *whole), dtype))
        far.append(pltpu.VMEM(full, BF if mode == "gather" else dtype))
        if len(arrays) > 1:
            stacks.append(pltpu.VMEM(whole, dtype))
    specs = [VMEM] * len(outs)
    block_specs, block_scratch, inputs = [], [], len(given)
    copies = len(parts) * (stages + ways - 1)
    if block is not None:
        shape = (ways * block.shape[0], block.shape[1])
        given.append(block)
        block_specs.append(ANY)
        block_scratch.append(pltpu.VMEM(shape, BF))
        outs.append(sds(shape, BF))
        copies += line_copies(ways)
    more, more_outs, more_specs, more_scratch, more_copies = extra_shapes(ways, grads, swaps)
    copies += more_copies
    return pl.pallas_call(
        functools.partial(
            exchange_kernel,
            ways,
            tuple(modes),
            tuple(pieces),
            by_tp,
            by_x,
            block is not None,
            grads is not None,
            len(swaps),
        ),
        out_shape=outs + more_outs,
        in_specs=[VMEM] * inputs + block_specs + [ANY] * len(more),
        out_specs=specs + block_specs + more_specs,
        scratch_shapes=held
        + arrived
        + far
        + stacks
        + block_scratch
        + more_scratch
        + [
            pltpu.SemaphoreType.DMA((3,)),
            pltpu.SemaphoreType.DMA((copies,)),
            pltpu.SemaphoreType.DMA((copies,)),
        ],
        compiler_params=pltpu.CompilerParams(collective_id=number, has_side_effects=True),
        name="exchange",
    )(*given, *more)


def exchange_plain(parts, by_tp, by_x):
    near = (("ctx",) if by_x else ()) + (("tp",) if by_tp else ())
    outs = []
    for arrays, mode in parts:
        wide = jnp.concatenate(arrays, 0).astype(F32)
        if mode == "gather":
            outs.append(lax.all_gather(lax.psum(wide, near), "shard", axis=0))
        elif mode == "scatter":
            total = lax.psum_scatter(wide, "shard", scatter_dimension=0, tiled=True)
            outs.append(lax.psum(total, near)[0])
        else:
            outs.append(lax.psum(wide, ("shard",) + near))
    return outs


def loss_kernel(
    loss_scale,
    first_head,
    hidden_ref,
    ends_ref,
    packed_ref,
    target_ref,
    weight_ref,
    grad_out,
    small_out,
    head_out,
    loss_out,
):
    hidden, head = hidden_ref[...], packed_ref[first_head : first_head + PDIM, :].astype(BF)
    shift, scale = ends_ref[0:1, :], ends_ref[1:2, :]
    centre, scale_by = norm_rows(hidden)
    normed = (centre * scale_by * (1.0 + scale) + shift).astype(BF)
    misfit = dot_wide(normed, head) - target_ref[...]
    weighted = weight_ref[...] * misfit
    rows = jnp.sum(weighted * misfit, 1, keepdims=True)
    loss_out[...] = jnp.sum(rows, 0, keepdims=True) * loss_scale
    grad_pred = (2.0 * loss_scale * weighted).astype(BF)
    head_out[...] = dot_tall(grad_pred, normed)
    grad_out[...] = jnp.zeros_like(grad_out)
    modulate_backward(dot(grad_pred, head), hidden, scale, grad_out, small_out)


def loss_and_grad(hidden, ends, packed, first_head, target, weight, loss_scale):
    rows, model = hidden.shape
    return pl.pallas_call(
        functools.partial(loss_kernel, loss_scale, first_head),
        out_shape=[
            sds((rows, model), F32),
            sds((2, model), F32),
            sds((PDIM, model), F32),
            sds((1, 1), F32),
        ],
        in_specs=[VMEM] * 5,
        out_specs=[VMEM] * 4,
        name="loss_and_grad",
    )(hidden, ends, packed, target, weight)


def spread(values, at, axis_size):
    full = jnp.zeros((*values.shape[:-1], axis_size), values.dtype)
    return lax.dynamic_update_slice_in_dim(full, values, at, values.ndim - 1)


def silu_grad(values):
    gate = jax.nn.sigmoid(values)
    return gate * (1.0 + values * (1.0 - gate))


def local(
    noised,
    velocity,
    labels,
    time_ids,
    stem,
    stem_mean,
    stem_square,
    modulation,
    modulation_mean,
    modulation_square,
    attention_in,
    attention_in_mean,
    attention_in_square,
    attention_out,
    attention_out_mean,
    attention_out_square,
    feedforward,
    feedforward_mean,
    feedforward_square,
):
    tensor_ways = lax.axis_size("tp")
    shard_ways = lax.axis_size("shard")
    own_latent = lax.axis_index("shard")
    own_ctx = lax.axis_index("ctx")
    own_tp = lax.axis_index("tp")
    owned = stem.shape[1]
    first_owned = (own_latent * tensor_ways + lax.axis_index("tp")) * owned

    def own_columns(values):
        return lax.dynamic_slice_in_dim(values, first_owned, owned, values.ndim - 1)

    stem_low = stem.astype(jnp.bfloat16)
    class_own, time_in_own, time_out_own, shift_own, scale_own, patch_own, head_own = split_stem(
        stem_low
    )
    modulation_low = modulation.astype(jnp.bfloat16)
    mine = (jnp.arange(shard_ways) == own_latent).astype(jnp.float32)[:, None]
    packed_ids = mine * jnp.concatenate([labels, time_ids]).astype(jnp.float32)[None, :]
    ids_wide = jnp.pad(packed_ids, ((0, 0), (0, 126)))
    (ids_all,) = exchange([([ids_wide], "sum")], 10, by_tp=False)
    all_labels, all_times = ids_all[:, 0].astype(jnp.int32), ids_all[:, 1].astype(jnp.int32)
    latents = all_labels.shape[0]
    features = time_features(all_times).astype(jnp.bfloat16)
    time_pre = jnp.dot(features, time_in_own, preferred_element_type=jnp.float32)
    time_hidden_own = jax.nn.silu(time_pre).astype(jnp.bfloat16)
    hidden_half = feedforward.shape[3] // lax.axis_size("ctx")
    feed_low = lax.dynamic_slice_in_dim(feedforward, own_ctx * hidden_half, hidden_half, 3).astype(
        jnp.bfloat16
    )
    in_low, out_low = attention_in.astype(jnp.bfloat16), attention_out.astype(jnp.bfloat16)
    hops = shard_ways <= HOP_WAYS
    own_blocks, blocks = [], []
    for layer_at in range(LAYERS):
        parts = [in_low[layer_at, 0], out_low[layer_at], in_low[layer_at, 1], in_low[layer_at, 2]]
        own_blocks.append(jnp.concatenate(parts, 1))
        own_blocks.append(jnp.concatenate([feed_low[layer_at, 0], feed_low[layer_at, 1]], 1))
    to_send = jnp.concatenate([time_hidden_own, patch_own, head_own], 0)
    half_rows = own_blocks[0].shape[0] // 2
    exchanged = exchange(
        [([spread(to_send, first_owned, D)], "sum")], 11, block=own_blocks[0][:half_rows]
    )
    packed_wide = exchanged[0]
    packed = packed_wide.astype(jnp.bfloat16)
    time_hidden = packed[:latents]
    patch_in = packed[latents : latents + PDIM]
    onehot = (all_labels[:, None] == jnp.arange(CLASSES)[None, :]).astype(jnp.bfloat16)
    condition = jnp.dot(time_hidden, time_out_own, preferred_element_type=jnp.float32) + jnp.dot(
        onehot, class_own, preferred_element_type=jnp.float32
    )
    gated_own = jax.nn.silu(condition).astype(jnp.bfloat16)
    mod_part = jnp.einsum(
        "bd,lde->ble", gated_own, modulation_low, preferred_element_type=jnp.float32
    )
    first_half = exchanged[1:]
    mod_part = mod_part.reshape(latents, LAYERS * 6, D)
    exchanged = exchange(
        [([mod_part], "scatter"), ([spread(gated_own, first_owned, D)], "sum")],
        12,
        block=own_blocks[0][half_rows:],
    )
    layer_mods = exchanged[0].reshape(LAYERS, 6, D)
    gated = exchanged[1].astype(jnp.bfloat16)
    if hops:
        both = [part.reshape(shard_ways, half_rows, -1) for part in (first_half[0], exchanged[2])]
        blocks.append(jnp.concatenate(both, 1).reshape(shard_ways * 2 * half_rows, -1))
    else:
        for block in own_blocks:
            blocks.append(lax.all_gather(block, "shard", axis=0, tiled=True))
    end_own = jnp.stack(
        [
            jnp.dot(gated, shift_own, preferred_element_type=jnp.float32),
            jnp.dot(gated, scale_own, preferred_element_type=jnp.float32),
        ],
        1,
    )
    (end_mods,) = exchange([([spread(end_own, first_owned, D)], "scatter")], 13)

    pieces = patchify(noised)[0]
    rows_here = noised.shape[2] // PATCH
    first_row = (own_ctx * tensor_ways + lax.axis_index("tp")) * rows_here
    embedded = jnp.dot(pieces, patch_in, preferred_element_type=jnp.float32)
    hidden = embedded + positions(first_row, rows_here, noised.shape[3] // PATCH, D)
    saved, weights = [], blocks[0]
    for layer_at in range(LAYERS):
        final = layer_at + 1 == LAYERS
        feed_own, ahead, feed_weights = None, None, None
        if hops:
            feed_own = own_blocks[2 * layer_at + 1]
            ahead = None if final else own_blocks[2 * layer_at + 2]
        else:
            weights, feed_weights = blocks[2 * layer_at : 2 * layer_at + 2]
        hidden, kept_attention, kept_feed, feed_weights, following = layer_forward(
            hidden, layer_mods[layer_at], weights, feed_weights, feed_own, ahead, 2 + int(final)
        )
        saved.append((kept_attention, kept_feed, (weights, feed_weights)))
        weights = following

    target_rows = patchify(velocity)[0].astype(jnp.float32)
    weighting = 0.5 + time_ids.astype(jnp.float32)[:, None] / STEPS
    loss_scale = 1.0 / (shard_ways * PATCHES * PDIM)
    grad_hidden, grad_ends, grad_head, loss_local = loss_and_grad(
        hidden, end_mods, packed_wide, latents + PDIM, target_rows, weighting, loss_scale
    )

    small = [None] * (2 * LAYERS)
    shards, others = [None] * (2 * LAYERS), [None] * (2 * LAYERS)
    prior = None
    for layer_at in reversed(range(LAYERS)):
        kept_attention, kept_feed, pair = saved[layer_at]
        one, two = 2 * layer_at, 2 * layer_at + 1
        (
            grad_hidden,
            small[two],
            small[one],
            feed_grads,
            grads,
            shard_before,
            shards[two],
            swapped,
        ) = layer_backward(
            grad_hidden,
            layer_mods[layer_at],
            pair,
            kept_attention,
            kept_feed,
            prior,
            5 + int(prior is None),
        )
        if prior is not None:
            shards[one + 2] = shard_before
            others[two + 2], others[one + 2] = swapped[0], swapped[1]
        if hops:
            prior = (grads, shards[two])
        else:
            for half, local_grads in ((one, grads), (two, feed_grads)):
                shards[half] = lax.psum_scatter(
                    local_grads, "shard", scatter_dimension=0, tiled=True
                )
                others[half] = lax.ppermute(shards[half], "ctx", [(0, 1), (1, 0)])
    grad_embed = grad_hidden.astype(jnp.bfloat16)
    grad_patch = jnp.einsum("pf,pd->fd", pieces, grad_embed, preferred_element_type=jnp.float32)

    pixel = [grad_patch.astype(jnp.bfloat16), grad_head.astype(jnp.bfloat16)]
    loss_row = loss_local[0, 0] * jnp.ones((1, 128), jnp.float32)
    result = exchange(
        [(small + [grad_ends], "gather"), (pixel, "sum"), ([loss_row], "sum")],
        14,
        by_x=True,
        grads=grads,
        swaps=[shards[1]],
    )
    small, pixel, train_loss = result[0], result[1], result[2][0, 0]
    if hops:
        shards[0], others[1] = result[3], result[4][0]
    grad_mod = small[:, : 6 * LAYERS].reshape(latents, LAYERS, 6 * D)
    grad_ends = small[:, 6 * LAYERS :]
    ends_here = own_columns(grad_ends)
    gated_part = jnp.dot(
        ends_here[:, 0], shift_own.astype(jnp.float32).T, precision=highest
    ) + jnp.dot(ends_here[:, 1], scale_own.astype(jnp.float32).T, precision=highest)
    result = exchange([([gated_part], "sum")], 15, swaps=[shards[0]])
    if hops:
        others[0] = result[1][0]
    grad_gated = own_columns(result[0]) + jnp.einsum(
        "ble,lde->bd", grad_mod, modulation_low.astype(jnp.float32), precision=highest
    )
    grad_condition = grad_gated * silu_grad(condition)
    time_part = jnp.dot(grad_condition, time_out_own.astype(jnp.float32).T, precision=highest)
    (grad_time_hidden,) = exchange([([time_part], "sum")], 16)
    grad_time_hidden = own_columns(grad_time_hidden)
    grad_time_pre = grad_time_hidden * silu_grad(time_pre)
    gated_wide = gated.astype(jnp.float32)
    grad_ends_own = own_columns(pixel)
    shard_stem = jnp.concatenate(
        [
            jnp.dot(onehot.astype(jnp.float32).T, grad_condition, precision=highest),
            jnp.dot(features.astype(jnp.float32).T, grad_time_pre, precision=highest),
            jnp.dot(time_hidden.astype(jnp.float32).T, grad_condition, precision=highest),
            jnp.dot(gated_wide.T, ends_here[:, 0], precision=highest),
            jnp.dot(gated_wide.T, ends_here[:, 1], precision=highest),
            grad_ends_own,
        ],
        0,
    )
    shard_modulation = jnp.einsum(
        "bd,ble->lde", gated_own.astype(jnp.float32), grad_mod, precision=highest
    )
    cut = attention_in.shape[3]
    shard_in, shard_out, shard_hidden = [], [], []
    for layer_at in range(LAYERS):
        own, other = shards[2 * layer_at], others[2 * layer_at]
        both = own.astype(jnp.float32) + other.astype(jnp.float32)
        shard_out.append(both[:, cut : 2 * cut])
        shard_in.append(
            jnp.stack([both[:, number * cut : (number + 1) * cut] for number in (0, 2, 3)])
        )
        own, other = shards[2 * layer_at + 1], others[2 * layer_at + 1]
        low, high = jnp.where(own_ctx == 0, own, other), jnp.where(own_ctx == 0, other, own)
        shard_hidden.append(
            jnp.stack(
                [
                    jnp.concatenate([low[:, :hidden_half], high[:, :hidden_half]], 1),
                    jnp.concatenate([low[:, hidden_half:], high[:, hidden_half:]], 1),
                ]
            )
        )
    shard_in, shard_out = jnp.stack(shard_in), jnp.stack(shard_out)
    shard_hidden = jnp.stack(shard_hidden).astype(jnp.float32)
    flat_mod = grad_mod.reshape(latents, -1)
    wide_own = gated_own.astype(jnp.float32)
    modulation_square_sum = jnp.sum(
        jnp.dot(wide_own, wide_own.T, precision=highest)
        * jnp.dot(flat_mod, flat_mod.T, precision=highest)
    )
    squares = (
        jnp.sum(shard_stem * shard_stem)
        + modulation_square_sum
        + jnp.sum(shard_in * shard_in)
        + jnp.sum(shard_out * shard_out)
        + jnp.sum(shard_hidden * shard_hidden)
    )
    (sums,) = exchange([([squares * jnp.ones((1, 128), jnp.float32)], "sum")], 17)
    square_total = sums[0, 0]
    total_norm = jnp.sqrt(square_total)
    factor = clip_level / jnp.maximum(total_norm, clip_level)
    stem_out = adam_update(stem, stem_mean, stem_square, shard_stem, factor)
    mod_out = adam_update(modulation, modulation_mean, modulation_square, shard_modulation, factor)
    in_out = adam_update(attention_in, attention_in_mean, attention_in_square, shard_in, factor)
    proj_out = adam_update(
        attention_out, attention_out_mean, attention_out_square, shard_out, factor
    )
    feed_out = adam_update(feedforward, feedforward_mean, feedforward_square, shard_hidden, factor)
    return (
        train_loss,
        total_norm,
        stem_out[0],
        stem_out[1],
        stem_out[2],
        stem_out[3],
        mod_out[0],
        mod_out[1],
        mod_out[2],
        mod_out[3],
        in_out[0],
        in_out[1],
        in_out[2],
        in_out[3],
        proj_out[0],
        proj_out[1],
        proj_out[2],
        proj_out[3],
        feed_out[0],
        feed_out[1],
        feed_out[2],
        feed_out[3],
    )


def solution(mesh):
    placed = (
        P("shard", None, ("ctx", "tp"), None),
        P("shard", None, ("ctx", "tp"), None),
        P("shard"),
        P("shard"),
        P(None, ("shard", "tp")),
        P(None, ("shard", "tp")),
        P(None, ("shard", "tp")),
        P(None, ("shard", "tp"), None),
        P(None, ("shard", "tp"), None),
        P(None, ("shard", "tp"), None),
        P(None, None, "shard", "tp"),
        P(None, None, "shard", "tp"),
        P(None, None, "shard", "tp"),
        P(None, "shard", "tp"),
        P(None, "shard", "tp"),
        P(None, "shard", "tp"),
        P(None, None, "shard", "tp"),
        P(None, None, "shard", "tp"),
        P(None, None, "shard", "tp"),
    )
    return jax.shard_map(
        local,
        mesh=mesh,
        in_specs=placed,
        out_specs=(
            P(),
            P(),
            P(None, ("shard", "tp")),
            P(None, ("shard", "tp")),
            P(None, ("shard", "tp")),
            P(None, ("shard", "tp")),
            P(None, ("shard", "tp"), None),
            P(None, ("shard", "tp"), None),
            P(None, ("shard", "tp"), None),
            P(None, ("shard", "tp"), None),
            P(None, None, "shard", "tp"),
            P(None, None, "shard", "tp"),
            P(None, None, "shard", "tp"),
            P(None, None, "shard", "tp"),
            P(None, "shard", "tp"),
            P(None, "shard", "tp"),
            P(None, "shard", "tp"),
            P(None, "shard", "tp"),
            P(None, None, "shard", "tp"),
            P(None, None, "shard", "tp"),
            P(None, None, "shard", "tp"),
            P(None, None, "shard", "tp"),
        ),
        check_vma=False,
    )
```
